8 devices in a mesh: dp: 1 (over z), yax: 2 (over y), xax: 4 (over x, core).
Axes of the slice: x: 2, y: 2, z: 1, core: 2. Of those that a mesh axis runs over, the one named last changes fastest.
Arguments:
- hidden: bfloat16 [128, 4096], P('dp', 'xax')
- cache_len: int32 [128], P('dp')
- k_cache: bfloat16 [128, 8192, 128], P(('dp', 'yax', 'xax'))
- v_cache: bfloat16 [128, 8192, 128], P(('dp', 'yax', 'xax'))
- g_attn: float32 [4096], P('xax')
- w_query: bfloat16 [4096, 4096], P('xax', 'yax')
- w_key: bfloat16 [4096, 128], P('xax')
- w_value: bfloat16 [4096, 128], P('xax')
- w_gate: bfloat16 [4096, 16384], P('xax', 'yax')
- w_up: bfloat16 [4096, 16384], P('xax', 'yax')
- w_out: bfloat16 [4096, 4096], P('yax', 'xax')
- w_down: bfloat16 [16384, 4096], P('yax', 'xax')
- g_final: float32 [4096], P('xax')
- embedding: bfloat16 [50432, 4096], P('yax', 'xax')
Outputs:
- output 1: bfloat16 [128, 128], P(('dp', 'yax', 'xax'))
- output 2: bfloat16 [128, 128], P(('dp', 'yax', 'xax'))
- output 3: float32 [128, 50432], P('dp', ('yax', 'xax'))
- output 4: float32 [128], P('dp')
All inputs are finite; a program needn't handle non-finite values.
Results may differ from the reference program's by a relative error of at most 0.001.
Values are sent between devices in bfloat16 or wider.
A program may use at most 1 GiB of HBM per device.

```python
import jax
import jax.numpy as jnp
from jax import lax

D = 4096
HEADS = 32
HEAD = 128
FF = 16384
VOCAB = 50432
BATCH = 128
SEQ = 8192
ROW_BLOCK = 16

EPS = 1e-6
ROPE_BASE = 10000.0


def draw_lengths(key):
    drawn = jax.random.randint(key, (BATCH,), 1, SEQ, dtype=jnp.int32)
    row_ids = jnp.arange(BATCH)
    return jnp.where(row_ids == 0, SEQ - 1, jnp.where(row_ids == 1, 1, drawn)).astype(jnp.int32)


def setup_inputs(seed: int = 0, part: int = 0) -> dict:
    base_key = jax.random.key(seed)
    shared = jax.random.split(base_key, 10)
    own = jax.random.split(jax.random.fold_in(base_key, part), 5)

    def weight(key, shape, fan_in, gain):
        return (gain * fan_in ** -0.5 * jax.random.normal(key, shape, jnp.float32)).astype(jnp.bfloat16)

    col_scale = jnp.exp(0.5 * jax.random.normal(own[0], (D,), jnp.float32))
    hidden = jax.random.normal(own[1], (BATCH, D), jnp.float32) * col_scale
    k_cache = 2.5 * jax.random.normal(own[3], (BATCH, SEQ, HEAD), jnp.float32)
    v_cache = 2.0 * jax.random.normal(own[4], (BATCH, SEQ, HEAD), jnp.float32)
    return {
        "hidden": hidden.astype(jnp.bfloat16),
        "cache_len": draw_lengths(own[2]),
        "k_cache": k_cache.astype(jnp.bfloat16),
        "v_cache": v_cache.astype(jnp.bfloat16),
        "g_attn": 1.0 + 0.3 * jax.random.normal(shared[0], (D,), jnp.float32),
        "w_query": weight(shared[1], (D, HEADS * HEAD), D, 1.0),
        "w_key": weight(shared[2], (D, HEAD), D, 1.0),
        "w_value": weight(shared[3], (D, HEAD), D, 1.0),
        "w_gate": weight(shared[4], (D, FF), D, 1.0),
        "w_up": weight(shared[5], (D, FF), D, 1.0),
        "w_out": weight(shared[6], (HEADS * HEAD, D), HEADS * HEAD, 1.0),
        "w_down": weight(shared[7], (FF, D), FF, 1.0),
        "g_final": 1.0 + 0.3 * jax.random.normal(shared[8], (D,), jnp.float32),
        "embedding": weight(shared[9], (VOCAB, D), D, 2.0),
    }


def layer_norm(values_in, gain):
    row_mean = jnp.mean(values_in, axis=-1, keepdims=True)
    row_var = jnp.mean(jnp.square(values_in - row_mean), axis=-1, keepdims=True)
    return (values_in - row_mean) * lax.rsqrt(row_var + EPS) * gain


def rope_angle(positions):
    half_dim = HEAD // 2
    inv_freq = ROPE_BASE ** (-(jnp.arange(half_dim, dtype=jnp.float32) * 2.0) / HEAD)
    return positions.astype(jnp.float32)[:, None] * inv_freq[None, :]


def rotary(values_in, angles):
    half_dim = values_in.shape[-1] // 2
    cos_a = jnp.cos(angles)
    sin_a = jnp.sin(angles)
    first = values_in[..., :half_dim]
    second = values_in[..., half_dim:]
    return jnp.concatenate([first * cos_a - second * sin_a, second * cos_a + first * sin_a], axis=-1)


def attend_block(block):
    q_blk, kc_blk, vc_blk, kn_blk, vn_blk, len_blk = block
    positions = jnp.arange(SEQ)
    at_slot = positions[None, :, None] == len_blk[:, None, None]
    keys_all = jnp.where(at_slot, kn_blk[:, None, :], kc_blk)
    values_all = jnp.where(at_slot, vn_blk[:, None, :], vc_blk)
    scores = jnp.einsum("rhe,rse->rhs", q_blk.astype(jnp.float32), keys_all.astype(jnp.float32)) * HEAD ** -0.5
    valid = positions[None, None, :] <= len_blk[:, None, None]
    scores = jnp.where(valid, scores, -jnp.inf)
    prob_all = jax.nn.softmax(scores, axis=-1).astype(jnp.bfloat16)
    mixed = jnp.einsum("rhs,rse->rhe", prob_all.astype(jnp.float32), values_all.astype(jnp.float32))
    return mixed.astype(jnp.bfloat16)


def reference(hidden, cache_len, k_cache, v_cache, g_attn, w_query, w_key, w_value,
              w_gate, w_up, w_out, w_down, g_final, embedding):
    residual = hidden.astype(jnp.float32)
    normed = layer_norm(residual, g_attn).astype(jnp.bfloat16)
    query = jnp.dot(normed, w_query, preferred_element_type=jnp.float32).astype(jnp.bfloat16)
    key_new = jnp.dot(normed, w_key, preferred_element_type=jnp.float32).astype(jnp.bfloat16)
    value_new = jnp.dot(normed, w_value, preferred_element_type=jnp.float32).astype(jnp.bfloat16)
    gate = jnp.dot(normed, w_gate, preferred_element_type=jnp.float32).astype(jnp.bfloat16)
    up_val = jnp.dot(normed, w_up, preferred_element_type=jnp.float32).astype(jnp.bfloat16)
    angles = rope_angle(cache_len)
    query = rotary(query.astype(jnp.float32).reshape(BATCH, HEADS, HEAD), angles[:, None, :]).astype(jnp.bfloat16)
    key_new = rotary(key_new.astype(jnp.float32), angles).astype(jnp.bfloat16)
    blocks = BATCH // ROW_BLOCK
    attn_out = lax.map(attend_block, (
        query.reshape(blocks, ROW_BLOCK, HEADS, HEAD),
        k_cache.reshape(blocks, ROW_BLOCK, SEQ, HEAD),
        v_cache.reshape(blocks, ROW_BLOCK, SEQ, HEAD),
        key_new.reshape(blocks, ROW_BLOCK, HEAD),
        value_new.reshape(blocks, ROW_BLOCK, HEAD),
        cache_len.reshape(blocks, ROW_BLOCK)))
    attn_out = attn_out.reshape(BATCH, HEADS * HEAD)
    mlp_act = (jax.nn.silu(gate.astype(jnp.float32)) * up_val.astype(jnp.float32)).astype(jnp.bfloat16)
    branch_sum = (jnp.dot(attn_out, w_out, preferred_element_type=jnp.float32)
                  + jnp.dot(mlp_act, w_down, preferred_element_type=jnp.float32))
    residual_out = residual + branch_sum
    final_norm = layer_norm(residual_out, g_final).astype(jnp.bfloat16)
    logits = jnp.dot(final_norm, embedding.T, preferred_element_type=jnp.float32)
    log_norm = jax.nn.logsumexp(logits, axis=-1)
    return key_new, value_new, logits - log_norm[:, None], log_norm
```

```python
import functools

import jax
import jax.numpy as jnp
from jax import lax
from jax.experimental import pallas as pl
from jax.experimental.pallas import tpu as pltpu
from jax.sharding import PartitionSpec as P

EPS = 1e-6
ROPE_BASE = 10000.0
MESH = pl.DeviceIdType.MESH
F32 = jnp.float32
BF16 = jnp.bfloat16
LOW = -3e38


def place():
    y = lax.axis_index("yax")
    xi = lax.axis_index("xax")
    chip = xi // 2
    core = xi % 2
    return y, xi, chip, core, chip * 2 + (1 - core), (1 - chip) * 2 + core


def send(src, dst, send_sem, recv_sem, y, xi):
    return pltpu.make_async_remote_copy(src_ref=src, dst_ref=dst, send_sem=send_sem, recv_sem=recv_sem,
                                        device_id={"yax": y, "xax": xi}, device_id_type=MESH)


def enter(peers):
    barrier = pltpu.get_barrier_semaphore()
    for y, xi in peers:
        pl.semaphore_signal(barrier, inc=1, device_id={"yax": y, "xax": xi}, device_id_type=MESH)
    return lambda: pl.semaphore_wait(barrier, len(peers))


def to_lanes(first, second):
    rows = first.shape[0]
    lane = lax.broadcasted_iota(jnp.int32, (rows, 128), 1)
    tile = jnp.where(lane == 0, first, jnp.where(lane == 1, second, 0.0))
    if rows < 128:
        tile = jnp.concatenate([tile, jnp.zeros((128 - rows, 128), F32)], axis=0)
    return tile.T[:8]


def to_columns(first, second):
    row = lax.broadcasted_iota(jnp.int32, (128, 128), 0)
    tile = jnp.where(row == 0, first, jnp.where(row == 1, second, 0.0)).T
    return tile[:, 0:1], tile[:, 1:2]


def norm_stats(values, stat, y, xi, send_sems, recv_sems, ready, size):
    rows, width = values.shape
    mean_own = jnp.sum(values, axis=1, keepdims=True) / width
    diff = values - mean_own
    stat[xi] = to_lanes(mean_own, jnp.sum(diff * diff, axis=1, keepdims=True))
    ready()
    copies = [send(stat.at[xi], stat.at[xi], send_sems.at[d - 1], recv_sems.at[d - 1], y, (xi + d) % size)
              for d in range(1, size)]
    for copy in copies:
        copy.start()
    for copy in copies:
        copy.wait()
    tiles = [stat[i] for i in range(size)]
    mean_all = sum(t[0:1] for t in tiles) / size
    spread = sum(t[1:2] for t in tiles) + width * sum((t[0:1] - mean_all) * (t[0:1] - mean_all) for t in tiles)
    mean_col, rstd_col = to_columns(mean_all, lax.rsqrt(spread / (width * size) + EPS))
    return mean_col[:rows], rstd_col[:rows]


def qkv_kernel(hid, gain, cos, sin, wq, wk, wv, q_out, k_out, v_out, n_out,
               w_all, part, got_a, sum_b, got_b, total, q_rot, q_full, stat,
               w_sem, stat_s, stat_r, pair_s, pair_r):
    y, xi, chip, core, partner, twin = place()
    qc = wq.shape[1]
    hd = wk.shape[1]
    loads = [pltpu.make_async_copy(wq, w_all.at[:, pl.ds(0, qc)], w_sem.at[0]),
             pltpu.make_async_copy(wk, w_all.at[:, pl.ds(qc, hd)], w_sem.at[1]),
             pltpu.make_async_copy(wv, w_all.at[:, pl.ds(qc + hd, hd)], w_sem.at[2])]
    for load in loads:
        load.start()
    ready = enter([(y, (xi + d) % 4) for d in (1, 2, 3)] + [(1 - y, xi)])
    h = hid[...].astype(F32)
    mean, rstd = norm_stats(h, stat, y, xi, stat_s, stat_r, ready, 4)
    normed = ((h - mean) * rstd * gain[...]).astype(BF16)
    for core_o in range(2):
        for chip_o in range(2):
            for y_o in range(2):
                src = (y_o * 4 + chip_o * 2 + core_o) * 16
                dst = (core_o * 4 + chip_o * 2 + y_o) * 16
                n_out[dst:dst + 16, :] = normed[src:src + 16, :]
    for load in loads:
        load.wait()
    step = 256

    def project(i, carry):
        cols = pl.ds(pl.multiple_of(i * step, step), step)
        prod = jnp.dot(n_out[...], w_all[:, cols], preferred_element_type=F32)
        part[:, :, :, cols] = prod.reshape(2, 2, 32, step)
        return carry

    lax.fori_loop(0, (qc + 2 * hd) // step, project, 0)
    hop_a = send(part.at[1 - core], got_a, pair_s.at[0], pair_r.at[0], y, partner)
    hop_a.start()
    hop_a.wait_recv()
    sum_b[...] = part[core, 1 - chip] + got_a[1 - chip]
    hop_b = send(sum_b, got_b, pair_s.at[1], pair_r.at[1], y, twin)
    hop_b.start()
    own = part[core, chip] + got_a[chip]
    hop_b.wait_recv()
    total[...] = (own + got_b[...]).astype(BF16).astype(F32).reshape(2, 16, qc + 2 * hd)
    for y_o in range(2):
        block = y_o * 4 + chip * 2 + core
        cos_r, sin_r = cos[block], sin[block]
        for head in range(qc // hd):
            val = total[y_o, :, head * hd:(head + 1) * hd]
            q_rot[y_o, :, head * hd:(head + 1) * hd] = (val * cos_r + pltpu.roll(val, hd // 2, 1) * sin_r).astype(BF16)
    hop_c = send(q_rot.at[1 - y], q_full.at[y], pair_s.at[2], pair_r.at[2], 1 - y, xi)
    hop_c.start()
    mine = y * 4 + chip * 2 + core
    key = total[y, :, qc:qc + hd]
    k_out[...] = (key * cos[mine] + pltpu.roll(key, hd // 2, 1) * sin[mine]).astype(BF16)
    v_out[...] = total[y, :, qc + hd:qc + 2 * hd].astype(BF16)
    q_out[y] = q_rot[y]
    hop_c.wait_recv()
    q_out[1 - y] = q_full[1 - y]
    hop_a.wait_send()
    hop_b.wait_send()
    hop_c.wait_send()


def qkv_call(hid, gain, cos, sin, wq, wk, wv):
    rows, width = hid.shape
    qc, hd = wq.shape[1], wk.shape[1]
    cols = qc + 2 * hd
    vmem = pl.BlockSpec(memory_space=pltpu.VMEM)
    hbm = pl.BlockSpec(memory_space=pl.ANY)
    return pl.pallas_call(
        qkv_kernel, name="qkv",
        out_shape=[jax.ShapeDtypeStruct((2, 16, qc), BF16), jax.ShapeDtypeStruct((16, hd), BF16),
                   jax.ShapeDtypeStruct((16, hd), BF16), jax.ShapeDtypeStruct((rows, width), BF16)],
        in_specs=[vmem] * 4 + [hbm] * 3, out_specs=[vmem] * 4,
        scratch_shapes=[
            pltpu.VMEM((width, cols), BF16), pltpu.VMEM((2, 2, 32, cols), F32), pltpu.VMEM((2, 32, cols), F32),
            pltpu.VMEM((32, cols), F32), pltpu.VMEM((32, cols), F32), pltpu.VMEM((2, 16, cols), F32),
            pltpu.VMEM((2, 16, qc), BF16), pltpu.VMEM((2, 16, qc), BF16), pltpu.VMEM((4, 8, 128), F32),
            pltpu.SemaphoreType.DMA((3,)), pltpu.SemaphoreType.DMA((3,)), pltpu.SemaphoreType.DMA((3,)),
            pltpu.SemaphoreType.DMA((3,)), pltpu.SemaphoreType.DMA((3,))],
        compiler_params=pltpu.CompilerParams(collective_id=0, has_side_effects=True, vmem_limit_bytes=60 * 2**20),
    )(hid, gain, cos, sin, wq, wk, wv)


CHUNK = 1024
SLOTS = 4


def attend_kernel(lens, q_ref, kn_ref, vn_ref, k_hbm, v_hbm, o_ref, k_buf, v_buf, scores, k_sem, v_sem):
    seqs = q_ref.shape[0]
    scale = q_ref.shape[2] ** -0.5

    def chunks(b):
        return (lens[b] + CHUNK - 1) // CHUNK

    def fetch(b):
        slot = b % SLOTS

        def one(i, carry):
            rows = pl.ds(pl.multiple_of(i * CHUNK, CHUNK), CHUNK)
            pltpu.make_async_copy(k_hbm.at[b, rows], k_buf.at[slot, rows], k_sem.at[slot, i]).start()
            pltpu.make_async_copy(v_hbm.at[b, rows], v_buf.at[slot, rows], v_sem.at[slot, i]).start()
            return carry

        lax.fori_loop(0, chunks(b), one, 0)

    for b in range(SLOTS - 1):
        fetch(b)

    def sequence(b, carry):
        slot = b % SLOTS

        @pl.when(b + SLOTS - 1 < seqs)
        def _():
            fetch(b + SLOTS - 1)

        q = q_ref[b]
        length = lens[b]
        s_new = jnp.sum(q.astype(F32) * kn_ref[b].astype(F32), axis=1, keepdims=True) * scale

        def score(i, top):
            rows = pl.ds(pl.multiple_of(i * CHUNK, CHUNK), CHUNK)
            pltpu.make_async_copy(k_hbm.at[b, rows], k_buf.at[slot, rows], k_sem.at[slot, i]).wait()
            s = lax.dot_general(q, k_buf[slot, rows], (((1,), (1,)), ((), ())), preferred_element_type=F32) * scale
            pos = lax.broadcasted_iota(jnp.int32, s.shape, 1) + i * CHUNK
            s = jnp.where(pos < length, s, -jnp.inf)
            scores[i] = s
            return jnp.maximum(top, jnp.max(s, axis=1, keepdims=True))

        count = chunks(b)
        top = lax.fori_loop(0, count, score, s_new)

        def weigh(i, acc):
            e = jnp.exp(scores[i] - top)
            scores[i] = e
            return acc + jnp.sum(e, axis=1, keepdims=True)

        e_new = jnp.exp(s_new - top)
        inv = 1.0 / lax.fori_loop(0, count, weigh, e_new)

        def mix(i, acc):
            rows = pl.ds(pl.multiple_of(i * CHUNK, CHUNK), CHUNK)
            pltpu.make_async_copy(v_hbm.at[b, rows], v_buf.at[slot, rows], v_sem.at[slot, i]).wait()
            p = (scores[i] * inv).astype(BF16)
            return acc + jnp.dot(p, v_buf[slot, rows], preferred_element_type=F32)

        o_new = (e_new * inv).astype(BF16).astype(F32) * vn_ref[b].astype(F32)
        o_ref[b] = lax.fori_loop(0, count, mix, o_new).astype(BF16)
        return carry

    lax.fori_loop(0, seqs, sequence, 0)


def attend_call(lens, q, k_new, v_new, k_cache, v_cache):
    seqs, heads, hd = q.shape
    length = k_cache.shape[1]
    vmem = pl.BlockSpec(memory_space=pltpu.VMEM)
    hbm = pl.BlockSpec(memory_space=pl.ANY)
    return pl.pallas_call(
        attend_kernel, name="attend",
        out_shape=jax.ShapeDtypeStruct((seqs, heads, hd), BF16),
        in_specs=[pl.BlockSpec(memory_space=pltpu.SMEM)] + [vmem] * 3 + [hbm] * 2, out_specs=vmem,
        scratch_shapes=[
            pltpu.VMEM((SLOTS, length, hd), BF16), pltpu.VMEM((SLOTS, length, hd), BF16),
            pltpu.VMEM((length // CHUNK, heads, CHUNK), F32),
            pltpu.SemaphoreType.DMA((SLOTS, length // CHUNK)), pltpu.SemaphoreType.DMA((SLOTS, length // CHUNK))],
        compiler_params=pltpu.CompilerParams(vmem_limit_bytes=60 * 2**20),
    )(lens, q, k_new.reshape(seqs, 1, hd), v_new.reshape(seqs, 1, hd), k_cache, v_cache)


FC = 512
RING = 4


def mlp_kernel(normed, o_in, hid, gain, wg, wu, wo, wd, f_out,
               w_ring, wd_all, wo_all, part, got_a, sum_b, got_b, act, o_all, acc, y_got, f_all, stat,
               w_sem, wd_sem, wo_sem, a_s, a_r, b_s, b_r, m_s, m_r, p_s, p_r, o_s, o_r, stat_s, stat_r):
    y, xi, chip, core, partner, twin = place()
    steps = part.shape[0]
    ready = enter([(y, (xi + d) % 4) for d in (1, 2, 3)] + [(1 - y, xi)])

    def w_loads(j):
        cols = pl.ds(pl.multiple_of(j * FC, FC), FC)
        slot = j % RING
        return (pltpu.make_async_copy(wg.at[:, cols], w_ring.at[slot, 0], w_sem.at[slot, 0]),
                pltpu.make_async_copy(wu.at[:, cols], w_ring.at[slot, 1], w_sem.at[slot, 1]))

    def wd_load(j):
        return pltpu.make_async_copy(wd.at[pl.ds(pl.multiple_of(j * FC, FC), FC)], wd_all.at[j], wd_sem.at[j])

    def hop_a(j):
        return send(part.at[j, 1 - core], got_a.at[j], a_s.at[j], a_r.at[j], y, partner)

    def hop_b(j):
        return send(sum_b.at[j], got_b.at[j], b_s.at[j], b_r.at[j], y, twin)

    def hop_m(j):
        return send(act.at[j, core, chip], act.at[j, core, chip], m_s.at[j], m_r.at[j], y, twin)

    def hop_p(j):
        return send(act.at[j, core], act.at[j, core], p_s.at[j], p_r.at[j], y, partner)

    for j in range(RING - 1):
        for load in w_loads(j):
            load.start()
    hop_o0 = send(o_in.at[1 - y], o_all.at[core, chip, y], o_s.at[0], o_r.at[0], 1 - y, xi)
    hop_o1 = send(o_all.at[core, chip], o_all.at[core, chip], o_s.at[1], o_r.at[1], y, twin)
    hop_o2 = send(o_all.at[core], o_all.at[core], o_s.at[2], o_r.at[2], y, partner)
    o_all[core, chip, y] = o_in[y]
    ready()
    hop_o0.start()

    def add_pair(j):
        hop_a(j).wait_recv()
        sum_b[j] = part[j, core, 1 - chip] + got_a[j, 1 - chip]
        hop_b(j).start()

    def project(j, carry):
        @pl.when(j + RING - 1 < steps)
        def _():
            for load in w_loads(j + RING - 1):
                load.start()

        @pl.when(j + RING - 1 >= steps)
        def _():
            wd_load(j + RING - 1 - steps).start()

        slot = j % RING
        for i, load in enumerate(w_loads(j)):
            load.wait()
            prod = jnp.dot(normed[...], w_ring[slot, i], preferred_element_type=F32)
            part[j, :, :, :, i * FC:(i + 1) * FC] = prod.reshape(2, 2, 32, FC)
        hop_a(j).start()

        @pl.when(j >= 1)
        def _():
            add_pair(j - 1)
        return carry

    lax.fori_loop(0, steps, project, 0)
    for j in range(RING - 1, steps):
        wd_load(j).start()
    load_o = pltpu.make_async_copy(wo, wo_all, wo_sem)
    load_o.start()
    add_pair(steps - 1)
    hop_o0.wait_recv()
    hop_o1.start()
    acc[...] = jnp.zeros_like(acc)

    def activate(j):
        hop_b(j).wait_recv()
        both = part[j, core, chip] + got_a[j, chip] + got_b[j]
        gate = both[:, :FC].astype(BF16).astype(F32)
        up_val = both[:, FC:].astype(BF16).astype(F32)
        act[j, core, chip] = (jax.nn.silu(gate) * up_val).astype(BF16)
        hop_m(j).start()

    def pass_on(j):
        hop_m(j).wait_recv()
        hop_p(j).start()

    def contract(j):
        hop_p(j).wait_recv()
        wd_load(j).wait()
        acc[...] += jnp.dot(act[j].reshape(128, FC), wd_all[j], preferred_element_type=F32).reshape(acc.shape)

    def reduce(j, carry):
        @pl.when(j < steps)
        def _():
            activate(j)

        @pl.when((j >= 1) & (j < steps + 1))
        def _():
            pass_on(j - 1)

        @pl.when(j == 1)
        def _():
            hop_o1.wait_recv()
            hop_o2.start()

        @pl.when(j == 2)
        def _():
            hop_o2.wait_recv()
            load_o.wait()
            part_o = jnp.dot(o_all[...].reshape(128, o_all.shape[-1]), wo_all[...], preferred_element_type=F32)
            acc[...] += part_o.reshape(acc.shape)

        @pl.when(j >= 2)
        def _():
            contract(j - 2)
        return carry

    lax.fori_loop(0, steps + 2, reduce, 0)

    width = acc.shape[-1]
    hop_y = send(acc.at[:, 1 - y], y_got, o_s.at[3], o_r.at[3], 1 - y, xi)
    hop_y.start()
    hop_y.wait_recv()
    res = [hid[y * 4 + (i % 2) * 2 + i // 2].astype(F32) for i in range(4)]
    branch = acc[:, y] + y_got[...]
    r = jnp.concatenate(res, axis=0) + branch.reshape(64, width)
    mean, rstd = norm_stats(r, stat, y, xi, stat_s, stat_r, lambda: None, 4)
    f = ((r - mean) * rstd * gain[...]).astype(BF16)
    for i in range(4):
        f_all[y, (i % 2) * 2 + i // 2] = f[i * 16:(i + 1) * 16]
    hop_f = send(f_all.at[y], f_all.at[y], o_s.at[4], o_r.at[4], 1 - y, xi)
    hop_f.start()
    f_out[y] = f_all[y]
    hop_f.wait_recv()
    f_out[1 - y] = f_all[1 - y]

    def drain(j, carry):
        hop_a(j).wait_send()
        hop_b(j).wait_send()
        hop_m(j).wait_send()
        hop_p(j).wait_send()
        return carry

    lax.fori_loop(0, steps, drain, 0)
    for hop in (hop_o0, hop_o1, hop_o2, hop_y, hop_f):
        hop.wait_send()


def mlp_call(normed, o_in, hid, gain, wg, wu, wo, wd):
    width = normed.shape[1]
    steps = wg.shape[1] // FC
    oc = wo.shape[0]
    vmem = pl.BlockSpec(memory_space=pltpu.VMEM)
    hbm = pl.BlockSpec(memory_space=pl.ANY)
    dma = pltpu.SemaphoreType.DMA
    return pl.pallas_call(
        mlp_kernel, name="mlp",
        out_shape=jax.ShapeDtypeStruct((2, 4, 16, width), BF16),
        in_specs=[vmem] * 4 + [hbm] * 4, out_specs=vmem,
        scratch_shapes=[
            pltpu.VMEM((RING, 2, width, FC), BF16), pltpu.VMEM((steps, FC, width), BF16), pltpu.VMEM((oc, width), BF16),
            pltpu.VMEM((steps, 2, 2, 32, 2 * FC), F32), pltpu.VMEM((steps, 2, 32, 2 * FC), F32),
            pltpu.VMEM((steps, 32, 2 * FC), F32), pltpu.VMEM((steps, 32, 2 * FC), F32),
            pltpu.VMEM((steps, 2, 2, 32, FC), BF16), pltpu.VMEM((2, 2, 2, 16, oc), BF16),
            pltpu.VMEM((4, 2, 16, width), F32), pltpu.VMEM((4, 16, width), F32), pltpu.VMEM((2, 4, 16, width), BF16),
            pltpu.VMEM((4, 8, 128), F32),
            dma((RING, 2)), dma((steps,)), dma, dma((steps,)), dma((steps,)), dma((steps,)), dma((steps,)),
            dma((steps,)), dma((steps,)), dma((steps,)), dma((steps,)), dma((5,)), dma((5,)), dma((3,)), dma((3,))],
        compiler_params=pltpu.CompilerParams(collective_id=1, has_side_effects=True, vmem_limit_bytes=60 * 2**20),
    )(normed, o_in, hid, gain, wg, wu, wo, wd)


VC = 512
ERING = 8


def head_kernel(share, f_ref, emb, z_out, lse_out,
                e_ring, e_tail, buf_a, buf_b, buf_c, buf_d, got_a, got_b, got_c,
                t_a, t_b, t_c, t_d, tg_a, tg_b, tg_c, top, total, stat,
                e_sem, tail_sem, a_s, a_r, b_s, b_r, c_s, c_r, t_s, t_r, stat_s, stat_r):
    y, xi, chip, core, partner, twin = place()
    full = share // VC
    rest = share - full * VC
    tail = full * VC
    ready = enter([(y, (xi + d) % 4) for d in (1, 2, 3)] + [(1 - y, (xi + d) % 4) for d in range(4)])
    far = (1 - chip) * 2
    near = chip * 2

    def share_of(i):
        side = i // 2
        mine = i % 2
        base = far + side * (near - far)
        return base + (1 - core) + mine * (2 * core - 1)

    def e_load(t):
        k = (t // 2) % full
        i = (t // (2 * full)) * 2 + t % 2
        rows = pl.ds(pl.multiple_of(share_of(i) * share + k * VC, 32), VC)
        return pltpu.make_async_copy(emb.at[rows], e_ring.at[t % ERING], e_sem.at[t % ERING])

    def tail_load(i):
        rows = pl.ds(pl.multiple_of(share_of(i) * share + tail, 32), rest)
        return pltpu.make_async_copy(emb.at[rows], e_tail.at[i], tail_sem.at[i])

    for i in range(4):
        tail_load(i).start()
    for t in range(ERING - 1):
        e_load(t).start()

    def hop_a(k):
        return send(buf_a.at[k], got_a.at[k], a_s.at[k], a_r.at[k], y, partner)

    def hop_b(k):
        return send(buf_b.at[k], got_b.at[k], b_s.at[k], b_r.at[k], y, twin)

    def hop_c(k):
        return send(buf_c.at[k], got_c.at[k], c_s.at[k], c_r.at[k], y, partner)

    hop_ta = send(t_a, tg_a, t_s.at[0], t_r.at[0], y, partner)
    hop_tb = send(t_b, tg_b, t_s.at[1], t_r.at[1], y, twin)
    hop_tc = send(t_c, tg_c, t_s.at[2], t_r.at[2], y, partner)

    def product(e):
        return lax.dot_general(f_ref[...], e, (((1,), (1,)), ((), ())), preferred_element_type=F32)

    for t_ref in (t_a, t_b, t_c, t_d):
        t_ref[...] = jnp.zeros_like(t_ref)

    def tail_product(i, t_ref):
        tail_load(i).wait()
        t_ref[:, :rest] = product(e_tail[i])

    def chunk_product(t, buf, k):
        @pl.when(t + ERING - 1 < 4 * full)
        def _():
            e_load(t + ERING - 1).start()

        e_load(t).wait()
        buf[k] = product(e_ring[t % ERING])

    tail_product(0, t_a)
    ready()
    hop_ta.start()
    tail_product(1, t_b)
    hop_ta.wait_recv()
    t_b[...] += tg_a[...]
    hop_tb.start()

    def add_pair(k):
        hop_a(k).wait_recv()
        buf_b[k] += got_a[k]
        hop_b(k).start()

    def outward(k, carry):
        chunk_product(2 * k, buf_a, k)
        hop_a(k).start()
        chunk_product(2 * k + 1, buf_b, k)

        @pl.when(k >= 1)
        def _():
            add_pair(k - 1)
        return carry

    lax.fori_loop(0, full, outward, 0)
    add_pair(full - 1)
    tail_product(2, t_c)
    hop_tc.start()
    tail_product(3, t_d)

    def inward(k, carry):
        chunk_product(2 * full + 2 * k, buf_c, k)
        hop_c(k).start()
        chunk_product(2 * full + 2 * k + 1, buf_d, k)
        return carry

    lax.fori_loop(0, full, inward, 0)

    top[...] = jnp.full_like(top, LOW)
    total[...] = jnp.zeros_like(total)

    def fold(z):
        groups = [z[:, i:i + 128] for i in range(0, z.shape[1], 128)]
        high = functools.reduce(jnp.maximum, groups, top[...])
        total[...] = total[...] * jnp.exp(top[...] - high) + sum(jnp.exp(g - high) for g in groups)
        top[...] = high

    hop_tc.wait_recv()
    hop_tb.wait_recv()
    z_tail = t_d[...] + tg_c[...] + tg_b[...]
    z_out[:, tail:] = z_tail[:, :rest]
    lane = lax.broadcasted_iota(jnp.int32, z_tail.shape, 1)
    fold(jnp.where(lane < rest, z_tail, LOW))

    def finish(k, carry):
        hop_c(k).wait_recv()
        hop_b(k).wait_recv()
        z = buf_d[k] + got_c[k] + got_b[k]
        z_out[:, pl.ds(pl.multiple_of(k * VC, VC), VC)] = z
        fold(z)
        return carry

    lax.fori_loop(0, full, finish, 0)
    high = jnp.max(top[...], axis=1, keepdims=True)
    mass = jnp.sum(total[...] * jnp.exp(top[...] - high), axis=1, keepdims=True)
    me = y * 4 + xi
    stat[me] = to_lanes(high, mass)
    copies = []
    for dy in range(2):
        for d in range(4):
            if dy or d:
                i = dy * 4 + d - 1
                copies.append(send(stat.at[me], stat.at[me], stat_s.at[i], stat_r.at[i],
                                   y + dy * (1 - 2 * y), (xi + d) % 4))
    for copy in copies:
        copy.start()
    for copy in copies:
        copy.wait()
    highs = [stat[i][0:1] for i in range(8)]
    best = functools.reduce(jnp.maximum, highs)
    mass_all = sum(stat[i][1:2] * jnp.exp(highs[i] - best) for i in range(8))
    lse_out[...] = best + jnp.log(mass_all)

    def drain(k, carry):
        hop_a(k).wait_send()
        hop_b(k).wait_send()
        hop_c(k).wait_send()
        return carry

    lax.fori_loop(0, full, drain, 0)
    for hop in (hop_ta, hop_tb, hop_tc):
        hop.wait_send()


def head_call(f, emb):
    rows, width = f.shape
    share = emb.shape[0] // 4
    full = share // VC
    rest = share - full * VC
    vmem = pl.BlockSpec(memory_space=pltpu.VMEM)
    hbm = pl.BlockSpec(memory_space=pl.ANY)
    dma = pltpu.SemaphoreType.DMA
    tail_w = -(-rest // 128) * 128
    return pl.pallas_call(
        functools.partial(head_kernel, share), name="head",
        out_shape=[jax.ShapeDtypeStruct((rows, share), F32), jax.ShapeDtypeStruct((1, rows), F32)],
        in_specs=[vmem, hbm], out_specs=[vmem, vmem],
        scratch_shapes=[pltpu.VMEM((ERING, VC, width), BF16), pltpu.VMEM((4, rest, width), BF16)]
        + [pltpu.VMEM((full, rows, VC), F32)] * 7 + [pltpu.VMEM((rows, tail_w), F32)] * 7
        + [pltpu.VMEM((rows, 128), F32)] * 2 + [pltpu.VMEM((8, 8, 128), F32)]
        + [dma((ERING,)), dma((4,))] + [dma((full,))] * 6 + [dma((3,))] * 2 + [dma((7,))] * 2,
        compiler_params=pltpu.CompilerParams(collective_id=2, has_side_effects=True, vmem_limit_bytes=60 * 2**20),
    )(f, emb)


def solution(mesh):
    row_spec = P(("dp", "yax", "xax"))

    def local_step(hidden, cache_len, k_cache, v_cache, g_attn, w_query, w_key, w_value,
                   w_gate, w_up, w_out, w_down, g_final, embedding):
        rows, width = hidden.shape
        own_rows, _, head_dim = k_cache.shape
        half = head_dim // 2
        own_start = (lax.axis_index("yax") * 4 + lax.axis_index("xax")) * own_rows
        inv_freq = ROPE_BASE ** (-(jnp.arange(half, dtype=F32) * 2.0) / head_dim)
        angles = cache_len.astype(F32)[:, None] * inv_freq[None, :]
        cos_a, sin_a = jnp.cos(angles), jnp.sin(angles)
        cos_t = jnp.concatenate([cos_a, cos_a], axis=1).reshape(8, own_rows, head_dim)
        sin_t = jnp.concatenate([-sin_a, sin_a], axis=1).reshape(8, own_rows, head_dim)

        q, key_own, value_own, normed = qkv_call(hidden, g_attn[None], cos_t, sin_t, w_query, w_key, w_value)
        half_heads = w_query.shape[1] // head_dim
        q = q.reshape(2, own_rows, half_heads, head_dim).transpose(1, 0, 2, 3).reshape(own_rows, 2 * half_heads, head_dim)
        len_own = lax.dynamic_slice_in_dim(cache_len, own_start, own_rows, axis=0)
        attn = attend_call(len_own, q, key_own, value_own, k_cache, v_cache)
        attn = attn.reshape(own_rows, 2, half_heads * head_dim).transpose(1, 0, 2)
        f = mlp_call(normed, attn, hidden.reshape(8, own_rows, width), g_final[None], w_gate, w_up, w_out, w_down)
        logits, log_norm = head_call(f.reshape(rows, width), embedding)
        log_norm = log_norm[0]
        return key_own, value_own, logits - log_norm[:, None], log_norm

    in_specs = (P("dp", "xax"), P("dp"), row_spec, row_spec, P("xax"), P("xax", "yax"),
                P("xax", None), P("xax", None), P("xax", "yax"), P("xax", "yax"),
                P("yax", "xax"), P("yax", "xax"), P("xax"), P("yax", "xax"))
    out_specs = (row_spec, row_spec, P("dp", ("yax", "xax")), P("dp"))
    return jax.shard_map(local_step, mesh=mesh, in_specs=in_specs, out_specs=out_specs, check_vma=False)
```

```python
import functools

import jax
import jax.numpy as jnp
from jax import lax
from jax.experimental import pallas as pl
from jax.experimental.pallas import tpu as pltpu
from jax.sharding import PartitionSpec as P

EPS = 1e-6
ROPE_BASE = 10000.0
MESH = pl.DeviceIdType.MESH
F32 = jnp.float32
BF16 = jnp.bfloat16
LOW = -3e38


def place():
    y = lax.axis_index("yax")
    xi = lax.axis_index("xax")
    chip = xi // 2
    core = xi % 2
    return y, xi, chip, core, chip * 2 + (1 - core), (1 - chip) * 2 + core


def send(src, dst, send_sem, recv_sem, y, xi):
    return pltpu.make_async_remote_copy(src_ref=src, dst_ref=dst, send_sem=send_sem, recv_sem=recv_sem,
                                        device_id={"yax": y, "xax": xi}, device_id_type=MESH)


def enter(peers):
    barrier = pltpu.get_barrier_semaphore()
    for y, xi in peers:
        pl.semaphore_signal(barrier, inc=1, device_id={"yax": y, "xax": xi}, device_id_type=MESH)
    return lambda: pl.semaphore_wait(barrier, len(peers))


def to_lanes(first, second):
    rows = first.shape[0]
    lane = lax.broadcasted_iota(jnp.int32, (rows, 128), 1)
    tile = jnp.where(lane == 0, first, jnp.where(lane == 1, second, 0.0))
    if rows < 128:
        tile = jnp.concatenate([tile, jnp.zeros((128 - rows, 128), F32)], axis=0)
    return tile.T[:8]


def to_columns(first, second):
    row = lax.broadcasted_iota(jnp.int32, (128, 128), 0)
    tile = jnp.where(row == 0, first, jnp.where(row == 1, second, 0.0)).T
    return tile[:, 0:1], tile[:, 1:2]


def norm_stats(values, stat, y, xi, send_sems, recv_sems, ready, size):
    rows, width = values.shape
    mean_own = jnp.sum(values, axis=1, keepdims=True) / width
    diff = values - mean_own
    stat[xi] = to_lanes(mean_own, jnp.sum(diff * diff, axis=1, keepdims=True))
    ready()
    copies = [send(stat.at[xi], stat.at[xi], send_sems.at[d - 1], recv_sems.at[d - 1], y, (xi + d) % size)
              for d in range(1, size)]
    for copy in copies:
        copy.start()
    for copy in copies:
        copy.wait()
    tiles = [stat[i] for i in range(size)]
    mean_all = sum(t[0:1] for t in tiles) / size
    spread = sum(t[1:2] for t in tiles) + width * sum((t[0:1] - mean_all) * (t[0:1] - mean_all) for t in tiles)
    mean_col, rstd_col = to_columns(mean_all, lax.rsqrt(spread / (width * size) + EPS))
    return mean_col[:rows], rstd_col[:rows]


FC = 512
RING = 4
GROUP = 4
KVS = 3


def layer_kernel(lens, hid, gain, gain_f, cos, sin, wq, wk, wv, wg, wu, wo, wd, k_hbm, v_hbm,
                 k_out, v_out, f_out,
                 n_perm, w_ring, w_kv, part_q, ga_q, sb_q, gb_q, total, q_rot, q_full, q_heads, o_heads, kn, vn,
                 part, got_a, sum_b, got_b, act, o_in, o_all, wd_ring, k_buf, v_buf, scores, probs,
                 acc, y_got, f_all, stat, stat_f,
                 w_sem, kv_sem, wd_sem, k_sem, v_sem, a_s, a_r, b_s, b_r, m_s, m_r, p_s, p_r,
                 q_s, q_r, o_s, o_r, st_s, st_r, sf_s, sf_r):
    y, xi, chip, core, partner, twin = place()
    width = n_perm.shape[1]
    qc, hd = wq.shape[1], wk.shape[1]
    heads = qc // hd
    steps = part.shape[0]
    groups = act.shape[0]
    seqs = q_heads.shape[0]
    length = k_buf.shape[1]
    mine = y * 4 + xi
    ready = enter([(y, (xi + d) % 4) for d in (1, 2, 3)] + [(1 - y, xi)])

    def q_loads(s):
        return [pltpu.make_async_copy(wq.at[:, pl.ds((2 * s + i) * FC, FC)], w_ring.at[s, i], w_sem.at[s, i])
                for i in range(2)]

    def w_loads(j):
        cols = pl.ds(pl.multiple_of(j * FC, FC), FC)
        slot = (j + 2) % RING
        return [pltpu.make_async_copy(w.at[:, cols], w_ring.at[slot, i], w_sem.at[slot, i])
                for i, w in enumerate((wg, wu))]

    def start(copies):
        for copy in copies:
            copy.start()

    kv_w = [pltpu.make_async_copy(w, w_kv.at[:, pl.ds(i * hd, hd)], kv_sem.at[i]) for i, w in enumerate((wk, wv))]
    start(q_loads(0))
    start(q_loads(1))
    start(kv_w)
    start(w_loads(0))

    def cache_loads(b):
        slot = b % KVS
        return [pltpu.make_async_copy(k_hbm.at[b], k_buf.at[slot], k_sem.at[slot]),
                pltpu.make_async_copy(v_hbm.at[b], v_buf.at[slot], v_sem.at[slot])]

    def wd_load(g):
        src = wo if g == groups else wd.at[pl.ds(g * GROUP * FC, GROUP * FC)]
        return pltpu.make_async_copy(src, wd_ring.at[g % 2], wd_sem.at[g % 2])

    def hop_a(j):
        return send(part.at[j, 1 - core], got_a.at[j], a_s.at[j], a_r.at[j], y, partner)

    def hop_b(j):
        return send(sum_b.at[j], got_b.at[j], b_s.at[j], b_r.at[j], y, twin)

    def hop_m(g):
        return send(act.at[g, core, chip], act.at[g, core, chip], m_s.at[g], m_r.at[g], y, twin)

    def hop_p(g):
        return send(act.at[g, core], act.at[g, core], p_s.at[g], p_r.at[g], y, partner)

    hop_qa = send(part_q.at[1 - core], ga_q, q_s.at[0], q_r.at[0], y, partner)
    hop_qb = send(sb_q, gb_q, q_s.at[1], q_r.at[1], y, twin)
    hop_qc = send(q_rot.at[1 - y], q_full.at[y], q_s.at[2], q_r.at[2], 1 - y, xi)
    hop_o0 = send(o_in.at[1 - y], o_all.at[core, chip, y], o_s.at[0], o_r.at[0], 1 - y, xi)
    hop_o1 = send(o_all.at[core, chip], o_all.at[core, chip], o_s.at[1], o_r.at[1], y, twin)
    hop_o2 = send(o_all.at[core], o_all.at[core], o_s.at[2], o_r.at[2], y, partner)
    hop_y = send(acc.at[:, 1 - y], y_got, o_s.at[3], o_r.at[3], 1 - y, xi)
    hop_f = send(f_all.at[y], f_all.at[y], o_s.at[4], o_r.at[4], 1 - y, xi)

    h = hid[...].astype(F32).reshape(128, width)
    mean, rstd = norm_stats(h, stat, y, xi, st_s, st_r, ready, 4)
    normed = ((h - mean) * rstd * gain[...]).astype(BF16)
    for core_o in range(2):
        for chip_o in range(2):
            for y_o in range(2):
                src = (y_o * 4 + chip_o * 2 + core_o) * 16
                dst = (core_o * 4 + chip_o * 2 + y_o) * 16
                n_perm[dst:dst + 16, :] = normed[src:src + 16, :]

    for s in range(2):
        for i, load in enumerate(q_loads(s)):
            load.wait()
            prod = jnp.dot(n_perm[...], w_ring[s, i], preferred_element_type=F32)
            part_q[:, :, :, (2 * s + i) * FC:(2 * s + i + 1) * FC] = prod.reshape(2, 2, 32, FC)
        start(w_loads(s + 1))
    for load in kv_w:
        load.wait()
    part_q[:, :, :, qc:] = jnp.dot(n_perm[...], w_kv[...], preferred_element_type=F32).reshape(2, 2, 32, 2 * hd)
    hop_qa.start()

    def rotate_queries():
        hop_qb.wait_recv()
        both = part_q[core, chip] + ga_q[chip] + gb_q[...]
        total[...] = both.astype(BF16).astype(F32).reshape(2, 16, qc + 2 * hd)
        for y_o in range(2):
            block = y_o * 4 + chip * 2 + core
            cos_r, sin_r = cos[block], sin[block]
            for head in range(heads):
                val = total[y_o, :, head * hd:(head + 1) * hd]
                q_rot[y_o, :, head * hd:(head + 1) * hd] = (val * cos_r + pltpu.roll(val, hd // 2, 1) * sin_r).astype(BF16)
        hop_qc.start()
        key = total[y, :, qc:qc + hd]
        key = (key * cos[mine] + pltpu.roll(key, hd // 2, 1) * sin[mine]).astype(BF16)
        k_out[...] = key
        v_out[...] = total[y, :, qc + hd:].astype(BF16)
        kn[:, 0, :] = key.astype(F32)
        vn[:, 0, :] = total[y, :, qc + hd:]
        q_full[y] = q_rot[y]

    def spread_queries():
        hop_qc.wait_recv()
        for y_o in range(2):
            for head in range(heads):
                q_heads[:, y_o * heads + head, :] = q_full[y_o, :, head * hd:(head + 1) * hd].astype(F32)

    def add_pair(j):
        hop_a(j).wait_recv()
        sum_b[j] = part[j, core, 1 - chip] + got_a[j, 1 - chip]
        hop_b(j).start()

    def project(j, carry):
        @pl.when(j + 3 < steps)
        def _():
            start(w_loads(j + 3))

        slot = (j + 2) % RING
        for i, load in enumerate(w_loads(j)):
            load.wait()
            prod = jnp.dot(n_perm[...], w_ring[slot, i], preferred_element_type=F32)
            part[j, :, :, :, i * FC:(i + 1) * FC] = prod.reshape(2, 2, 32, FC)
        hop_a(j).start()

        @pl.when(j == 0)
        def _():
            hop_qa.wait_recv()
            sb_q[...] = part_q[core, 1 - chip] + ga_q[1 - chip]
            hop_qb.start()

        @pl.when(j >= 1)
        def _():
            add_pair(j - 1)

        @pl.when(j == 4)
        def _():
            for b in range(KVS):
                start(cache_loads(b))

        @pl.when(j == 8)
        def _():
            rotate_queries()

        @pl.when(j == 12)
        def _():
            spread_queries()
        return carry

    lax.fori_loop(0, steps, project, 0)
    add_pair(steps - 1)
    wd_load(0).start()
    wd_load(1).start()

    def activate(j):
        hop_b(j).wait_recv()
        both = part[j, core, chip] + got_a[j, chip] + got_b[j]
        gate = both[:, :FC].astype(BF16).astype(F32)
        up_val = both[:, FC:].astype(BF16).astype(F32)
        cols = pl.ds(pl.multiple_of((j % GROUP) * FC, FC), FC)
        act[j // GROUP, core, chip, :, cols] = (jax.nn.silu(gate) * up_val).astype(BF16)

        @pl.when(j % GROUP == GROUP - 1)
        def _():
            hop_m(j // GROUP).start()

    part_len = 1024

    def attend(b):
        slot = b % KVS
        scale = hd ** -0.5
        q32 = q_heads[b]
        q = q32.astype(BF16)
        limit = lens[mine * 16 + b]
        s_new = jnp.sum(q32 * kn[b], axis=1, keepdims=True) * scale
        load_k, load_v = cache_loads(b)
        load_k.wait()
        high = None
        for i in range(length // part_len):
            rows = slice(i * part_len, (i + 1) * part_len)
            s = lax.dot_general(q, k_buf[slot, rows], (((1,), (1,)), ((), ())), preferred_element_type=F32) * scale
            pos = lax.broadcasted_iota(jnp.int32, s.shape, 1) + i * part_len
            s = jnp.where(pos < limit, s, -jnp.inf)
            scores[:, rows] = s
            for c in range(0, part_len, 128):
                high = s[:, c:c + 128] if high is None else jnp.maximum(high, s[:, c:c + 128])
        top = jnp.maximum(jnp.max(high, axis=1, keepdims=True), s_new)
        mass = None
        for i in range(length // part_len):
            rows = slice(i * part_len, (i + 1) * part_len)
            e = jnp.exp(scores[:, rows] - top)
            scores[:, rows] = e
            for c in range(0, part_len, 128):
                mass = e[:, c:c + 128] if mass is None else mass + e[:, c:c + 128]
        e_new = jnp.exp(s_new - top)
        inv = 1.0 / (jnp.sum(mass, axis=1, keepdims=True) + e_new)
        for i in range(length // part_len):
            rows = slice(i * part_len, (i + 1) * part_len)
            probs[:, rows] = (scores[:, rows] * inv).astype(BF16)
        load_v.wait()
        o = jnp.dot(probs[...], v_buf[slot], preferred_element_type=F32)
        o = o + (e_new * inv).astype(BF16).astype(F32) * vn[b]
        o_heads[b] = o.astype(BF16).astype(F32)

        @pl.when(b + KVS < seqs)
        def _():
            start(cache_loads(b + KVS))

    def mix(j, carry):
        attend(j)
        activate(j)
        return carry

    lax.fori_loop(0, steps, mix, 0)
    for y_o in range(2):
        for head in range(heads):
            o_in[y_o, :, head * hd:(head + 1) * hd] = o_heads[:, y_o * heads + head, :].astype(BF16)
    o_all[core, chip, y] = o_in[y]
    hop_o0.start()
    for g in range(groups + 1):
        if g < groups:
            hop_m(g).wait_recv()
            hop_p(g).start()
            if g == 0:
                hop_o0.wait_recv()
                hop_o1.start()
            hop_p(g).wait_recv()
            left = act[g].reshape(128, GROUP * FC)
        else:
            hop_o1.wait_recv()
            hop_o2.start()
            hop_o2.wait_recv()
            left = o_all[...].reshape(128, qc)
        wd_load(g).wait()
        prod = jnp.dot(left, wd_ring[g % 2], preferred_element_type=F32).reshape(acc.shape)
        acc[...] = prod if g == 0 else acc[...] + prod
        if g + 2 <= groups:
            wd_load(g + 2).start()

    hop_y.start()
    hop_y.wait_recv()
    res = [hid[y * 4 + (i % 2) * 2 + i // 2].astype(F32) for i in range(4)]
    branch = acc[:, y] + y_got[...]
    r = jnp.concatenate(res, axis=0) + branch.reshape(64, width)
    mean, rstd = norm_stats(r, stat_f, y, xi, sf_s, sf_r, lambda: None, 4)
    f = ((r - mean) * rstd * gain_f[...]).astype(BF16)
    for i in range(4):
        f_all[y, (i % 2) * 2 + i // 2] = f[i * 16:(i + 1) * 16]
    hop_f.start()
    f_out[y] = f_all[y]
    hop_f.wait_recv()
    f_out[1 - y] = f_all[1 - y]

    def drain(j, carry):
        hop_a(j).wait_send()
        hop_b(j).wait_send()
        return carry

    lax.fori_loop(0, steps, drain, 0)
    for g in range(groups):
        hop_m(g).wait_send()
        hop_p(g).wait_send()
    for hop in (hop_qa, hop_qb, hop_qc, hop_o0, hop_o1, hop_o2, hop_y, hop_f):
        hop.wait_send()


def layer_call(lens, hid, gain, gain_f, cos, sin, wq, wk, wv, wg, wu, wo, wd, k_cache, v_cache):
    width = hid.shape[2]
    qc, hd = wq.shape[1], wk.shape[1]
    seqs, length, _ = k_cache.shape
    cols = qc + 2 * hd
    steps = wg.shape[1] // FC
    heads = 2 * qc // hd
    vmem = pl.BlockSpec(memory_space=pltpu.VMEM)
    hbm = pl.BlockSpec(memory_space=pl.ANY)
    dma = pltpu.SemaphoreType.DMA

    def f32(*shape):
        return pltpu.VMEM(shape, F32)

    def bf16(*shape):
        return pltpu.VMEM(shape, BF16)

    return pl.pallas_call(
        layer_kernel, name="layer",
        out_shape=[jax.ShapeDtypeStruct((16, hd), BF16), jax.ShapeDtypeStruct((16, hd), BF16),
                   jax.ShapeDtypeStruct((2, 4, 16, width), BF16)],
        in_specs=[pl.BlockSpec(memory_space=pltpu.SMEM)] + [vmem] * 5 + [hbm] * 9, out_specs=[vmem] * 3,
        scratch_shapes=[
            bf16(128, width), bf16(RING, 2, width, FC), bf16(width, 2 * hd),
            f32(2, 2, 32, cols), f32(2, 32, cols), f32(32, cols), f32(32, cols), f32(2, 16, cols),
            bf16(2, 16, qc), bf16(2, 16, qc), f32(seqs, heads, hd), f32(seqs, heads, hd), f32(seqs, 1, hd), f32(seqs, 1, hd),
            f32(steps, 2, 2, 32, 2 * FC), f32(steps, 2, 32, 2 * FC), f32(steps, 32, 2 * FC), f32(steps, 32, 2 * FC),
            bf16(steps // GROUP, 2, 2, 32, GROUP * FC), bf16(2, 16, qc), bf16(2, 2, 2, 16, qc), bf16(2, GROUP * FC, width),
            bf16(KVS, length, hd), bf16(KVS, length, hd), f32(heads, length), bf16(heads, length),
            f32(4, 2, 16, width), f32(4, 16, width), bf16(2, 4, 16, width), f32(4, 8, 128), f32(4, 8, 128),
            dma((RING, 2)), dma((2,)), dma((2,)), dma((KVS,)), dma((KVS,))] + [dma((steps,))] * 4
        + [dma((steps // GROUP,))] * 4 + [dma((3,))] * 2 + [dma((5,))] * 2 + [dma((3,))] * 4,
        compiler_params=pltpu.CompilerParams(collective_id=0, has_side_effects=True, vmem_limit_bytes=63 * 2**20),
    )(lens, hid, gain, gain_f, cos, sin, wq, wk, wv, wg, wu, wo, wd, k_cache, v_cache)


VC = 512
ERING = 8


def head_kernel(share, f_ref, emb, z_out, lse_out,
                e_ring, e_tail, buf_a, buf_b, buf_c, buf_d, got_a, got_b, got_c,
                t_a, t_b, t_c, t_d, tg_a, tg_b, tg_c, top, total, stat,
                e_sem, tail_sem, a_s, a_r, b_s, b_r, c_s, c_r, t_s, t_r, stat_s, stat_r):
    y, xi, chip, core, partner, twin = place()
    full = share // VC
    rest = share - full * VC
    tail = full * VC
    ready = enter([(y, (xi + d) % 4) for d in (1, 2, 3)] + [(1 - y, (xi + d) % 4) for d in range(4)])
    far = (1 - chip) * 2
    near = chip * 2

    def share_of(i):
        side = i // 2
        mine = i % 2
        base = far + side * (near - far)
        return base + (1 - core) + mine * (2 * core - 1)

    def e_load(t):
        k = (t // 2) % full
        i = (t // (2 * full)) * 2 + t % 2
        rows = pl.ds(pl.multiple_of(share_of(i) * share + k * VC, 32), VC)
        return pltpu.make_async_copy(emb.at[rows], e_ring.at[t % ERING], e_sem.at[t % ERING])

    def tail_load(i):
        rows = pl.ds(pl.multiple_of(share_of(i) * share + tail, 32), rest)
        return pltpu.make_async_copy(emb.at[rows], e_tail.at[i], tail_sem.at[i])

    for i in range(4):
        tail_load(i).start()
    for t in range(ERING - 1):
        e_load(t).start()

    def hop_a(k):
        return send(buf_a.at[k], got_a.at[k], a_s.at[k], a_r.at[k], y, partner)

    def hop_b(k):
        return send(buf_b.at[k], got_b.at[k], b_s.at[k], b_r.at[k], y, twin)

    def hop_c(k):
        return send(buf_c.at[k], got_c.at[k], c_s.at[k], c_r.at[k], y, partner)

    hop_ta = send(t_a, tg_a, t_s.at[0], t_r.at[0], y, partner)
    hop_tb = send(t_b, tg_b, t_s.at[1], t_r.at[1], y, twin)
    hop_tc = send(t_c, tg_c, t_s.at[2], t_r.at[2], y, partner)

    def product(e):
        return lax.dot_general(f_ref[...], e, (((1,), (1,)), ((), ())), preferred_element_type=F32)

    for t_ref in (t_a, t_b, t_c, t_d):
        t_ref[...] = jnp.zeros_like(t_ref)

    def tail_product(i, t_ref):
        tail_load(i).wait()
        t_ref[:, :rest] = product(e_tail[i])

    def chunk_product(t, buf, k):
        @pl.when(t + ERING - 1 < 4 * full)
        def _():
            e_load(t + ERING - 1).start()

        e_load(t).wait()
        buf[k] = product(e_ring[t % ERING])

    tail_product(0, t_a)
    ready()
    hop_ta.start()
    tail_product(1, t_b)
    hop_ta.wait_recv()
    t_b[...] += tg_a[...]
    hop_tb.start()

    def add_pair(k):
        hop_a(k).wait_recv()
        buf_b[k] += got_a[k]
        hop_b(k).start()

    def outward(k, carry):
        chunk_product(2 * k, buf_a, k)
        hop_a(k).start()
        chunk_product(2 * k + 1, buf_b, k)

        @pl.when(k >= 1)
        def _():
            add_pair(k - 1)
        return carry

    lax.fori_loop(0, full, outward, 0)
    add_pair(full - 1)
    tail_product(2, t_c)
    hop_tc.start()
    tail_product(3, t_d)

    def inward(k, carry):
        chunk_product(2 * full + 2 * k, buf_c, k)
        hop_c(k).start()
        chunk_product(2 * full + 2 * k + 1, buf_d, k)
        return carry

    lax.fori_loop(0, full, inward, 0)

    top[...] = jnp.full_like(top, LOW)
    total[...] = jnp.zeros_like(total)

    def fold(z):
        groups = [z[:, i:i + 128] for i in range(0, z.shape[1], 128)]
        high = functools.reduce(jnp.maximum, groups, top[...])
        total[...] = total[...] * jnp.exp(top[...] - high) + sum(jnp.exp(g - high) for g in groups)
        top[...] = high

    hop_tc.wait_recv()
    hop_tb.wait_recv()
    z_tail = t_d[...] + tg_c[...] + tg_b[...]
    z_out[:, tail:] = z_tail[:, :rest]
    lane = lax.broadcasted_iota(jnp.int32, z_tail.shape, 1)
    fold(jnp.where(lane < rest, z_tail, LOW))

    def finish(k, carry):
        hop_c(k).wait_recv()
        hop_b(k).wait_recv()
        z = buf_d[k] + got_c[k] + got_b[k]
        z_out[:, pl.ds(pl.multiple_of(k * VC, VC), VC)] = z
        fold(z)
        return carry

    lax.fori_loop(0, full, finish, 0)
    high = jnp.max(top[...], axis=1, keepdims=True)
    mass = jnp.sum(total[...] * jnp.exp(top[...] - high), axis=1, keepdims=True)
    me = y * 4 + xi
    stat[me] = to_lanes(high, mass)
    copies = []
    for dy in range(2):
        for d in range(4):
            if dy or d:
                i = dy * 4 + d - 1
                copies.append(send(stat.at[me], stat.at[me], stat_s.at[i], stat_r.at[i],
                                   y + dy * (1 - 2 * y), (xi + d) % 4))
    for copy in copies:
        copy.start()
    for copy in copies:
        copy.wait()
    highs = [stat[i][0:1] for i in range(8)]
    best = functools.reduce(jnp.maximum, highs)
    mass_all = sum(stat[i][1:2] * jnp.exp(highs[i] - best) for i in range(8))
    lse_out[...] = best + jnp.log(mass_all)

    def drain(k, carry):
        hop_a(k).wait_send()
        hop_b(k).wait_send()
        hop_c(k).wait_send()
        return carry

    lax.fori_loop(0, full, drain, 0)
    for hop in (hop_ta, hop_tb, hop_tc):
        hop.wait_send()


def head_call(f, emb):
    rows, width = f.shape
    share = emb.shape[0] // 4
    full = share // VC
    rest = share - full * VC
    vmem = pl.BlockSpec(memory_space=pltpu.VMEM)
    hbm = pl.BlockSpec(memory_space=pl.ANY)
    dma = pltpu.SemaphoreType.DMA
    tail_w = -(-rest // 128) * 128
    return pl.pallas_call(
        functools.partial(head_kernel, share), name="head",
        out_shape=[jax.ShapeDtypeStruct((rows, share), F32), jax.ShapeDtypeStruct((1, rows), F32)],
        in_specs=[vmem, hbm], out_specs=[vmem, vmem],
        scratch_shapes=[pltpu.VMEM((ERING, VC, width), BF16), pltpu.VMEM((4, rest, width), BF16)]
        + [pltpu.VMEM((full, rows, VC), F32)] * 7 + [pltpu.VMEM((rows, tail_w), F32)] * 7
        + [pltpu.VMEM((rows, 128), F32)] * 2 + [pltpu.VMEM((8, 8, 128), F32)]
        + [dma((ERING,)), dma((4,))] + [dma((full,))] * 6 + [dma((3,))] * 2 + [dma((7,))] * 2,
        compiler_params=pltpu.CompilerParams(collective_id=1, has_side_effects=True, vmem_limit_bytes=60 * 2**20),
    )(f, emb)


def solution(mesh):
    row_spec = P(("dp", "yax", "xax"))

    def local_step(hidden, cache_len, k_cache, v_cache, g_attn, w_query, w_key, w_value,
                   w_gate, w_up, w_out, w_down, g_final, embedding):
        rows, width = hidden.shape
        own_rows, _, head_dim = k_cache.shape
        half = head_dim // 2
        inv_freq = ROPE_BASE ** (-(jnp.arange(half, dtype=F32) * 2.0) / head_dim)
        angles = cache_len.astype(F32)[:, None] * inv_freq[None, :]
        cos_a, sin_a = jnp.cos(angles), jnp.sin(angles)
        cos_t = jnp.concatenate([cos_a, cos_a], axis=1).reshape(8, own_rows, head_dim)
        sin_t = jnp.concatenate([-sin_a, sin_a], axis=1).reshape(8, own_rows, head_dim)

        key_own, value_own, f = layer_call(cache_len, hidden.reshape(8, own_rows, width), g_attn[None], g_final[None], cos_t, sin_t,
                                           w_query, w_key, w_value, w_gate, w_up, w_out, w_down, k_cache, v_cache)
        logits, log_norm = head_call(f.reshape(rows, width), embedding)
        log_norm = log_norm[0]
        return key_own, value_own, logits - log_norm[:, None], log_norm

    in_specs = (P("dp", "xax"), P("dp"), row_spec, row_spec, P("xax"), P("xax", "yax"),
                P("xax", None), P("xax", None), P("xax", "yax"), P("xax", "yax"),
                P("yax", "xax"), P("yax", "xax"), P("xax"), P("yax", "xax"))
    out_specs = (row_spec, row_spec, P("dp", ("yax", "xax")), P("dp"))
    return jax.shard_map(local_step, mesh=mesh, in_specs=in_specs, out_specs=out_specs, check_vma=False)
```

```python
import functools

import jax
import jax.numpy as jnp
from jax import lax
from jax.experimental import pallas as pl
from jax.experimental.pallas import tpu as pltpu
from jax.sharding import PartitionSpec as P

EPS = 1e-6
ROPE_BASE = 10000.0
MESH = pl.DeviceIdType.MESH
F32 = jnp.float32
BF16 = jnp.bfloat16
LOW = -3e38
TWO, QUAD, OCT, OWN, PAIR, HALF, LANES = 2, 4, 8, 16, 32, 64, 128


def place():
    y = lax.axis_index("yax")
    xi = lax.axis_index("xax")
    chip = xi // 2
    core = xi % 2
    return y, xi, chip, core, chip * 2 + (1 - core), (1 - chip) * 2 + core


def send(src, dst, send_sem, recv_sem, y, xi):
    return pltpu.make_async_remote_copy(src_ref=src, dst_ref=dst, send_sem=send_sem, recv_sem=recv_sem,
                                        device_id={"yax": y, "xax": xi}, device_id_type=MESH)


def enter(peers):
    barrier = pltpu.get_barrier_semaphore()
    for y, xi in peers:
        pl.semaphore_signal(barrier, inc=1, device_id={"yax": y, "xax": xi}, device_id_type=MESH)
    return lambda: pl.semaphore_wait(barrier, len(peers))


def to_lanes(first, second):
    rows = first.shape[0]
    lane = lax.broadcasted_iota(jnp.int32, (rows, 128), 1)
    tile = jnp.where(lane == 0, first, jnp.where(lane == 1, second, 0.0))
    if rows < 128:
        tile = jnp.concatenate([tile, jnp.zeros((128 - rows, 128), F32)], axis=0)
    return tile.T[:8]


def to_columns(first, second):
    row = lax.broadcasted_iota(jnp.int32, (128, 128), 0)
    tile = jnp.where(row == 0, first, jnp.where(row == 1, second, 0.0)).T
    return tile[:, 0:1], tile[:, 1:2]


def norm_stats(values, stat, y, xi, send_sems, recv_sems, ready, size, after=lambda: None):
    rows, width = values.shape
    mean_own = jnp.sum(values, axis=1, keepdims=True) / width
    diff = values - mean_own
    stat[xi] = to_lanes(mean_own, jnp.sum(diff * diff, axis=1, keepdims=True))
    ready()
    copies = [send(stat.at[xi], stat.at[xi], send_sems.at[d - 1], recv_sems.at[d - 1], y, (xi + d) % size)
              for d in range(1, size)]
    for copy in copies:
        copy.start()
    after()
    for copy in copies:
        copy.wait()
    tiles = [stat[i] for i in range(size)]
    mean_all = sum(t[0:1] for t in tiles) / size
    spread = sum(t[1:TWO] for t in tiles) + width * sum((t[0:1] - mean_all) * (t[0:1] - mean_all) for t in tiles)
    mean_col, rstd_col = to_columns(mean_all, lax.rsqrt(spread / (width * size) + EPS))
    return mean_col[:rows], rstd_col[:rows]


FC = 512
WB = 1024
RING = 6
KVS = 3
HELD = 5


def step_kernel(lens, hid_h, gain_h, gain_fh, freq, wq, wk, wv, wg, wu, wo, wd, emb, k_hbm, v_hbm,
                kv_out, z_out, lse_out,
                hid, gain, gain_f, cos, sin, n_perm, ring, w_kv, part_q, ga_q, sb_q, gb_q, total, q_rot, q_full, q_heads, o_heads, kn, vn,
                pool, act, o_in, o_all, k_buf, v_buf, scores, probs, acc, y_got, f_all, f_nat, e_tail,
                t_a, t_b, tg_a, tg_b, t_c, tg_c, top, mass_l, stat, stat_f, stat_z,
                i_sem, r_sem, kv_sem, tail_sem, k_sem, v_sem, a_s, a_r, b_s, b_r, m_s, m_r, p_s, p_r, q_s, q_r,
                o_s, o_r, y_s, y_r, f_s, f_r, st_s, st_r, sf_s, sf_r,
                la_s, la_r, lb_s, lb_r, lc_s, lc_r, ta_s, ta_r, tb_s, tb_r, tc_s, tc_r, sz_s, sz_r):
    y, xi, chip, core, partner, twin = place()
    width = n_perm.shape[1]
    hw = width // TWO
    qc, hd = wq.shape[1], wk.shape[1]
    heads = qc // hd
    steps = wg.shape[1] // FC
    seqs = q_heads.shape[0]
    length = k_buf.shape[1]
    share = emb.shape[0] // 4
    full = share // WB
    rest = share - full * WB
    mine = y * 4 + xi
    ready = enter([(y, (xi + d) % 4) for d in (1, TWO, 3)] + [(1 - y, (xi + d) % 4) for d in range(4)])

    def start(copies):
        for copy in copies:
            copy.start()

    def q_loads(s):
        return [pltpu.make_async_copy(wq.at[:, pl.ds((TWO * s + i) * FC, FC)], ring.at[s, i], r_sem.at[s, i]) for i in range(TWO)]

    def w_loads(j):
        cols = pl.ds(pl.multiple_of(j * FC, FC), FC)
        slot = (j + TWO) % RING
        return [pltpu.make_async_copy(w.at[:, cols], ring.at[slot, i], r_sem.at[slot, i]) for i, w in enumerate((wg, wu))]

    inputs = [pltpu.make_async_copy(src, dst, i_sem.at[i])
              for i, (src, dst) in enumerate(((hid_h, hid), (gain_h, gain), (gain_fh, gain_f)))]
    start(inputs)
    kv_w = [pltpu.make_async_copy(w, w_kv.at[:, pl.ds(i * hd, hd)], kv_sem.at[i]) for i, w in enumerate((wk, wv))]
    start(q_loads(0))
    start(q_loads(1))
    start(kv_w)
    for j in range(RING - 3):
        start(w_loads(j))

    nd, no = wd.shape[0] // WB, wo.shape[0] // WB
    np_ = nd + no
    e_base = (np_, TWO * np_ + TWO * full)
    c_base = TWO * np_ + 4 * full
    d_base = c_base + full
    items = d_base + full
    far, near = (1 - chip) * TWO, chip * TWO

    def block(src, row, t):
        slot = t % RING
        return [pltpu.make_async_copy(src.at[pl.ds(row, WB), pl.ds(i * hw, hw)], ring.at[slot, i], r_sem.at[slot, i])
                for i in range(TWO)]

    def emb_row(quarter, k):
        return pl.multiple_of(quarter * share + k * WB, PAIR)

    def load_item(t):
        for base in (0, np_ + TWO * full):
            @pl.when((t >= base) & (t < base + nd))
            def _(base=base):
                start(block(wd, pl.multiple_of((t - base) * WB, WB), t))

            @pl.when((t >= base + nd) & (t < base + np_))
            def _(base=base):
                start(block(wo, pl.multiple_of((t - base - nd) * WB, WB), t))

        for base in e_base:
            @pl.when((t >= base) & (t < base + TWO * full))
            def _(base=base):
                k, own = (t - base) // TWO, (t - base) % TWO
                start(block(emb, emb_row(far + (1 - core) + own * (TWO * core - 1), k), t))

        @pl.when((t >= c_base) & (t < d_base))
        def _():
            start(block(emb, emb_row(near + 1 - core, t - c_base), t))

        @pl.when((t >= d_base) & (t < items))
        def _():
            start(block(emb, emb_row(near + core, t - d_base), t))

    def take_item(t):
        load_item(t + RING - 1)
        for copy in block(wd, 0, t):
            copy.wait()
        return t % RING

    def tail_load(i):
        quarter = (far + 1 - core, far + core, near + 1 - core, near + core)[i]
        rows = pl.ds(pl.multiple_of(quarter * share + full * WB, PAIR), rest)
        return pltpu.make_async_copy(emb.at[rows], e_tail.at[i], tail_sem.at[i])

    def cache_loads(b):
        slot = b % KVS
        return [pltpu.make_async_copy(k_hbm.at[b], k_buf.at[slot], k_sem.at[slot]),
                pltpu.make_async_copy(v_hbm.at[b], v_buf.at[slot], v_sem.at[slot])]

    def hop_a(j):
        return send(pool.at[pl.ds(TWO * j, TWO), 1 - core], pool.at[TWO * steps + j], a_s.at[j], a_r.at[j], y, partner)

    def sum_at(hf, p):
        return pool.at[3 * steps + hf * (steps // 4) + p // TWO, p % TWO]

    def got_at(hf, p):
        return pool.at[3 * steps + (TWO + hf) * (steps // 4) + p // TWO, p % TWO]

    def hop_b(hf, p):
        return send(sum_at(hf, p), got_at(hf, p), b_s.at[hf, p], b_r.at[hf, p], y, twin)

    def hop_m(hf, g):
        return send(act.at[hf, g, core, chip], act.at[hf, g, core, chip], m_s.at[hf, g], m_r.at[hf, g], y, twin)

    def hop_p(hf, g):
        return send(act.at[hf, g, core], act.at[hf, g, core], p_s.at[hf, g], p_r.at[hf, g], y, partner)

    hop_qa = send(part_q.at[:, 1 - core], ga_q, q_s.at[0], q_r.at[0], y, partner)
    hop_qb = send(sb_q, gb_q, q_s.at[1], q_r.at[1], y, twin)
    hop_qc = send(q_rot.at[1 - y], q_full.at[y], q_s.at[TWO], q_r.at[TWO], 1 - y, xi)

    def hop_o(hf, n):
        if n == 0:
            return send(o_in.at[1 - y, hf], o_all.at[hf, core, chip, y], o_s.at[hf, 0], o_r.at[hf, 0], 1 - y, xi)
        if n == 1:
            return send(o_all.at[hf, core, chip], o_all.at[hf, core, chip], o_s.at[hf, 1], o_r.at[hf, 1], y, twin)
        return send(o_all.at[hf, core], o_all.at[hf, core], o_s.at[hf, TWO], o_r.at[hf, TWO], y, partner)

    def hop_y(hf):
        return send(acc.at[hf, :, 1 - y], y_got.at[hf], y_s.at[hf], y_r.at[hf], 1 - y, xi)

    def hop_f(hf):
        return send(f_all.at[hf, y], f_all.at[hf, y], f_s.at[hf], f_r.at[hf], 1 - y, xi)

    def turns(owner):
        row = lax.broadcasted_iota(jnp.int32, (OWN, hd), 0)
        pos = functools.reduce(lambda acc_, r: jnp.where(row == r, lens[owner * OWN + r], acc_), range(OWN), jnp.zeros((OWN, hd), jnp.int32))
        angle = pos.astype(F32) * freq[...]
        lane = lax.broadcasted_iota(jnp.int32, (OWN, hd), 1)
        return jnp.cos(angle), jnp.where(lane < hd // TWO, -jnp.sin(angle), jnp.sin(angle))

    for y_o in range(TWO):
        cos[y_o], sin[y_o] = turns(y_o * 4 + chip * TWO + core)
    for load in inputs:
        load.wait()
    h = hid[...].astype(F32).reshape(LANES, width)
    mean, rstd = norm_stats(h, stat, y, xi, st_s, st_r, ready, 4)
    normed = ((h - mean) * rstd * gain[...]).astype(BF16)
    for hf in range(TWO):
        for core_o in range(TWO):
            for chip_o in range(TWO):
                for y_o in range(TWO):
                    src = (y_o * 4 + chip_o * TWO + core_o) * OWN + hf * 8
                    dst = hf * HALF + core_o * PAIR + chip_o * OWN + y_o * 8
                    n_perm[dst:dst + 8, :] = normed[src:src + 8, :]

    for s in range(TWO):
        for i, load in enumerate(q_loads(s)):
            load.wait()
            prod = jnp.dot(n_perm[...], ring[s, i], preferred_element_type=F32)
            part_q[:, :, :, :, (TWO * s + i) * FC:(TWO * s + i + 1) * FC] = prod.reshape(TWO, TWO, TWO, OWN, FC)
        start(w_loads(RING - 3 + s))
    for load in kv_w:
        load.wait()
    part_q[..., qc:] = jnp.dot(n_perm[...], w_kv[...], preferred_element_type=F32).reshape(TWO, TWO, TWO, OWN, TWO * hd)
    hop_qa.start()

    def rotate_queries():
        hop_qb.wait_recv()
        both = part_q[:, core, chip] + ga_q[:, chip] + gb_q[...]
        total[...] = both.astype(BF16).astype(F32).reshape(TWO, TWO, 8, qc + TWO * hd)
        for y_o in range(TWO):
            cos_r, sin_r = cos[y_o], sin[y_o]
            for head in range(heads):
                val = total[:, y_o, :, head * hd:(head + 1) * hd].reshape(OWN, hd)
                q_rot[y_o, :, head * hd:(head + 1) * hd] = (val * cos_r + pltpu.roll(val, hd // TWO, 1) * sin_r).astype(BF16)
        hop_qc.start()
        key = total[:, y, :, qc:qc + hd].reshape(OWN, hd)
        value = total[:, y, :, qc + hd:].reshape(OWN, hd)
        key = (key * cos[y] + pltpu.roll(key, hd // TWO, 1) * sin[y]).astype(BF16)
        kv_out[0] = key
        kv_out[1] = value.astype(BF16)
        kn[:, 0, :] = key.astype(F32)
        vn[:, 0, :] = value
        q_full[y] = q_rot[y]

    def spread_queries():
        hop_qc.wait_recv()
        for y_o in range(TWO):
            for head in range(heads):
                q_heads[:, y_o * heads + head, :] = q_full[y_o, :, head * hd:(head + 1) * hd].astype(F32)

    def add_pair(j):
        hop_a(j).wait_recv()
        for hf in range(TWO):
            sum_at(hf, j // TWO)[j % TWO] = pool[TWO * j + hf, core, 1 - chip] + pool[TWO * steps + j, hf, 1 - chip]

        @pl.when(j % TWO == 1)
        def _():
            hop_b(0, j // TWO).start()

    def project(j, carry):
        @pl.when(j + RING - 1 < steps)
        def _():
            start(w_loads(j + RING - 1))

        slot = (j + TWO) % RING
        for i, load in enumerate(w_loads(j)):
            load.wait()
            prod = jnp.dot(n_perm[...], ring[slot, i], preferred_element_type=F32)
            pool[pl.ds(TWO * j, TWO), :, :, :, i * FC:(i + 1) * FC] = prod.reshape(TWO, TWO, TWO, OWN, FC)
        hop_a(j).start()

        @pl.when(j == 0)
        def _():
            hop_qa.wait_recv()
            sb_q[...] = part_q[:, core, 1 - chip] + ga_q[:, 1 - chip]
            hop_qb.start()

        @pl.when(j >= 1)
        def _():
            add_pair(j - 1)

        @pl.when(j == 4)
        def _():
            for b in range(KVS):
                start(cache_loads(b))

        @pl.when(j == 8)
        def _():
            rotate_queries()

        @pl.when(j == 12)
        def _():
            spread_queries()
        return carry

    lax.fori_loop(0, steps, project, 0)
    add_pair(steps - 1)
    for t in range(RING - 1):
        start(block(wd, t * WB, t))
    for i in range(4):
        tail_load(i).start()

    def activate(hf, p):
        hop_b(hf, p).wait_recv()
        for i in range(TWO):
            j = TWO * p + i
            both = pool[TWO * j + hf, core, chip] + pool[TWO * steps + j, hf, chip] + got_at(hf, p)[i]
            gate = both[:, :FC].astype(BF16).astype(F32)
            up_val = both[:, FC:].astype(BF16).astype(F32)
            cols = pl.ds(pl.multiple_of(((p % 4) * TWO + i) * FC, FC), FC)
            act[hf, p // 4, core, chip, :, cols] = (jax.nn.silu(gate) * up_val).astype(BF16)

        @pl.when(p % 4 == 3)
        def _():
            hop_m(hf, p // 4).start()

    part_len = 1024

    def attend(b):
        slot = b % KVS
        scale = hd ** -0.5
        q32 = q_heads[b]
        q = q32.astype(BF16)
        limit = lens[mine * OWN + b]
        s_new = jnp.sum(q32 * kn[b], axis=1, keepdims=True) * scale
        load_k, load_v = cache_loads(b)
        load_k.wait()
        high = None
        for i in range(length // part_len):
            rows = slice(i * part_len, (i + 1) * part_len)
            s = lax.dot_general(q, k_buf[slot, rows], (((1,), (1,)), ((), ())), preferred_element_type=F32) * scale
            pos = lax.broadcasted_iota(jnp.int32, s.shape, 1) + i * part_len
            s = jnp.where(pos < limit, s, -jnp.inf)
            scores[:, rows] = s
            for c in range(0, part_len, LANES):
                high = s[:, c:c + LANES] if high is None else jnp.maximum(high, s[:, c:c + LANES])
        best = jnp.maximum(jnp.max(high, axis=1, keepdims=True), s_new)
        mass = None
        for i in range(length // part_len):
            rows = slice(i * part_len, (i + 1) * part_len)
            e = jnp.exp(scores[:, rows] - best)
            scores[:, rows] = e
            for c in range(0, part_len, LANES):
                mass = e[:, c:c + LANES] if mass is None else mass + e[:, c:c + LANES]
        e_new = jnp.exp(s_new - best)
        inv = 1.0 / (jnp.sum(mass, axis=1, keepdims=True) + e_new)
        for i in range(length // part_len):
            rows = slice(i * part_len, (i + 1) * part_len)
            probs[:, rows] = (scores[:, rows] * inv).astype(BF16)
        load_v.wait()
        o = jnp.dot(probs[...], v_buf[slot], preferred_element_type=F32)
        o = o + (e_new * inv).astype(BF16).astype(F32) * vn[b]
        o_heads[b] = o.astype(BF16).astype(F32)

        @pl.when(b + KVS < seqs)
        def _():
            start(cache_loads(b + KVS))

    def send_heads(hf):
        for y_o in range(TWO):
            for head in range(heads):
                o_in[y_o, hf, :, head * hd:(head + 1) * hd] = o_heads[hf * 8:hf * 8 + 8, y_o * heads + head, :].astype(BF16)
        o_all[hf, core, chip, y] = o_in[y, hf]
        hop_o(hf, 0).start()

    def contract(hf):
        base = hf * (np_ + TWO * full)
        acc[hf] = jnp.zeros(acc.shape[1:], F32)

        def add(t, left):
            slot = take_item(t)
            for i in range(TWO):
                prod = jnp.dot(left, ring[slot, i], preferred_element_type=F32)
                acc[hf, :, :, :, i * hw:(i + 1) * hw] += prod.reshape(4, TWO, 8, hw)

        for g in range(TWO):
            hop_p(hf, g).wait_recv()

            def from_act(i, carry):
                add(base + g * (nd // TWO) + i, act[hf, g, :, :, :, pl.ds(pl.multiple_of(i * WB, WB), WB)].reshape(HALF, WB))
                return carry

            lax.fori_loop(0, nd // TWO, from_act, 0)
        hop_o(hf, TWO).wait_recv()

        def from_heads(i, carry):
            add(base + nd + i, o_all[hf, :, :, :, :, pl.ds(pl.multiple_of(i * WB, WB), WB)].reshape(HALF, WB))
            return carry

        lax.fori_loop(0, no, from_heads, 0)

    def finish_layer(hf, after):
        hop_y(hf).wait_recv()
        res = [hid[y * 4 + (i % TWO) * TWO + i // TWO, hf * 8:hf * 8 + 8].astype(F32) for i in range(4)]
        branch = acc[hf, :, y] + y_got[hf]
        r = jnp.concatenate(res, axis=0) + branch.reshape(PAIR, width)
        mean, rstd = norm_stats(r, stat_f.at[hf], y, xi, sf_s.at[hf], sf_r.at[hf], lambda: None, 4, after)
        f = ((r - mean) * rstd * gain_f[...]).astype(BF16)
        for i in range(4):
            f_all[hf, y, (i % TWO) * TWO + i // TWO] = f[i * 8:(i + 1) * 8]
        hop_f(hf).start()

    def each(body, low, high):
        def step(p, carry):
            body(p)
            return carry

        lax.fori_loop(low, high, step, 0)

    def pass_m(hf):
        for g in range(TWO):
            hop_m(hf, g).wait_recv()
            hop_p(hf, g).start()

    def pass_o(hf, n):
        hop_o(hf, n).wait_recv()
        hop_o(hf, n + 1).start()

    def mix(i):
        pl.when(i == 8)(lambda: send_heads(0))
        attend(i)
        pl.when(i < 8)(lambda: activate(0, i))

        @pl.when(i == 8)
        def _():
            pass_o(0, 0)
            each(lambda p: hop_b(1, p).start(), 0, HELD)

        pl.when(i == 10)(lambda: pass_m(0))
        pl.when(i == 11)(lambda: pass_o(0, 1))

        @pl.when(i == 12)
        def _():
            each(lambda j: hop_a(j).wait_send(), 0, steps)
            each(lambda p: hop_b(0, p).wait_send(), 0, 8)
            contract(0)
            hop_y(0).start()
            each(lambda p: activate(1, p), 0, TWO)

        @pl.when(i == 13)
        def _():
            finish_layer(0, lambda: each(lambda p: hop_b(1, p).start(), HELD, 8))

    each(mix, 0, seqs)
    hop_f(0).wait_recv()
    send_heads(1)
    each(lambda p: activate(1, p), TWO, 4)

    def out_at(hf, k):
        return 56 - hf * 6 + k

    def in_at(hf, k):
        return PAIR + k if hf else 20 + TWO * k

    def lhop_a(hf, k):
        return send(pool.at[k], pool.at[8 + TWO * k], la_s.at[hf, k], la_r.at[hf, k], y, partner)

    def lhop_b(hf, k):
        return send(pool.at[out_at(hf, k)], pool.at[in_at(hf, k)], lb_s.at[hf, k], lb_r.at[hf, k], y, twin)

    def lhop_c(k):
        return send(pool.at[pl.ds(6 + TWO * k, TWO)], pool.at[pl.ds(38 + TWO * k, TWO)], lc_s.at[k], lc_r.at[k], y, partner)

    def thop_a(hf):
        return send(t_a.at[hf], tg_a.at[hf], ta_s.at[hf], ta_r.at[hf], y, partner)

    def thop_b(hf):
        return send(t_b.at[hf], tg_b.at[hf], tb_s.at[hf], tb_r.at[hf], y, twin)

    thop_c = send(t_c, tg_c, tc_s.at[0], tc_r.at[0], y, partner)
    nt = (((1,), (1,)), ((), ()))

    def product(left, slot, n):
        rows = slice(n * hw, (n + 1) * hw)
        return (lax.dot_general(left[:, :hw], ring[slot, 0, rows], nt, preferred_element_type=F32)
                + lax.dot_general(left[:, hw:], ring[slot, 1, rows], nt, preferred_element_type=F32))

    def tail_product(left, i):
        return lax.dot_general(left, e_tail[i], nt, preferred_element_type=F32)

    t_a[...] = jnp.zeros_like(t_a)
    t_b[...] = jnp.zeros_like(t_b)
    t_c[...] = jnp.zeros_like(t_c)

    def outward(hf):
        def chunk(k):
            left = f_all[hf].reshape(HALF, width)
            if hf == 1:
                lhop_a(0, k).wait_send()
            slot = take_item(e_base[hf] + TWO * k)
            for n in range(TWO):
                pool[k, :, :, :, n * hw:(n + 1) * hw] = product(left, slot, n).reshape(TWO, TWO, OWN, hw)
            lhop_a(hf, k).start()
            slot = take_item(e_base[hf] + TWO * k + 1)
            for n in range(TWO):
                pool[out_at(hf, k), :, :, :, n * hw:(n + 1) * hw] = product(left, slot, n).reshape(TWO, TWO, OWN, hw)
            lhop_a(hf, k).wait_recv()
            pool[out_at(hf, k)] += pool[8 + TWO * k]
            if hf == 0:
                pl.when(k < full - TWO)(lambda: lhop_b(0, k).start())

                @pl.when(k == 0)
                def _():
                    each(lambda p: activate(1, p), 4, 8)
                    pass_o(1, 0)
            else:
                lhop_b(1, k).start()

        each(chunk, 0, full)
        left = f_all[hf].reshape(HALF, width)
        if hf == 0:
            tail_load(0).wait()
            tail_load(1).wait()
        t_a[hf, :, :rest] = tail_product(left, 0)
        thop_a(hf).start()
        t_b[hf, :, :rest] = tail_product(left, 1)
        thop_a(hf).wait_recv()
        t_b[hf] += tg_a[hf]
        if hf == 1:
            thop_b(1).start()

    def release():
        each(lambda k: lhop_b(0, k).start(), full - TWO, full)
        thop_b(0).start()

    outward(0)
    pass_m(1)
    pass_o(1, 1)
    each(lambda p: hop_b(1, p).wait_send(), 0, 8)
    contract(1)
    hop_y(1).start()
    finish_layer(1, release)
    hop_f(1).wait_recv()
    outward(1)

    for g in range(8):
        for hf in range(TWO):
            f_nat[g * OWN + hf * 8:g * OWN + hf * 8 + 8, :] = f_all[hf, g // 4, g % 4]

    def inward(k, carry):
        slot = take_item(c_base + k)
        for n in range(TWO):
            pool[pl.ds(6 + TWO * k, TWO), :, :, :, n * hw:(n + 1) * hw] = product(f_nat[...], slot, n).reshape(TWO, TWO, TWO, OWN, hw)
        lhop_c(k).start()
        return carry

    lax.fori_loop(0, full, inward, 0)
    tail_load(TWO).wait()
    t_c[:, :rest] = tail_product(f_nat[...], TWO)
    thop_c.start()
    tail_load(3).wait()

    top[...] = jnp.full_like(top, LOW)
    mass_l[...] = jnp.zeros_like(mass_l)

    def fold(z):
        tiles = [z[:, i:i + LANES] for i in range(0, z.shape[1], LANES)]
        high = functools.reduce(jnp.maximum, tiles, top[...])
        mass_l[...] = mass_l[...] * jnp.exp(top[...] - high) + sum(jnp.exp(g - high) for g in tiles)
        top[...] = high

    def weave(first, second):
        n = first.shape[-1]
        return jnp.stack([first.reshape(8, 8, n), second.reshape(8, 8, n)], axis=1).reshape(LANES, n)

    def finish(k, carry):
        slot = take_item(d_base + k)
        lhop_c(k).wait_recv()
        lhop_b(0, k).wait_recv()
        lhop_b(1, k).wait_recv()
        for n in range(TWO):
            cols = slice(n * hw, (n + 1) * hw)
            z = product(f_nat[...], slot, n) + pool[pl.ds(38 + TWO * k, TWO), :, :, :, cols].reshape(LANES, hw)
            z = z + weave(pool[in_at(0, k), :, :, :, cols], pool[in_at(1, k), :, :, :, cols])
            z_out[pl.ds(pl.multiple_of(k * WB + n * hw, hw), hw), :] = z.T
            fold(z)
        return carry

    lax.fori_loop(0, full, finish, 0)
    thop_c.wait_recv()
    thop_b(0).wait_recv()
    thop_b(1).wait_recv()
    z_tail = tg_c[...] + weave(tg_b[0], tg_b[1])
    own = tail_product(f_nat[...], 3)
    z_tail = z_tail + jnp.concatenate([own, jnp.zeros((LANES, z_tail.shape[1] - rest), F32)], axis=1)
    z_out[full * WB:, :] = z_tail.T[:rest]
    lane = lax.broadcasted_iota(jnp.int32, z_tail.shape, 1)
    fold(jnp.where(lane < rest, z_tail, LOW))

    high = jnp.max(top[...], axis=1, keepdims=True)
    stat_z[mine] = to_lanes(high, jnp.sum(mass_l[...] * jnp.exp(top[...] - high), axis=1, keepdims=True))
    copies = []
    for dy in range(TWO):
        for d in range(4):
            if dy or d:
                i = dy * 4 + d - 1
                copies.append(send(stat_z.at[mine], stat_z.at[mine], sz_s.at[i], sz_r.at[i],
                                   y + dy * (1 - TWO * y), (xi + d) % 4))
    start(copies)
    for copy in copies:
        copy.wait()
    highs = [stat_z[i][0:1] for i in range(8)]
    best_all = functools.reduce(jnp.maximum, highs)
    lse_out[...] = best_all + jnp.log(sum(stat_z[i][1:TWO] * jnp.exp(highs[i] - best_all) for i in range(8)))

    def drain_logits(k, carry):
        lhop_a(1, k).wait_send()
        lhop_b(0, k).wait_send()
        lhop_b(1, k).wait_send()
        lhop_c(k).wait_send()
        return carry

    lax.fori_loop(0, full, drain_logits, 0)
    for hf in range(TWO):
        for g in range(TWO):
            hop_m(hf, g).wait_send()
            hop_p(hf, g).wait_send()
        for n in range(3):
            hop_o(hf, n).wait_send()
        for hop in (hop_y, hop_f, thop_a, thop_b):
            hop(hf).wait_send()
    for hop in (hop_qa, hop_qb, hop_qc, thop_c):
        hop.wait_send()


def step_call(lens, hid, gain, gain_f, freq, wq, wk, wv, wg, wu, wo, wd, emb, k_cache, v_cache):
    width = hid.shape[TWO]
    qc, hd = wq.shape[1], wk.shape[1]
    seqs, length, _ = k_cache.shape
    cols = qc + TWO * hd
    steps = wg.shape[1] // FC
    heads = TWO * qc // hd
    share = emb.shape[0] // QUAD
    full = share // WB
    rest = share - full * WB
    tail_w = -(-rest // LANES) * LANES
    vmem = pl.BlockSpec(memory_space=pltpu.VMEM)
    hbm = pl.BlockSpec(memory_space=pl.ANY)

    def f32(*shape):
        return pltpu.VMEM(shape, F32)

    def bf16(*shape):
        return pltpu.VMEM(shape, BF16)

    def dma(*shape):
        return pltpu.SemaphoreType.DMA(shape)

    return pl.pallas_call(
        step_kernel, name="step",
        out_shape=[jax.ShapeDtypeStruct((TWO, OWN, hd), BF16), jax.ShapeDtypeStruct((share, LANES), F32),
                   jax.ShapeDtypeStruct((1, LANES), F32)],
        in_specs=[pl.BlockSpec(memory_space=pltpu.SMEM)] + [hbm] * 3 + [vmem] + [hbm] * 10, out_specs=[vmem] * 3,
        scratch_shapes=[
            bf16(OCT, OWN, width), f32(1, width), f32(1, width), f32(TWO, OWN, hd), f32(TWO, OWN, hd),
            bf16(LANES, width), bf16(RING, TWO, width, FC), bf16(width, TWO * hd),
            f32(TWO, TWO, TWO, OWN, cols), f32(TWO, TWO, OWN, cols), f32(TWO, OWN, cols), f32(TWO, OWN, cols), f32(TWO, TWO, OCT, cols),
            bf16(TWO, OWN, qc), bf16(TWO, OWN, qc), f32(seqs, heads, hd), f32(seqs, heads, hd), f32(seqs, 1, hd), f32(seqs, 1, hd),
            f32(QUAD * steps, TWO, TWO, OWN, TWO * FC), bf16(TWO, TWO, TWO, TWO, OWN, steps // TWO * FC),
            bf16(TWO, TWO, OCT, qc), bf16(TWO, TWO, TWO, TWO, OCT, qc),
            bf16(KVS, length, hd), bf16(KVS, length, hd), f32(heads, length), bf16(heads, length),
            f32(TWO, QUAD, TWO, OCT, width), f32(TWO, QUAD, OCT, width), bf16(TWO, TWO, QUAD, OCT, width), bf16(LANES, width), bf16(QUAD, rest, width),
            f32(TWO, HALF, tail_w), f32(TWO, HALF, tail_w), f32(TWO, HALF, tail_w), f32(TWO, HALF, tail_w), f32(LANES, tail_w), f32(LANES, tail_w),
            f32(LANES, LANES), f32(LANES, LANES), f32(QUAD, OCT, LANES), f32(TWO, QUAD, OCT, LANES), f32(OCT, OCT, LANES),
            dma(3), dma(RING, TWO), dma(TWO), dma(QUAD), dma(KVS), dma(KVS), dma(steps), dma(steps), dma(TWO, steps // TWO), dma(TWO, steps // TWO),
            dma(TWO, TWO), dma(TWO, TWO), dma(TWO, TWO), dma(TWO, TWO), dma(3), dma(3),
            dma(TWO, 3), dma(TWO, 3), dma(TWO), dma(TWO), dma(TWO), dma(TWO), dma(3), dma(3), dma(TWO, 3), dma(TWO, 3),
            dma(TWO, full), dma(TWO, full), dma(TWO, full), dma(TWO, full), dma(full), dma(full),
            dma(TWO), dma(TWO), dma(TWO), dma(TWO), dma(1), dma(1), dma(7), dma(7)],
        compiler_params=pltpu.CompilerParams(collective_id=0, has_side_effects=True, vmem_limit_bytes=63 * TWO**20),
    )(lens, hid, gain, gain_f, freq, wq, wk, wv, wg, wu, wo, wd, emb, k_cache, v_cache)


def solution(mesh):
    row_spec = P(("dp", "yax", "xax"))

    def local_step(hidden, cache_len, k_cache, v_cache, g_attn, w_query, w_key, w_value,
                   w_gate, w_up, w_out, w_down, g_final, embedding):
        width = hidden.shape[1]
        own_rows, _, head_dim = k_cache.shape
        half = head_dim // TWO
        lane = jnp.arange(head_dim)
        inv_freq = ROPE_BASE ** (-((lane % half).astype(F32) * 2.0) / head_dim)
        kv_new, logits_t, log_norm = step_call(
            cache_len, hidden.reshape(8, own_rows, width), g_attn[None], g_final[None], inv_freq[None],
            w_query, w_key, w_value, w_gate, w_up, w_out, w_down, embedding, k_cache, v_cache)
        return kv_new[0], kv_new[1], (logits_t - log_norm).T, log_norm[0]

    in_specs = (P("dp", "xax"), P("dp"), row_spec, row_spec, P("xax"), P("xax", "yax"),
                P("xax", None), P("xax", None), P("xax", "yax"), P("xax", "yax"),
                P("yax", "xax"), P("yax", "xax"), P("xax"), P("yax", "xax"))
    out_specs = (row_spec, row_spec, P("dp", ("yax", "xax")), P("dp"))
    return jax.shard_map(local_step, mesh=mesh, in_specs=in_specs, out_specs=out_specs, check_vma=False)
```

```python
import functools

import jax
import jax.numpy as jnp
from jax import lax
from jax.experimental import pallas as pl
from jax.experimental.pallas import tpu as pltpu
from jax.sharding import PartitionSpec as P

EPS = 1e-6
ROPE_BASE = 10000.0
MESH = pl.DeviceIdType.MESH
F32 = jnp.float32
BF16 = jnp.bfloat16
LOW = -3e38
TWO, QUAD, OCT, OWN, PAIR, HALF, LANES = 2, 4, 8, 16, 32, 64, 128


def place():
    y = lax.axis_index("yax")
    xi = lax.axis_index("xax")
    chip = xi // 2
    core = xi % 2
    return y, xi, chip, core, chip * 2 + (1 - core), (1 - chip) * 2 + core


def send(src, dst, send_sem, recv_sem, y, xi):
    return pltpu.make_async_remote_copy(src_ref=src, dst_ref=dst, send_sem=send_sem, recv_sem=recv_sem,
                                        device_id={"yax": y, "xax": xi}, device_id_type=MESH)


def enter(peers):
    barrier = pltpu.get_barrier_semaphore()
    for y, xi in peers:
        pl.semaphore_signal(barrier, inc=1, device_id={"yax": y, "xax": xi}, device_id_type=MESH)
    return lambda: pl.semaphore_wait(barrier, len(peers))


def to_lanes(first, second):
    rows = first.shape[0]
    lane = lax.broadcasted_iota(jnp.int32, (rows, 128), 1)
    tile = jnp.where(lane == 0, first, jnp.where(lane == 1, second, 0.0))
    if rows < 128:
        tile = jnp.concatenate([tile, jnp.zeros((128 - rows, 128), F32)], axis=0)
    return tile.T[:8]


def to_columns(first, second):
    row = lax.broadcasted_iota(jnp.int32, (128, 128), 0)
    tile = jnp.where(row == 0, first, jnp.where(row == 1, second, 0.0)).T
    return tile[:, 0:1], tile[:, 1:2]


def norm_stats(values, stat, y, xi, send_sems, recv_sems, ready, size, after=lambda: None):
    rows, width = values.shape
    mean_own = jnp.sum(values, axis=1, keepdims=True) / width
    diff = values - mean_own
    stat[xi] = to_lanes(mean_own, jnp.sum(diff * diff, axis=1, keepdims=True))
    ready()
    copies = [send(stat.at[xi], stat.at[xi], send_sems.at[d - 1], recv_sems.at[d - 1], y, (xi + d) % size)
              for d in range(1, size)]
    for copy in copies:
        copy.start()
    after()
    for copy in copies:
        copy.wait()
    tiles = [stat[i] for i in range(size)]
    mean_all = sum(t[0:1] for t in tiles) / size
    spread = sum(t[1:TWO] for t in tiles) + width * sum((t[0:1] - mean_all) * (t[0:1] - mean_all) for t in tiles)
    mean_col, rstd_col = to_columns(mean_all, lax.rsqrt(spread / (width * size) + EPS))
    return mean_col[:rows], rstd_col[:rows]


FC = 512
WB = 1024
RING = 6
KVS = 3
HELD = 6


def step_kernel(lens, hid_h, gain_h, gain_fh, freq, wq, wk, wv, wg, wu, wo, wd, emb, k_hbm, v_hbm,
                kv_out, z_out, lse_out, kv_v, z_v,
                hid, gain, gain_f, cos, sin, n_perm, ring, w_kv, part_q, ga_q, sb_q, gb_q, total, q_rot, q_full, q_heads, o_heads, kn, vn,
                pool, act, o_in, o_all, k_buf, v_buf, scores, probs, acc, y_got, f_all, f_nat, e_tail,
                t_a, t_b, tg_a, tg_b, t_c, tg_c, top, mass_l, stat, stat_f, stat_z,
                i_sem, z_sem, r_sem, kv_sem, tail_sem, k_sem, v_sem, a_s, a_r, b_s, b_r, m_s, m_r, p_s, p_r, q_s, q_r,
                o_s, o_r, y_s, y_r, f_s, f_r, st_s, st_r, sf_s, sf_r,
                la_s, la_r, lb_s, lb_r, lc_s, lc_r, ta_s, ta_r, tb_s, tb_r, tc_s, tc_r, sz_s, sz_r):
    y, xi, chip, core, partner, twin = place()
    width = n_perm.shape[1]
    hw = width // TWO
    qc, hd = wq.shape[1], wk.shape[1]
    heads = qc // hd
    steps = wg.shape[1] // FC
    seqs = q_heads.shape[0]
    length = k_buf.shape[1]
    share = emb.shape[0] // 4
    full = share // WB
    rest = share - full * WB
    mine = y * 4 + xi
    ready = enter([(y, (xi + d) % 4) for d in (1, TWO, 3)] + [(1 - y, (xi + d) % 4) for d in range(4)])

    def start(copies):
        for copy in copies:
            copy.start()

    def q_loads(s):
        return [pltpu.make_async_copy(wq.at[:, pl.ds((TWO * s + i) * FC, FC)], ring.at[s, i], r_sem.at[s, i]) for i in range(TWO)]

    def w_loads(j):
        cols = pl.ds(pl.multiple_of(j * FC, FC), FC)
        slot = (j + TWO) % RING
        return [pltpu.make_async_copy(w.at[:, cols], ring.at[slot, i], r_sem.at[slot, i]) for i, w in enumerate((wg, wu))]

    inputs = [pltpu.make_async_copy(src, dst, i_sem.at[i])
              for i, (src, dst) in enumerate(((hid_h, hid), (gain_h, gain), (gain_fh, gain_f)))]
    start(inputs)
    kv_w = [pltpu.make_async_copy(w, w_kv.at[:, pl.ds(i * hd, hd)], kv_sem.at[i]) for i, w in enumerate((wk, wv))]
    start(q_loads(0))
    start(q_loads(1))
    start(kv_w)
    for j in range(RING - 3):
        start(w_loads(j))

    nd, no = wd.shape[0] // WB, wo.shape[0] // WB
    np_ = nd + no
    e_base = (np_, TWO * np_ + TWO * full)
    c_base = TWO * np_ + 4 * full
    d_base = c_base + full
    items = d_base + full
    far, near = (1 - chip) * TWO, chip * TWO

    def block(src, row, t):
        slot = t % RING
        return [pltpu.make_async_copy(src.at[pl.ds(row, WB), pl.ds(i * hw, hw)], ring.at[slot, i], r_sem.at[slot, i])
                for i in range(TWO)]

    def emb_row(quarter, k):
        return pl.multiple_of(quarter * share + k * WB, PAIR)

    def load_item(t):
        for base in (0, np_ + TWO * full):
            @pl.when((t >= base) & (t < base + nd))
            def _(base=base):
                start(block(wd, pl.multiple_of((t - base) * WB, WB), t))

            @pl.when((t >= base + nd) & (t < base + np_))
            def _(base=base):
                start(block(wo, pl.multiple_of((t - base - nd) * WB, WB), t))

        for base in e_base:
            @pl.when((t >= base) & (t < base + TWO * full))
            def _(base=base):
                k, own = (t - base) // TWO, (t - base) % TWO
                start(block(emb, emb_row(far + (1 - core) + own * (TWO * core - 1), k), t))

        @pl.when((t >= c_base) & (t < d_base))
        def _():
            start(block(emb, emb_row(near + 1 - core, t - c_base), t))

        @pl.when((t >= d_base) & (t < items))
        def _():
            start(block(emb, emb_row(near + core, t - d_base), t))

    def take_item(t):
        load_item(t + RING - 1)
        for copy in block(wd, 0, t):
            copy.wait()
        return t % RING

    def tail_load(i):
        quarter = (far + 1 - core, far + core, near + 1 - core, near + core)[i]
        rows = pl.ds(pl.multiple_of(quarter * share + full * WB, PAIR), rest)
        return pltpu.make_async_copy(emb.at[rows], e_tail.at[i], tail_sem.at[i])

    def cache_loads(b):
        slot = b % KVS
        return [pltpu.make_async_copy(k_hbm.at[b], k_buf.at[slot], k_sem.at[slot]),
                pltpu.make_async_copy(v_hbm.at[b], v_buf.at[slot], v_sem.at[slot])]

    def hop_a(j):
        return send(pool.at[pl.ds(TWO * j, TWO), 1 - core], pool.at[TWO * steps + j], a_s.at[j], a_r.at[j], y, partner)

    def sum_at(hf, p):
        return pool.at[3 * steps + hf * (steps // 4) + p // TWO, p % TWO]

    def got_at(hf, p):
        return pool.at[3 * steps + (TWO + hf) * (steps // 4) + p // TWO, p % TWO]

    def hop_b(hf, p):
        return send(sum_at(hf, p), got_at(hf, p), b_s.at[hf, p], b_r.at[hf, p], y, twin)

    def hop_m(hf, g):
        return send(act.at[hf, g, core, chip], act.at[hf, g, core, chip], m_s.at[hf, g], m_r.at[hf, g], y, twin)

    def hop_p(hf, g):
        return send(act.at[hf, g, core], act.at[hf, g, core], p_s.at[hf, g], p_r.at[hf, g], y, partner)

    hop_qa = send(part_q.at[:, 1 - core], ga_q, q_s.at[0], q_r.at[0], y, partner)
    hop_qb = send(sb_q, gb_q, q_s.at[1], q_r.at[1], y, twin)
    hop_qc = send(q_rot.at[1 - y], q_full.at[y], q_s.at[TWO], q_r.at[TWO], 1 - y, xi)

    def hop_o(hf, n):
        if n == 0:
            return send(o_in.at[1 - y, hf], o_all.at[hf, core, chip, y], o_s.at[hf, 0], o_r.at[hf, 0], 1 - y, xi)
        if n == 1:
            return send(o_all.at[hf, core, chip], o_all.at[hf, core, chip], o_s.at[hf, 1], o_r.at[hf, 1], y, twin)
        return send(o_all.at[hf, core], o_all.at[hf, core], o_s.at[hf, TWO], o_r.at[hf, TWO], y, partner)

    def hop_y(hf):
        return send(acc.at[hf, :, 1 - y], y_got.at[hf], y_s.at[hf], y_r.at[hf], 1 - y, xi)

    def hop_f(hf):
        return send(f_all.at[hf, y], f_all.at[hf, y], f_s.at[hf], f_r.at[hf], 1 - y, xi)

    def turns(owner):
        row = lax.broadcasted_iota(jnp.int32, (OWN, hd), 0)
        pos = functools.reduce(lambda acc_, r: jnp.where(row == r, lens[owner * OWN + r], acc_), range(OWN), jnp.zeros((OWN, hd), jnp.int32))
        angle = pos.astype(F32) * freq[...]
        lane = lax.broadcasted_iota(jnp.int32, (OWN, hd), 1)
        return jnp.cos(angle), jnp.where(lane < hd // TWO, -jnp.sin(angle), jnp.sin(angle))

    for load in inputs:
        load.wait()
    h = hid[...].astype(F32).reshape(LANES, width)
    mean, rstd = norm_stats(h, stat, y, xi, st_s, st_r, ready, 4)
    normed = ((h - mean) * rstd * gain[...]).astype(BF16)
    for hf in range(TWO):
        for core_o in range(TWO):
            for chip_o in range(TWO):
                for y_o in range(TWO):
                    src = (y_o * 4 + chip_o * TWO + core_o) * OWN + hf * 8
                    dst = hf * HALF + core_o * PAIR + chip_o * OWN + y_o * 8
                    n_perm[dst:dst + 8, :] = normed[src:src + 8, :]

    for s in range(TWO):
        for i, load in enumerate(q_loads(s)):
            load.wait()
            prod = jnp.dot(n_perm[...], ring[s, i], preferred_element_type=F32)
            part_q[:, :, :, :, (TWO * s + i) * FC:(TWO * s + i + 1) * FC] = prod.reshape(TWO, TWO, TWO, OWN, FC)
        start(w_loads(RING - 3 + s))
    for load in kv_w:
        load.wait()
    part_q[..., qc:] = jnp.dot(n_perm[...], w_kv[...], preferred_element_type=F32).reshape(TWO, TWO, TWO, OWN, TWO * hd)
    hop_qa.start()

    kv_store = pltpu.make_async_copy(kv_v, kv_out, z_sem.at[full + 1])

    def z_store(k, size):
        rows = pl.ds(pl.multiple_of(k * WB, 8), size)
        return pltpu.make_async_copy(z_v.at[rows], z_out.at[rows], z_sem.at[k])

    def rotate_queries():
        hop_qb.wait_recv()
        both = part_q[:, core, chip] + ga_q[:, chip] + gb_q[...]
        total[...] = both.astype(BF16).astype(F32).reshape(TWO, TWO, 8, qc + TWO * hd)
        for y_o in range(TWO):
            cos_r, sin_r = cos[y_o], sin[y_o]
            for head in range(heads):
                val = total[:, y_o, :, head * hd:(head + 1) * hd].reshape(OWN, hd)
                q_rot[y_o, :, head * hd:(head + 1) * hd] = (val * cos_r + pltpu.roll(val, hd // TWO, 1) * sin_r).astype(BF16)
        hop_qc.start()
        key = total[:, y, :, qc:qc + hd].reshape(OWN, hd)
        value = total[:, y, :, qc + hd:].reshape(OWN, hd)
        key = (key * cos[y] + pltpu.roll(key, hd // TWO, 1) * sin[y]).astype(BF16)
        kv_v[0] = key
        kv_v[1] = value.astype(BF16)
        kv_store.start()
        kn[:, 0, :] = key.astype(F32)
        vn[:, 0, :] = value
        q_full[y] = q_rot[y]

    def spread_queries():
        hop_qc.wait_recv()
        for y_o in range(TWO):
            for head in range(heads):
                q_heads[:, y_o * heads + head, :] = q_full[y_o, :, head * hd:(head + 1) * hd].astype(F32)

    def add_pair(j):
        hop_a(j).wait_recv()
        for hf in range(TWO):
            sum_at(hf, j // TWO)[j % TWO] = pool[TWO * j + hf, core, 1 - chip] + pool[TWO * steps + j, hf, 1 - chip]

        @pl.when(j % TWO == 1)
        def _():
            hop_b(0, j // TWO).start()

    def project(j, carry):
        @pl.when(j + RING - 1 < steps)
        def _():
            start(w_loads(j + RING - 1))

        slot = (j + TWO) % RING
        for i, load in enumerate(w_loads(j)):
            load.wait()
            prod = jnp.dot(n_perm[...], ring[slot, i], preferred_element_type=F32)
            pool[pl.ds(TWO * j, TWO), :, :, :, i * FC:(i + 1) * FC] = prod.reshape(TWO, TWO, TWO, OWN, FC)
        hop_a(j).start()

        @pl.when(j == 0)
        def _():
            hop_qa.wait_recv()
            sb_q[...] = part_q[:, core, 1 - chip] + ga_q[:, 1 - chip]
            hop_qb.start()

        @pl.when(j >= 1)
        def _():
            add_pair(j - 1)

        @pl.when((j == TWO) | (j == 3))
        def _():
            cos[j - TWO], sin[j - TWO] = turns((j - TWO) * 4 + chip * TWO + core)

        @pl.when(j == 4)
        def _():
            for b in range(KVS):
                start(cache_loads(b))

        @pl.when(j == 8)
        def _():
            rotate_queries()

        @pl.when(j == 12)
        def _():
            spread_queries()
        return carry

    lax.fori_loop(0, steps, project, 0)
    add_pair(steps - 1)
    for t in range(RING - 1):
        start(block(wd, t * WB, t))
    for i in range(4):
        tail_load(i).start()

    def activate(hf, p):
        hop_b(hf, p).wait_recv()
        for i in range(TWO):
            j = TWO * p + i
            both = pool[TWO * j + hf, core, chip] + pool[TWO * steps + j, hf, chip] + got_at(hf, p)[i]
            gate = both[:, :FC].astype(BF16).astype(F32)
            up_val = both[:, FC:].astype(BF16).astype(F32)
            cols = pl.ds(pl.multiple_of(((p % 4) * TWO + i) * FC, FC), FC)
            act[hf, p // 4, core, chip, :, cols] = (jax.nn.silu(gate) * up_val).astype(BF16)

        @pl.when(p % 4 == 3)
        def _():
            hop_m(hf, p // 4).start()

    part_len = 1024

    def attend(b):
        slot = b % KVS
        scale = hd ** -0.5
        q32 = q_heads[b]
        q = q32.astype(BF16)
        limit = lens[mine * OWN + b]
        s_new = jnp.sum(q32 * kn[b], axis=1, keepdims=True) * scale
        load_k, load_v = cache_loads(b)
        load_k.wait()
        high = None
        for i in range(length // part_len):
            rows = slice(i * part_len, (i + 1) * part_len)
            s = lax.dot_general(q, k_buf[slot, rows], (((1,), (1,)), ((), ())), preferred_element_type=F32) * scale
            pos = lax.broadcasted_iota(jnp.int32, s.shape, 1) + i * part_len
            s = jnp.where(pos < limit, s, -jnp.inf)
            scores[:, rows] = s
            for c in range(0, part_len, LANES):
                high = s[:, c:c + LANES] if high is None else jnp.maximum(high, s[:, c:c + LANES])
        best = jnp.maximum(jnp.max(high, axis=1, keepdims=True), s_new)
        mass = None
        for i in range(length // part_len):
            rows = slice(i * part_len, (i + 1) * part_len)
            e = jnp.exp(scores[:, rows] - best)
            scores[:, rows] = e
            for c in range(0, part_len, LANES):
                mass = e[:, c:c + LANES] if mass is None else mass + e[:, c:c + LANES]
        e_new = jnp.exp(s_new - best)
        inv = 1.0 / (jnp.sum(mass, axis=1, keepdims=True) + e_new)
        for i in range(length // part_len):
            rows = slice(i * part_len, (i + 1) * part_len)
            probs[:, rows] = (scores[:, rows] * inv).astype(BF16)
        load_v.wait()
        o = jnp.dot(probs[...], v_buf[slot], preferred_element_type=F32)
        o = o + (e_new * inv).astype(BF16).astype(F32) * vn[b]
        o_heads[b] = o.astype(BF16).astype(F32)

        @pl.when(b + KVS < seqs)
        def _():
            start(cache_loads(b + KVS))

    def send_heads(hf):
        for y_o in range(TWO):
            for head in range(heads):
                o_in[y_o, hf, :, head * hd:(head + 1) * hd] = o_heads[hf * 8:hf * 8 + 8, y_o * heads + head, :].astype(BF16)
        o_all[hf, core, chip, y] = o_in[y, hf]
        hop_o(hf, 0).start()

    def contract(hf):
        base = hf * (np_ + TWO * full)
        acc[hf] = jnp.zeros(acc.shape[1:], F32)

        def add(t, left):
            slot = take_item(t)
            for i in range(TWO):
                prod = jnp.dot(left, ring[slot, i], preferred_element_type=F32)
                acc[hf, :, :, :, i * hw:(i + 1) * hw] += prod.reshape(4, TWO, 8, hw)

        for g in range(TWO):
            hop_p(hf, g).wait_recv()

            def from_act(i, carry):
                add(base + g * (nd // TWO) + i, act[hf, g, :, :, :, pl.ds(pl.multiple_of(i * WB, WB), WB)].reshape(HALF, WB))
                return carry

            lax.fori_loop(0, nd // TWO, from_act, 0)
        hop_o(hf, TWO).wait_recv()

        def from_heads(i, carry):
            add(base + nd + i, o_all[hf, :, :, :, :, pl.ds(pl.multiple_of(i * WB, WB), WB)].reshape(HALF, WB))
            return carry

        lax.fori_loop(0, no, from_heads, 0)

    def finish_layer(hf, after):
        hop_y(hf).wait_recv()
        res = [hid[y * 4 + (i % TWO) * TWO + i // TWO, hf * 8:hf * 8 + 8].astype(F32) for i in range(4)]
        branch = acc[hf, :, y] + y_got[hf]
        r = jnp.concatenate(res, axis=0) + branch.reshape(PAIR, width)
        mean, rstd = norm_stats(r, stat_f.at[hf], y, xi, sf_s.at[hf], sf_r.at[hf], lambda: None, 4, after)
        f = ((r - mean) * rstd * gain_f[...]).astype(BF16)
        for i in range(4):
            f_all[hf, y, (i % TWO) * TWO + i // TWO] = f[i * 8:(i + 1) * 8]
        hop_f(hf).start()

    def each(body, low, high):
        def step(p, carry):
            body(p)
            return carry

        lax.fori_loop(low, high, step, 0)

    def pass_m(hf):
        for g in range(TWO):
            hop_m(hf, g).wait_recv()
            hop_p(hf, g).start()

    def pass_o(hf, n):
        hop_o(hf, n).wait_recv()
        hop_o(hf, n + 1).start()

    def mix(i):
        pl.when(i == 8)(lambda: send_heads(0))
        attend(i)
        pl.when(i < 8)(lambda: activate(0, i))

        @pl.when(i == 8)
        def _():
            pass_o(0, 0)
            each(lambda p: hop_b(1, p).start(), 0, HELD)

        pl.when(i == 10)(lambda: pass_m(0))
        pl.when(i == 11)(lambda: pass_o(0, 1))

        @pl.when(i == 12)
        def _():
            each(lambda j: hop_a(j).wait_send(), 0, steps)
            each(lambda p: hop_b(0, p).wait_send(), 0, 8)
            contract(0)
            hop_y(0).start()
            each(lambda p: activate(1, p), 0, TWO)

        @pl.when(i == 13)
        def _():
            finish_layer(0, lambda: each(lambda p: hop_b(1, p).start(), HELD, 8))

    each(mix, 0, seqs)
    hop_f(0).wait_recv()
    send_heads(1)
    each(lambda p: activate(1, p), TWO, 4)

    def out_at(hf, k):
        return 56 - hf * 6 + k

    def in_at(hf, k):
        return PAIR + k if hf else 20 + TWO * k

    def lhop_a(hf, k):
        return send(pool.at[k], pool.at[8 + TWO * k], la_s.at[hf, k], la_r.at[hf, k], y, partner)

    def lhop_b(hf, k):
        return send(pool.at[out_at(hf, k)], pool.at[in_at(hf, k)], lb_s.at[hf, k], lb_r.at[hf, k], y, twin)

    def lhop_c(k):
        return send(pool.at[pl.ds(6 + TWO * k, TWO)], pool.at[pl.ds(38 + TWO * k, TWO)], lc_s.at[k], lc_r.at[k], y, partner)

    def thop_a(hf):
        return send(t_a.at[hf], tg_a.at[hf], ta_s.at[hf], ta_r.at[hf], y, partner)

    def thop_b(hf):
        return send(t_b.at[hf], tg_b.at[hf], tb_s.at[hf], tb_r.at[hf], y, twin)

    thop_c = send(t_c, tg_c, tc_s.at[0], tc_r.at[0], y, partner)
    nt = (((1,), (1,)), ((), ()))

    def product(left, slot, n):
        rows = slice(n * hw, (n + 1) * hw)
        return (lax.dot_general(left[:, :hw], ring[slot, 0, rows], nt, preferred_element_type=F32)
                + lax.dot_general(left[:, hw:], ring[slot, 1, rows], nt, preferred_element_type=F32))

    def tail_product(left, i):
        return lax.dot_general(left, e_tail[i], nt, preferred_element_type=F32)

    t_a[...] = jnp.zeros_like(t_a)
    t_b[...] = jnp.zeros_like(t_b)
    t_c[...] = jnp.zeros_like(t_c)

    def outward(hf):
        def chunk(k):
            left = f_all[hf].reshape(HALF, width)
            if hf == 1:
                lhop_a(0, k).wait_send()
            slot = take_item(e_base[hf] + TWO * k)
            for n in range(TWO):
                pool[k, :, :, :, n * hw:(n + 1) * hw] = product(left, slot, n).reshape(TWO, TWO, OWN, hw)
            lhop_a(hf, k).start()
            slot = take_item(e_base[hf] + TWO * k + 1)
            for n in range(TWO):
                pool[out_at(hf, k), :, :, :, n * hw:(n + 1) * hw] = product(left, slot, n).reshape(TWO, TWO, OWN, hw)
            lhop_a(hf, k).wait_recv()
            pool[out_at(hf, k)] += pool[8 + TWO * k]
            if hf == 0:
                pl.when(k < full - TWO)(lambda: lhop_b(0, k).start())

                @pl.when(k == 0)
                def _():
                    each(lambda p: activate(1, p), 4, 8)
                    pass_o(1, 0)
            else:
                lhop_b(1, k).start()

        each(chunk, 0, full)
        left = f_all[hf].reshape(HALF, width)
        if hf == 0:
            tail_load(0).wait()
            tail_load(1).wait()
        t_a[hf, :, :rest] = tail_product(left, 0)
        thop_a(hf).start()
        t_b[hf, :, :rest] = tail_product(left, 1)
        thop_a(hf).wait_recv()
        t_b[hf] += tg_a[hf]
        if hf == 1:
            thop_b(1).start()

    def release():
        each(lambda k: lhop_b(0, k).start(), full - TWO, full)
        thop_b(0).start()

    outward(0)
    pass_m(1)
    pass_o(1, 1)
    each(lambda p: hop_b(1, p).wait_send(), 0, 8)
    contract(1)
    hop_y(1).start()
    finish_layer(1, release)
    hop_f(1).wait_recv()
    outward(1)

    for g in range(8):
        for hf in range(TWO):
            f_nat[g * OWN + hf * 8:g * OWN + hf * 8 + 8, :] = f_all[hf, g // 4, g % 4]

    def inward(k, carry):
        slot = take_item(c_base + k)
        for n in range(TWO):
            pool[pl.ds(6 + TWO * k, TWO), :, :, :, n * hw:(n + 1) * hw] = product(f_nat[...], slot, n).reshape(TWO, TWO, TWO, OWN, hw)
        lhop_c(k).start()
        return carry

    lax.fori_loop(0, full, inward, 0)
    tail_load(TWO).wait()
    t_c[:, :rest] = tail_product(f_nat[...], TWO)
    thop_c.start()
    tail_load(3).wait()

    top[...] = jnp.full_like(top, LOW)
    mass_l[...] = jnp.zeros_like(mass_l)

    def fold(z):
        tiles = [z[:, i:i + LANES] for i in range(0, z.shape[1], LANES)]
        high = functools.reduce(jnp.maximum, tiles, top[...])
        mass_l[...] = mass_l[...] * jnp.exp(top[...] - high) + sum(jnp.exp(g - high) for g in tiles)
        top[...] = high

    def weave(first, second):
        n = first.shape[-1]
        return jnp.stack([first.reshape(8, 8, n), second.reshape(8, 8, n)], axis=1).reshape(LANES, n)

    def finish(k):
        slot = take_item(d_base + k)
        lhop_c(k).wait_recv()
        here = pl.ds(38 + TWO * k, TWO)
        for n in range(TWO):
            cols = slice(n * hw, (n + 1) * hw)
            pool[here, :, :, :, cols] += product(f_nat[...], slot, n).reshape(TWO, TWO, TWO, OWN, hw)
        lhop_b(0, k).wait_recv()
        lhop_b(1, k).wait_recv()
        for n in range(TWO):
            cols = slice(n * hw, (n + 1) * hw)
            z = pool[here, :, :, :, cols].reshape(LANES, hw)
            z = z + weave(pool[in_at(0, k), :, :, :, cols], pool[in_at(1, k), :, :, :, cols])
            z_v[pl.ds(pl.multiple_of(k * WB + n * hw, hw), hw), :] = z.T
            fold(z)
        z_store(k, WB).start()

    thop_c.wait_recv()
    tg_c[:, :rest] += tail_product(f_nat[...], 3)
    each(finish, 0, full)
    thop_b(0).wait_recv()
    thop_b(1).wait_recv()
    z_tail = tg_c[...] + weave(tg_b[0], tg_b[1])
    lane = lax.broadcasted_iota(jnp.int32, z_tail.shape, 1)
    fold(jnp.where(lane < rest, z_tail, LOW))
    z_v[full * WB:, :] = z_tail.T[:rest]
    z_store(full, rest).start()

    high = jnp.max(top[...], axis=1, keepdims=True)
    stat_z[mine] = to_lanes(high, jnp.sum(mass_l[...] * jnp.exp(top[...] - high), axis=1, keepdims=True))
    copies = []
    for dy in range(TWO):
        for d in range(4):
            if dy or d:
                i = dy * 4 + d - 1
                copies.append(send(stat_z.at[mine], stat_z.at[mine], sz_s.at[i], sz_r.at[i],
                                   y + dy * (1 - TWO * y), (xi + d) % 4))
    start(copies)
    for copy in copies:
        copy.wait()
    highs = [stat_z[i][0:1] for i in range(8)]
    best_all = functools.reduce(jnp.maximum, highs)
    lse_out[...] = best_all + jnp.log(sum(stat_z[i][1:TWO] * jnp.exp(highs[i] - best_all) for i in range(8)))

    each(lambda k: z_store(k, WB).wait(), 0, full)
    z_store(full, rest).wait()
    kv_store.wait()
    def drain_logits(k, carry):
        lhop_a(1, k).wait_send()
        lhop_b(0, k).wait_send()
        lhop_b(1, k).wait_send()
        lhop_c(k).wait_send()
        return carry

    lax.fori_loop(0, full, drain_logits, 0)
    for hf in range(TWO):
        for g in range(TWO):
            hop_m(hf, g).wait_send()
            hop_p(hf, g).wait_send()
        for n in range(3):
            hop_o(hf, n).wait_send()
        for hop in (hop_y, hop_f, thop_a, thop_b):
            hop(hf).wait_send()
    for hop in (hop_qa, hop_qb, hop_qc, thop_c):
        hop.wait_send()


def step_call(lens, hid, gain, gain_f, freq, wq, wk, wv, wg, wu, wo, wd, emb, k_cache, v_cache):
    width = hid.shape[TWO]
    qc, hd = wq.shape[1], wk.shape[1]
    seqs, length, _ = k_cache.shape
    cols = qc + TWO * hd
    steps = wg.shape[1] // FC
    heads = TWO * qc // hd
    share = emb.shape[0] // QUAD
    full = share // WB
    rest = share - full * WB
    tail_w = -(-rest // LANES) * LANES
    vmem = pl.BlockSpec(memory_space=pltpu.VMEM)
    hbm = pl.BlockSpec(memory_space=pl.ANY)

    def f32(*shape):
        return pltpu.VMEM(shape, F32)

    def bf16(*shape):
        return pltpu.VMEM(shape, BF16)

    def dma(*shape):
        return pltpu.SemaphoreType.DMA(shape)

    return pl.pallas_call(
        step_kernel, name="step",
        out_shape=[jax.ShapeDtypeStruct((TWO, OWN, hd), BF16), jax.ShapeDtypeStruct((share, LANES), F32),
                   jax.ShapeDtypeStruct((1, LANES), F32)],
        in_specs=[pl.BlockSpec(memory_space=pltpu.SMEM)] + [hbm] * 3 + [vmem] + [hbm] * 10, out_specs=[hbm, hbm, vmem],
        scratch_shapes=[
            bf16(TWO, OWN, hd), f32(share, LANES), bf16(OCT, OWN, width), f32(1, width), f32(1, width), f32(TWO, OWN, hd), f32(TWO, OWN, hd),
            bf16(LANES, width), bf16(RING, TWO, width, FC), bf16(width, TWO * hd),
            f32(TWO, TWO, TWO, OWN, cols), f32(TWO, TWO, OWN, cols), f32(TWO, OWN, cols), f32(TWO, OWN, cols), f32(TWO, TWO, OCT, cols),
            bf16(TWO, OWN, qc), bf16(TWO, OWN, qc), f32(seqs, heads, hd), f32(seqs, heads, hd), f32(seqs, 1, hd), f32(seqs, 1, hd),
            f32(QUAD * steps, TWO, TWO, OWN, TWO * FC), bf16(TWO, TWO, TWO, TWO, OWN, steps // TWO * FC),
            bf16(TWO, TWO, OCT, qc), bf16(TWO, TWO, TWO, TWO, OCT, qc),
            bf16(KVS, length, hd), bf16(KVS, length, hd), f32(heads, length), bf16(heads, length),
            f32(TWO, QUAD, TWO, OCT, width), f32(TWO, QUAD, OCT, width), bf16(TWO, TWO, QUAD, OCT, width), bf16(LANES, width), bf16(QUAD, rest, width),
            f32(TWO, HALF, tail_w), f32(TWO, HALF, tail_w), f32(TWO, HALF, tail_w), f32(TWO, HALF, tail_w), f32(LANES, tail_w), f32(LANES, tail_w),
            f32(LANES, LANES), f32(LANES, LANES), f32(QUAD, OCT, LANES), f32(TWO, QUAD, OCT, LANES), f32(OCT, OCT, LANES),
            dma(3), dma(full + TWO), dma(RING, TWO), dma(TWO), dma(QUAD), dma(KVS), dma(KVS), dma(steps), dma(steps), dma(TWO, steps // TWO), dma(TWO, steps // TWO),
            dma(TWO, TWO), dma(TWO, TWO), dma(TWO, TWO), dma(TWO, TWO), dma(3), dma(3),
            dma(TWO, 3), dma(TWO, 3), dma(TWO), dma(TWO), dma(TWO), dma(TWO), dma(3), dma(3), dma(TWO, 3), dma(TWO, 3),
            dma(TWO, full), dma(TWO, full), dma(TWO, full), dma(TWO, full), dma(full), dma(full),
            dma(TWO), dma(TWO), dma(TWO), dma(TWO), dma(1), dma(1), dma(7), dma(7)],
        compiler_params=pltpu.CompilerParams(collective_id=0, has_side_effects=True, vmem_limit_bytes=63 * TWO**20),
    )(lens, hid, gain, gain_f, freq, wq, wk, wv, wg, wu, wo, wd, emb, k_cache, v_cache)


def close_kernel(z_in, lse, kv, out, k_out, v_out, lse_out, buf, in_sem, out_sem):
    parts = buf.shape[0]
    rows = buf.shape[1]
    loads = [pltpu.make_async_copy(z_in.at[pl.ds(i * rows, rows)], buf.at[i], in_sem.at[i]) for i in range(parts)]
    stores = [pltpu.make_async_copy(buf.at[i], out.at[pl.ds(i * rows, rows)], out_sem.at[i]) for i in range(parts)]
    for load in loads:
        load.start()
    k_out[...] = kv[0]
    v_out[...] = kv[1]
    lse_out[...] = lse[...]
    for i in range(parts):
        loads[i].wait()
        buf[i] = buf[i] - lse[...]
        stores[i].start()
    for store in stores:
        store.wait()


def close_call(z, lse, kv):
    share, rows = z.shape
    parts = 4
    vmem = pl.BlockSpec(memory_space=pltpu.VMEM)
    hbm = pl.BlockSpec(memory_space=pl.ANY)
    small = jax.ShapeDtypeStruct(kv.shape[1:], BF16)
    return pl.pallas_call(
        close_kernel, name="close",
        out_shape=[jax.ShapeDtypeStruct((share, rows), F32), small, small, jax.ShapeDtypeStruct((1, rows), F32)],
        in_specs=[hbm, vmem, vmem], out_specs=[hbm, vmem, vmem, vmem],
        scratch_shapes=[pltpu.VMEM((parts, share // parts, rows), F32),
                        pltpu.SemaphoreType.DMA((parts,)), pltpu.SemaphoreType.DMA((parts,))],
        compiler_params=pltpu.CompilerParams(vmem_limit_bytes=63 * 2**20),
    )(z, lse, kv)


def solution(mesh):
    row_spec = P(("dp", "yax", "xax"))

    def local_step(hidden, cache_len, k_cache, v_cache, g_attn, w_query, w_key, w_value,
                   w_gate, w_up, w_out, w_down, g_final, embedding):
        width = hidden.shape[1]
        own_rows, _, head_dim = k_cache.shape
        half = head_dim // TWO
        lane = jnp.arange(head_dim)
        inv_freq = ROPE_BASE ** (-((lane % half).astype(F32) * 2.0) / head_dim)
        kv_new, logits_t, log_norm = step_call(
            cache_len, hidden.reshape(8, own_rows, width), g_attn[None], g_final[None], inv_freq[None],
            w_query, w_key, w_value, w_gate, w_up, w_out, w_down, embedding, k_cache, v_cache)
        log_probs, key_own, value_own, log_norm = close_call(logits_t, log_norm, kv_new)
        return key_own, value_own, log_probs.T, log_norm[0]

    in_specs = (P("dp", "xax"), P("dp"), row_spec, row_spec, P("xax"), P("xax", "yax"),
                P("xax", None), P("xax", None), P("xax", "yax"), P("xax", "yax"),
                P("yax", "xax"), P("yax", "xax"), P("xax"), P("yax", "xax"))
    out_specs = (row_spec, row_spec, P("dp", ("yax", "xax")), P("dp"))
    return jax.shard_map(local_step, mesh=mesh, in_specs=in_specs, out_specs=out_specs, check_vma=False)
```

```python
import functools

import jax
import jax.numpy as jnp
from jax import lax
from jax.experimental import pallas as pl
from jax.experimental.pallas import tpu as pltpu
from jax.sharding import PartitionSpec as P

EPS = 1e-6
ROPE_BASE = 10000.0
MESH = pl.DeviceIdType.MESH
F32 = jnp.float32
BF16 = jnp.bfloat16
LOW = -3e38
TWO, QUAD, OCT, OWN, PAIR, HALF, LANES = 2, 4, 8, 16, 32, 64, 128


def place():
    y = lax.axis_index("yax")
    xi = lax.axis_index("xax")
    chip = xi // 2
    core = xi % 2
    return y, xi, chip, core, chip * 2 + (1 - core), (1 - chip) * 2 + core


def send(src, dst, send_sem, recv_sem, y, xi):
    return pltpu.make_async_remote_copy(src_ref=src, dst_ref=dst, send_sem=send_sem, recv_sem=recv_sem,
                                        device_id={"yax": y, "xax": xi}, device_id_type=MESH)


def enter(peers):
    barrier = pltpu.get_barrier_semaphore()
    for y, xi in peers:
        pl.semaphore_signal(barrier, inc=1, device_id={"yax": y, "xax": xi}, device_id_type=MESH)
    return lambda: pl.semaphore_wait(barrier, len(peers))


def to_lanes(first, second):
    rows = first.shape[0]
    lane = lax.broadcasted_iota(jnp.int32, (rows, 128), 1)
    tile = jnp.where(lane == 0, first, jnp.where(lane == 1, second, 0.0))
    if rows < 128:
        tile = jnp.concatenate([tile, jnp.zeros((128 - rows, 128), F32)], axis=0)
    return tile.T[:8]


def to_columns(first, second):
    row = lax.broadcasted_iota(jnp.int32, (128, 128), 0)
    tile = jnp.where(row == 0, first, jnp.where(row == 1, second, 0.0)).T
    return tile[:, 0:1], tile[:, 1:2]


def norm_stats(values, stat, y, xi, send_sems, recv_sems, ready, size, after=lambda: None):
    rows, width = values.shape
    mean_own = jnp.sum(values, axis=1, keepdims=True) / width
    diff = values - mean_own
    stat[xi] = to_lanes(mean_own, jnp.sum(diff * diff, axis=1, keepdims=True))
    ready()
    copies = [send(stat.at[xi], stat.at[xi], send_sems.at[d - 1], recv_sems.at[d - 1], y, (xi + d) % size)
              for d in range(1, size)]
    for copy in copies:
        copy.start()
    after()
    for copy in copies:
        copy.wait()
    tiles = [stat[i] for i in range(size)]
    mean_all = sum(t[0:1] for t in tiles) / size
    spread = sum(t[1:TWO] for t in tiles) + width * sum((t[0:1] - mean_all) * (t[0:1] - mean_all) for t in tiles)
    mean_col, rstd_col = to_columns(mean_all, lax.rsqrt(spread / (width * size) + EPS))
    return mean_col[:rows], rstd_col[:rows]


FC = 512
WB = 1024
RING = 6
KVS = 3
VLIM = 121 * 2**19
HELD = 6


def step_kernel(lens, hid_h, gain_h, gain_fh, freq, wq, wk, wv, wg, wu, wo, wd, emb, k_hbm, v_hbm,
                kv_out, z_out, lse_out,
                hid, gain, gain_f, cos, sin, n_perm, ring, w_kv, part_q, ga_q, sb_q, gb_q, total, q_rot, q_full, q_heads, o_heads, kn, vn,
                pool, act, o_in, o_all, k_buf, v_buf, scores, probs, acc, y_got, f_all, f_nat, e_tail,
                t_a, t_b, tg_a, tg_b, t_c, tg_c, top, mass_l, stat, stat_f, stat_z,
                i_sem, r_sem, kv_sem, tail_sem, k_sem, v_sem, a_s, a_r, b_s, b_r, m_s, m_r, p_s, p_r, q_s, q_r,
                o_s, o_r, y_s, y_r, f_s, f_r, st_s, st_r, sf_s, sf_r,
                la_s, la_r, lb_s, lb_r, lc_s, lc_r, ta_s, ta_r, tb_s, tb_r, tc_s, tc_r, sz_s, sz_r):
    y, xi, chip, core, partner, twin = place()
    width = n_perm.shape[1]
    hw = width // TWO
    qc, hd = wq.shape[1], wk.shape[1]
    heads = qc // hd
    steps = wg.shape[1] // FC
    seqs = q_heads.shape[0]
    length = k_buf.shape[1]
    share = emb.shape[0] // 4
    full = share // WB
    rest = share - full * WB
    mine = y * 4 + xi
    ready = enter([(y, (xi + d) % 4) for d in (1, TWO, 3)] + [(1 - y, (xi + d) % 4) for d in range(4)])

    def start(copies):
        for copy in copies:
            copy.start()

    inputs = [pltpu.make_async_copy(src, dst, i_sem.at[i])
              for i, (src, dst) in enumerate(((hid_h, hid), (gain_h, gain), (gain_fh, gain_f)))]
    start(inputs)

    def q_loads(s):
        return [pltpu.make_async_copy(wq.at[:, pl.ds((TWO * s + i) * FC, FC)], ring.at[s, i], r_sem.at[s, i]) for i in range(TWO)]

    def w_loads(j):
        cols = pl.ds(pl.multiple_of(j * FC, FC), FC)
        slot = (j + TWO) % RING
        return [pltpu.make_async_copy(w.at[:, cols], ring.at[slot, i], r_sem.at[slot, i]) for i, w in enumerate((wg, wu))]

    kv_w = [pltpu.make_async_copy(w, w_kv.at[:, pl.ds(i * hd, hd)], kv_sem.at[i]) for i, w in enumerate((wk, wv))]
    start(q_loads(0))
    start(q_loads(1))
    start(kv_w)
    for j in range(RING - 3):
        start(w_loads(j))

    nd, no = wd.shape[0] // WB, wo.shape[0] // WB
    np_ = nd + no
    e_base = (np_, TWO * np_ + TWO * full)
    c_base = TWO * np_ + 4 * full
    d_base = c_base + full
    items = d_base + full
    far, near = (1 - chip) * TWO, chip * TWO

    def block(src, row, t):
        slot = t % RING
        return [pltpu.make_async_copy(src.at[pl.ds(row, WB), pl.ds(i * hw, hw)], ring.at[slot, i], r_sem.at[slot, i])
                for i in range(TWO)]

    def emb_row(quarter, k):
        return pl.multiple_of(quarter * share + k * WB, PAIR)

    def load_item(t):
        for base in (0, np_ + TWO * full):
            @pl.when((t >= base) & (t < base + nd))
            def _(base=base):
                start(block(wd, pl.multiple_of((t - base) * WB, WB), t))

            @pl.when((t >= base + nd) & (t < base + np_))
            def _(base=base):
                start(block(wo, pl.multiple_of((t - base - nd) * WB, WB), t))

        for base in e_base:
            @pl.when((t >= base) & (t < base + TWO * full))
            def _(base=base):
                k, own = (t - base) // TWO, (t - base) % TWO
                start(block(emb, emb_row(far + (1 - core) + own * (TWO * core - 1), k), t))

        @pl.when((t >= c_base) & (t < d_base))
        def _():
            start(block(emb, emb_row(near + 1 - core, t - c_base), t))

        @pl.when((t >= d_base) & (t < items))
        def _():
            start(block(emb, emb_row(near + core, t - d_base), t))

    def take_item(t):
        load_item(t + RING - 1)
        for copy in block(wd, 0, t):
            copy.wait()
        return t % RING

    def tail_load(i):
        quarter = (far + 1 - core, far + core, near + 1 - core, near + core)[i]
        rows = pl.ds(pl.multiple_of(quarter * share + full * WB, PAIR), rest)
        return pltpu.make_async_copy(emb.at[rows], e_tail.at[i], tail_sem.at[i])

    def cache_loads(b):
        slot = b % KVS
        return [pltpu.make_async_copy(k_hbm.at[b], k_buf.at[slot], k_sem.at[slot]),
                pltpu.make_async_copy(v_hbm.at[b], v_buf.at[slot], v_sem.at[slot])]

    def hop_a(j):
        return send(pool.at[pl.ds(TWO * j, TWO), 1 - core], pool.at[TWO * steps + j], a_s.at[j], a_r.at[j], y, partner)

    def sum_at(hf, p):
        return pool.at[3 * steps + hf * (steps // 4) + p // TWO, p % TWO]

    def got_at(hf, p):
        return pool.at[3 * steps + (TWO + hf) * (steps // 4) + p // TWO, p % TWO]

    def hop_b(hf, p):
        return send(sum_at(hf, p), got_at(hf, p), b_s.at[hf, p], b_r.at[hf, p], y, twin)

    def hop_m(hf, g):
        return send(act.at[hf, g, core, chip], act.at[hf, g, core, chip], m_s.at[hf, g], m_r.at[hf, g], y, twin)

    def hop_p(hf, g):
        return send(act.at[hf, g, core], act.at[hf, g, core], p_s.at[hf, g], p_r.at[hf, g], y, partner)

    q_cols = (pl.ds(0, TWO * FC), pl.ds(TWO * FC, qc + TWO * hd - TWO * FC))
    hop_qa = [send(part_q.at[:, 1 - core, :, :, cut], ga_q.at[..., cut], q_s.at[i, 0], q_r.at[i, 0], y, partner)
              for i, cut in enumerate(q_cols)]
    hop_qb = [send(sb_q.at[..., cut], gb_q.at[..., cut], q_s.at[i, 1], q_r.at[i, 1], y, twin) for i, cut in enumerate(q_cols)]

    def pair_queries(i):
        hop_qa[i].wait_recv()
        sb_q[:, :, q_cols[i]] = part_q[:, core, 1 - chip, :, q_cols[i]] + ga_q[:, 1 - chip, :, q_cols[i]]
        hop_qb[i].start()

    hop_qc = send(q_rot.at[1 - y], q_full.at[y], q_s.at[0, TWO], q_r.at[0, TWO], 1 - y, xi)

    def hop_o(hf, n):
        if n == 0:
            return send(o_in.at[1 - y, hf], o_all.at[hf, core, chip, y], o_s.at[hf, 0], o_r.at[hf, 0], 1 - y, xi)
        if n == 1:
            return send(o_all.at[hf, core, chip], o_all.at[hf, core, chip], o_s.at[hf, 1], o_r.at[hf, 1], y, twin)
        return send(o_all.at[hf, core], o_all.at[hf, core], o_s.at[hf, TWO], o_r.at[hf, TWO], y, partner)

    def hop_y(hf):
        return send(acc.at[hf, :, 1 - y], y_got.at[hf], y_s.at[hf], y_r.at[hf], 1 - y, xi)

    def hop_f(hf):
        return send(f_all.at[hf, y], f_all.at[hf, y], f_s.at[hf], f_r.at[hf], 1 - y, xi)

    def turns(owner):
        row = lax.broadcasted_iota(jnp.int32, (OWN, hd), 0)
        pos = functools.reduce(lambda acc_, r: jnp.where(row == r, lens[owner * OWN + r], acc_), range(OWN), jnp.zeros((OWN, hd), jnp.int32))
        angle = pos.astype(F32) * freq[...]
        lane = lax.broadcasted_iota(jnp.int32, (OWN, hd), 1)
        return jnp.cos(angle), jnp.where(lane < hd // TWO, -jnp.sin(angle), jnp.sin(angle))

    for load in inputs:
        load.wait()
    h = hid[...].astype(F32).reshape(LANES, width)
    mean, rstd = norm_stats(h, stat, y, xi, st_s, st_r, ready, 4)
    normed = ((h - mean) * rstd * gain[...]).astype(BF16)
    for hf in range(TWO):
        for core_o in range(TWO):
            for chip_o in range(TWO):
                for y_o in range(TWO):
                    src = (y_o * 4 + chip_o * TWO + core_o) * OWN + hf * 8
                    dst = hf * HALF + core_o * PAIR + chip_o * OWN + y_o * 8
                    n_perm[dst:dst + 8, :] = normed[src:src + 8, :]

    for s in range(TWO):
        for i, load in enumerate(q_loads(s)):
            load.wait()
            prod = jnp.dot(n_perm[...], ring[s, i], preferred_element_type=F32)
            part_q[:, :, :, :, (TWO * s + i) * FC:(TWO * s + i + 1) * FC] = prod.reshape(TWO, TWO, TWO, OWN, FC)
        start(w_loads(RING - 3 + s))
        if s == 0:
            hop_qa[0].start()
    for load in kv_w:
        load.wait()
    part_q[..., qc:] = jnp.dot(n_perm[...], w_kv[...], preferred_element_type=F32).reshape(TWO, TWO, TWO, OWN, TWO * hd)
    hop_qa[1].start()
    pair_queries(0)

    def rotate_queries():
        hop_qb[0].wait_recv()
        hop_qb[1].wait_recv()
        both = part_q[:, core, chip] + ga_q[:, chip] + gb_q[...]
        total[...] = both.astype(BF16).astype(F32).reshape(TWO, TWO, 8, qc + TWO * hd)
        for y_o in range(TWO):
            cos_r, sin_r = cos[y_o], sin[y_o]
            for head in range(heads):
                val = total[:, y_o, :, head * hd:(head + 1) * hd].reshape(OWN, hd)
                q_rot[y_o, :, head * hd:(head + 1) * hd] = (val * cos_r + pltpu.roll(val, hd // TWO, 1) * sin_r).astype(BF16)
        hop_qc.start()
        key = total[:, y, :, qc:qc + hd].reshape(OWN, hd)
        value = total[:, y, :, qc + hd:].reshape(OWN, hd)
        key = (key * cos[y] + pltpu.roll(key, hd // TWO, 1) * sin[y]).astype(BF16)
        kv_out[0] = key
        kv_out[1] = value.astype(BF16)
        kn[:, 0, :] = key.astype(F32)
        vn[:, 0, :] = value
        q_full[y] = q_rot[y]

    def spread_queries():
        hop_qc.wait_recv()
        for y_o in range(TWO):
            for head in range(heads):
                q_heads[:, y_o * heads + head, :] = q_full[y_o, :, head * hd:(head + 1) * hd].astype(F32)

    def add_pair(j):
        hop_a(j).wait_recv()
        for hf in range(TWO):
            sum_at(hf, j // TWO)[j % TWO] = pool[TWO * j + hf, core, 1 - chip] + pool[TWO * steps + j, hf, 1 - chip]

        @pl.when(j % TWO == 1)
        def _():
            hop_b(0, j // TWO).start()

    def project(j, carry):
        @pl.when(j + RING - 1 < steps)
        def _():
            start(w_loads(j + RING - 1))

        slot = (j + TWO) % RING
        for i, load in enumerate(w_loads(j)):
            load.wait()
            prod = jnp.dot(n_perm[...], ring[slot, i], preferred_element_type=F32)
            pool[pl.ds(TWO * j, TWO), :, :, :, i * FC:(i + 1) * FC] = prod.reshape(TWO, TWO, TWO, OWN, FC)
        hop_a(j).start()

        @pl.when(j == 0)
        def _():
            pair_queries(1)

        @pl.when(j >= 1)
        def _():
            add_pair(j - 1)

        @pl.when((j == TWO) | (j == 3))
        def _():
            cos[j - TWO], sin[j - TWO] = turns((j - TWO) * 4 + chip * TWO + core)

        @pl.when(j == 4)
        def _():
            for b in range(KVS):
                start(cache_loads(b))

        @pl.when(j == 8)
        def _():
            rotate_queries()

        @pl.when(j == 12)
        def _():
            spread_queries()
        return carry

    lax.fori_loop(0, steps, project, 0)
    add_pair(steps - 1)
    for t in range(RING - 1):
        start(block(wd, t * WB, t))
    for i in range(4):
        tail_load(i).start()

    def activate(hf, p):
        hop_b(hf, p).wait_recv()
        for i in range(TWO):
            j = TWO * p + i
            both = pool[TWO * j + hf, core, chip] + pool[TWO * steps + j, hf, chip] + got_at(hf, p)[i]
            gate = both[:, :FC].astype(BF16).astype(F32)
            up_val = both[:, FC:].astype(BF16).astype(F32)
            cols = pl.ds(pl.multiple_of(((p % 4) * TWO + i) * FC, FC), FC)
            act[hf, p // 4, core, chip, :, cols] = (jax.nn.silu(gate) * up_val).astype(BF16)

        @pl.when(p % 4 == 3)
        def _():
            hop_m(hf, p // 4).start()

    part_len = 1024

    def attend(b):
        slot = b % KVS
        scale = hd ** -0.5
        q32 = q_heads[b]
        q = q32.astype(BF16)
        limit = lens[mine * OWN + b]
        s_new = jnp.sum(q32 * kn[b], axis=1, keepdims=True) * scale
        load_k, load_v = cache_loads(b)
        load_k.wait()
        high = None
        for i in range(length // part_len):
            rows = slice(i * part_len, (i + 1) * part_len)
            s = lax.dot_general(q, k_buf[slot, rows], (((1,), (1,)), ((), ())), preferred_element_type=F32) * scale
            pos = lax.broadcasted_iota(jnp.int32, s.shape, 1) + i * part_len
            s = jnp.where(pos < limit, s, -jnp.inf)
            scores[:, rows] = s
            for c in range(0, part_len, LANES):
                high = s[:, c:c + LANES] if high is None else jnp.maximum(high, s[:, c:c + LANES])
        best = jnp.maximum(jnp.max(high, axis=1, keepdims=True), s_new)
        mass = None
        for i in range(length // part_len):
            rows = slice(i * part_len, (i + 1) * part_len)
            e = jnp.exp(scores[:, rows] - best)
            scores[:, rows] = e
            for c in range(0, part_len, LANES):
                mass = e[:, c:c + LANES] if mass is None else mass + e[:, c:c + LANES]
        e_new = jnp.exp(s_new - best)
        inv = 1.0 / (jnp.sum(mass, axis=1, keepdims=True) + e_new)
        for i in range(length // part_len):
            rows = slice(i * part_len, (i + 1) * part_len)
            probs[:, rows] = (scores[:, rows] * inv).astype(BF16)
        load_v.wait()
        o = jnp.dot(probs[...], v_buf[slot], preferred_element_type=F32)
        o = o + (e_new * inv).astype(BF16).astype(F32) * vn[b]
        o_heads[b] = o.astype(BF16).astype(F32)

        @pl.when(b + KVS < seqs)
        def _():
            start(cache_loads(b + KVS))

    def send_heads(hf):
        for y_o in range(TWO):
            for head in range(heads):
                o_in[y_o, hf, :, head * hd:(head + 1) * hd] = o_heads[hf * 8:hf * 8 + 8, y_o * heads + head, :].astype(BF16)
        o_all[hf, core, chip, y] = o_in[y, hf]
        hop_o(hf, 0).start()

    def contract(hf):
        base = hf * (np_ + TWO * full)
        acc[hf] = jnp.zeros(acc.shape[1:], F32)

        def add(t, left):
            slot = take_item(t)
            for i in range(TWO):
                prod = jnp.dot(left, ring[slot, i], preferred_element_type=F32)
                acc[hf, :, :, :, i * hw:(i + 1) * hw] += prod.reshape(4, TWO, 8, hw)

        for g in range(TWO):
            hop_p(hf, g).wait_recv()

            def from_act(i, carry):
                add(base + g * (nd // TWO) + i, act[hf, g, :, :, :, pl.ds(pl.multiple_of(i * WB, WB), WB)].reshape(HALF, WB))
                return carry

            lax.fori_loop(0, nd // TWO, from_act, 0)
        hop_o(hf, TWO).wait_recv()

        def from_heads(i, carry):
            add(base + nd + i, o_all[hf, :, :, :, :, pl.ds(pl.multiple_of(i * WB, WB), WB)].reshape(HALF, WB))
            return carry

        lax.fori_loop(0, no, from_heads, 0)

    def finish_layer(hf, after):
        hop_y(hf).wait_recv()
        res = [hid[y * 4 + (i % TWO) * TWO + i // TWO, hf * 8:hf * 8 + 8].astype(F32) for i in range(4)]
        branch = acc[hf, :, y] + y_got[hf]
        r = jnp.concatenate(res, axis=0) + branch.reshape(PAIR, width)
        mean, rstd = norm_stats(r, stat_f.at[hf], y, xi, sf_s.at[hf], sf_r.at[hf], lambda: None, 4, after)
        f = ((r - mean) * rstd * gain_f[...]).astype(BF16)
        for i in range(4):
            f_all[hf, y, (i % TWO) * TWO + i // TWO] = f[i * 8:(i + 1) * 8]
        hop_f(hf).start()

    def each(body, low, high):
        def step(p, carry):
            body(p)
            return carry

        lax.fori_loop(low, high, step, 0)

    def pass_m(hf):
        for g in range(TWO):
            hop_m(hf, g).wait_recv()
            hop_p(hf, g).start()

    def pass_o(hf, n):
        hop_o(hf, n).wait_recv()
        hop_o(hf, n + 1).start()

    def mix(i):
        pl.when(i == 8)(lambda: send_heads(0))
        attend(i)
        pl.when(i < 8)(lambda: activate(0, i))

        @pl.when(i == 8)
        def _():
            pass_o(0, 0)
            each(lambda p: hop_b(1, p).start(), 0, HELD)

        pl.when(i == 10)(lambda: pass_m(0))
        pl.when(i == 11)(lambda: pass_o(0, 1))

        @pl.when(i == 12)
        def _():
            each(lambda j: hop_a(j).wait_send(), 0, steps)
            each(lambda p: hop_b(0, p).wait_send(), 0, 8)
            contract(0)
            hop_y(0).start()
            each(lambda p: activate(1, p), 0, TWO)

        @pl.when(i == 13)
        def _():
            finish_layer(0, lambda: each(lambda p: hop_b(1, p).start(), HELD, 8))

    each(mix, 0, seqs)
    hop_f(0).wait_recv()
    send_heads(1)
    each(lambda p: activate(1, p), TWO, 4)

    def out_at(hf, k):
        return 56 - hf * 6 + k

    def in_at(hf, k):
        return PAIR + k if hf else 20 + TWO * k

    def lhop_a(hf, k):
        return send(pool.at[k], pool.at[8 + TWO * k], la_s.at[hf, k], la_r.at[hf, k], y, partner)

    def lhop_b(hf, k):
        return send(pool.at[out_at(hf, k)], pool.at[in_at(hf, k)], lb_s.at[hf, k], lb_r.at[hf, k], y, twin)

    def lhop_c(k):
        return send(pool.at[pl.ds(6 + TWO * k, TWO)], pool.at[pl.ds(38 + TWO * k, TWO)], lc_s.at[k], lc_r.at[k], y, partner)

    def thop_a(hf):
        return send(t_a.at[hf], tg_a.at[hf], ta_s.at[hf], ta_r.at[hf], y, partner)

    def thop_b(hf):
        return send(t_b.at[hf], tg_b.at[hf], tb_s.at[hf], tb_r.at[hf], y, twin)

    thop_c = send(t_c, tg_c, tc_s.at[0], tc_r.at[0], y, partner)
    nt = (((1,), (1,)), ((), ()))

    def product(left, slot, n):
        rows = slice(n * hw, (n + 1) * hw)
        return (lax.dot_general(left[:, :hw], ring[slot, 0, rows], nt, preferred_element_type=F32)
                + lax.dot_general(left[:, hw:], ring[slot, 1, rows], nt, preferred_element_type=F32))

    def tail_product(left, i):
        return lax.dot_general(left, e_tail[i], nt, preferred_element_type=F32)

    t_a[...] = jnp.zeros_like(t_a)
    t_b[...] = jnp.zeros_like(t_b)
    t_c[...] = jnp.zeros_like(t_c)

    def outward(hf):
        def chunk(k):
            left = f_all[hf].reshape(HALF, width)
            if hf == 1:
                lhop_a(0, k).wait_send()
            slot = take_item(e_base[hf] + TWO * k)
            for n in range(TWO):
                pool[k, :, :, :, n * hw:(n + 1) * hw] = product(left, slot, n).reshape(TWO, TWO, OWN, hw)
            lhop_a(hf, k).start()
            slot = take_item(e_base[hf] + TWO * k + 1)
            for n in range(TWO):
                pool[out_at(hf, k), :, :, :, n * hw:(n + 1) * hw] = product(left, slot, n).reshape(TWO, TWO, OWN, hw)
            lhop_a(hf, k).wait_recv()
            pool[out_at(hf, k)] += pool[8 + TWO * k]
            if hf == 0:
                pl.when(k < full - TWO)(lambda: lhop_b(0, k).start())

                @pl.when(k == 0)
                def _():
                    each(lambda p: activate(1, p), 4, 8)
                    pass_o(1, 0)
            else:
                lhop_b(1, k).start()

        each(chunk, 0, full)
        left = f_all[hf].reshape(HALF, width)
        if hf == 0:
            tail_load(0).wait()
            tail_load(1).wait()
        t_a[hf, :, :rest] = tail_product(left, 0)
        thop_a(hf).start()
        t_b[hf, :, :rest] = tail_product(left, 1)
        thop_a(hf).wait_recv()
        t_b[hf] += tg_a[hf]
        if hf == 1:
            thop_b(1).start()

    def release():
        each(lambda k: lhop_b(0, k).start(), full - TWO, full)
        thop_b(0).start()

    outward(0)
    pass_m(1)
    pass_o(1, 1)
    each(lambda p: hop_b(1, p).wait_send(), 0, 8)
    contract(1)
    hop_y(1).start()
    finish_layer(1, release)
    hop_f(1).wait_recv()
    outward(1)

    for g in range(8):
        for hf in range(TWO):
            f_nat[g * OWN + hf * 8:g * OWN + hf * 8 + 8, :] = f_all[hf, g // 4, g % 4]

    def inward(k, carry):
        slot = take_item(c_base + k)
        for n in range(TWO):
            pool[pl.ds(6 + TWO * k, TWO), :, :, :, n * hw:(n + 1) * hw] = product(f_nat[...], slot, n).reshape(TWO, TWO, TWO, OWN, hw)
        lhop_c(k).start()
        return carry

    lax.fori_loop(0, full, inward, 0)
    tail_load(TWO).wait()
    t_c[:, :rest] = tail_product(f_nat[...], TWO)
    thop_c.start()
    tail_load(3).wait()

    top[...] = jnp.full_like(top, LOW)
    mass_l[...] = jnp.zeros_like(mass_l)

    def fold(z):
        tiles = [z[:, i:i + LANES] for i in range(0, z.shape[1], LANES)]
        high = functools.reduce(jnp.maximum, tiles, top[...])
        mass_l[...] = mass_l[...] * jnp.exp(top[...] - high) + sum(jnp.exp(g - high) for g in tiles)
        top[...] = high

    def weave(first, second):
        n = first.shape[-1]
        return jnp.stack([first.reshape(8, 8, n), second.reshape(8, 8, n)], axis=1).reshape(LANES, n)

    def finish(k):
        slot = take_item(d_base + k)
        lhop_c(k).wait_recv()
        here = pl.ds(38 + TWO * k, TWO)
        for n in range(TWO):
            cols = slice(n * hw, (n + 1) * hw)
            pool[here, :, :, :, cols] += product(f_nat[...], slot, n).reshape(TWO, TWO, TWO, OWN, hw)
        lhop_b(0, k).wait_recv()
        lhop_b(1, k).wait_recv()
        for n in range(TWO):
            cols = slice(n * hw, (n + 1) * hw)
            z = pool[here, :, :, :, cols].reshape(LANES, hw)
            z = z + weave(pool[in_at(0, k), :, :, :, cols], pool[in_at(1, k), :, :, :, cols])
            z_out[pl.ds(pl.multiple_of(k * WB + n * hw, hw), hw), :] = z.T
            fold(z)

    thop_c.wait_recv()
    tg_c[:, :rest] += tail_product(f_nat[...], 3)
    each(finish, 0, full)
    thop_b(0).wait_recv()
    thop_b(1).wait_recv()
    z_tail = tg_c[...] + weave(tg_b[0], tg_b[1])
    lane = lax.broadcasted_iota(jnp.int32, z_tail.shape, 1)
    fold(jnp.where(lane < rest, z_tail, LOW))
    z_out[full * WB:, :] = z_tail.T[:rest]

    high = jnp.max(top[...], axis=1, keepdims=True)
    stat_z[mine] = to_lanes(high, jnp.sum(mass_l[...] * jnp.exp(top[...] - high), axis=1, keepdims=True))
    copies = []
    for dy in range(TWO):
        for d in range(4):
            if dy or d:
                i = dy * 4 + d - 1
                copies.append(send(stat_z.at[mine], stat_z.at[mine], sz_s.at[i], sz_r.at[i],
                                   y + dy * (1 - TWO * y), (xi + d) % 4))
    start(copies)
    for copy in copies:
        copy.wait()
    highs = [stat_z[i][0:1] for i in range(8)]
    best_all = functools.reduce(jnp.maximum, highs)
    lse_out[...] = best_all + jnp.log(sum(stat_z[i][1:TWO] * jnp.exp(highs[i] - best_all) for i in range(8)))

    def drain_logits(k, carry):
        lhop_a(1, k).wait_send()
        lhop_b(0, k).wait_send()
        lhop_b(1, k).wait_send()
        lhop_c(k).wait_send()
        return carry

    lax.fori_loop(0, full, drain_logits, 0)
    for hf in range(TWO):
        for g in range(TWO):
            hop_m(hf, g).wait_send()
            hop_p(hf, g).wait_send()
        for n in range(3):
            hop_o(hf, n).wait_send()
        for hop in (hop_y, hop_f, thop_a, thop_b):
            hop(hf).wait_send()
    for hop in (*hop_qa, *hop_qb, hop_qc, thop_c):
        hop.wait_send()


def step_call(lens, hid, gain, gain_f, freq, wq, wk, wv, wg, wu, wo, wd, emb, k_cache, v_cache):
    width = hid.shape[TWO]
    qc, hd = wq.shape[1], wk.shape[1]
    seqs, length, _ = k_cache.shape
    cols = qc + TWO * hd
    steps = wg.shape[1] // FC
    heads = TWO * qc // hd
    share = emb.shape[0] // QUAD
    full = share // WB
    rest = share - full * WB
    tail_w = -(-rest // LANES) * LANES
    vmem = pl.BlockSpec(memory_space=pltpu.VMEM)
    hbm = pl.BlockSpec(memory_space=pl.ANY)

    def f32(*shape):
        return pltpu.VMEM(shape, F32)

    def bf16(*shape):
        return pltpu.VMEM(shape, BF16)

    def dma(*shape):
        return pltpu.SemaphoreType.DMA(shape)

    return pl.pallas_call(
        step_kernel, name="step",
        out_shape=[bf16(TWO, OWN, hd), f32(share, LANES), f32(1, LANES)],
        in_specs=[pl.BlockSpec(memory_space=pltpu.SMEM)] + [hbm] * 3 + [vmem] + [hbm] * 10, out_specs=[vmem] * 3,
        scratch_shapes=[
            bf16(OCT, OWN, width), f32(1, width), f32(1, width), f32(TWO, OWN, hd), f32(TWO, OWN, hd),
            bf16(LANES, width), bf16(RING, TWO, width, FC), bf16(width, TWO * hd),
            f32(TWO, TWO, TWO, OWN, cols), f32(TWO, TWO, OWN, cols), f32(TWO, OWN, cols), f32(TWO, OWN, cols), f32(TWO, TWO, OCT, cols),
            bf16(TWO, OWN, qc), bf16(TWO, OWN, qc), f32(seqs, heads, hd), f32(seqs, heads, hd), f32(seqs, 1, hd), f32(seqs, 1, hd),
            f32(QUAD * steps, TWO, TWO, OWN, TWO * FC), bf16(TWO, TWO, TWO, TWO, OWN, steps // TWO * FC),
            bf16(TWO, TWO, OCT, qc), bf16(TWO, TWO, TWO, TWO, OCT, qc),
            bf16(KVS, length, hd), bf16(KVS, length, hd), f32(heads, length), bf16(heads, length),
            f32(TWO, QUAD, TWO, OCT, width), f32(TWO, QUAD, OCT, width), bf16(TWO, TWO, QUAD, OCT, width), bf16(LANES, width), bf16(QUAD, rest, width),
            f32(TWO, HALF, tail_w), f32(TWO, HALF, tail_w), f32(TWO, HALF, tail_w), f32(TWO, HALF, tail_w), f32(LANES, tail_w), f32(LANES, tail_w),
            f32(LANES, LANES), f32(LANES, LANES), f32(QUAD, OCT, LANES), f32(TWO, QUAD, OCT, LANES), f32(OCT, OCT, LANES),
            dma(3), dma(RING, TWO), dma(TWO), dma(QUAD), dma(KVS), dma(KVS), dma(steps), dma(steps), dma(TWO, steps // TWO), dma(TWO, steps // TWO),
            dma(TWO, TWO), dma(TWO, TWO), dma(TWO, TWO), dma(TWO, TWO), dma(TWO, 3), dma(TWO, 3),
            dma(TWO, 3), dma(TWO, 3), dma(TWO), dma(TWO), dma(TWO), dma(TWO), dma(3), dma(3), dma(TWO, 3), dma(TWO, 3),
            dma(TWO, full), dma(TWO, full), dma(TWO, full), dma(TWO, full), dma(full), dma(full),
            dma(TWO), dma(TWO), dma(TWO), dma(TWO), dma(1), dma(1), dma(7), dma(7)],
        compiler_params=pltpu.CompilerParams(collective_id=0, has_side_effects=True, vmem_limit_bytes=VLIM),
    )(lens, hid, gain, gain_f, freq, wq, wk, wv, wg, wu, wo, wd, emb, k_cache, v_cache)


def close_kernel(z, lse, kv, out, k_out, v_out, lse_out, buf, out_sem):
    parts = buf.shape[0]
    rows = buf.shape[1]
    stores = [pltpu.make_async_copy(buf.at[i], out.at[pl.ds(i * rows, rows)], out_sem.at[i]) for i in range(parts)]
    for i in range(parts):
        buf[i] = z[i * rows:(i + 1) * rows, :] - lse[...]
        stores[i].start()
    k_out[...] = kv[0]
    v_out[...] = kv[1]
    lse_out[...] = lse[...]
    for store in stores:
        store.wait()


def close_call(z, lse, kv):
    share, rows = z.shape
    parts = 4
    vmem = pl.BlockSpec(memory_space=pltpu.VMEM)
    hbm = pl.BlockSpec(memory_space=pl.ANY)
    small = jax.ShapeDtypeStruct(kv.shape[1:], BF16)
    return pl.pallas_call(
        close_kernel, name="close",
        out_shape=[jax.ShapeDtypeStruct((share, rows), F32), small, small, jax.ShapeDtypeStruct((1, rows), F32)],
        in_specs=[vmem] * 3, out_specs=[hbm, vmem, vmem, vmem],
        scratch_shapes=[pltpu.VMEM((parts, share // parts, rows), F32), pltpu.SemaphoreType.DMA((parts,))],
        compiler_params=pltpu.CompilerParams(vmem_limit_bytes=16 * 2**20),
    )(z, lse, kv)


def solution(mesh):
    row_spec = P(("dp", "yax", "xax"))

    def local_step(hidden, cache_len, k_cache, v_cache, g_attn, w_query, w_key, w_value,
                   w_gate, w_up, w_out, w_down, g_final, embedding):
        width = hidden.shape[1]
        own_rows, _, head_dim = k_cache.shape
        half = head_dim // TWO
        lane = jnp.arange(head_dim)
        inv_freq = ROPE_BASE ** (-((lane % half).astype(F32) * 2.0) / head_dim)
        kv_new, logits_t, log_norm = step_call(
            cache_len, hidden.reshape(8, own_rows, width), g_attn[None], g_final[None], inv_freq[None],
            w_query, w_key, w_value, w_gate, w_up, w_out, w_down, embedding, k_cache, v_cache)
        log_probs, key_own, value_own, log_norm = close_call(logits_t, log_norm, kv_new)
        return key_own, value_own, log_probs.T, log_norm[0]

    in_specs = (P("dp", "xax"), P("dp"), row_spec, row_spec, P("xax"), P("xax", "yax"),
                P("xax", None), P("xax", None), P("xax", "yax"), P("xax", "yax"),
                P("yax", "xax"), P("yax", "xax"), P("xax"), P("yax", "xax"))
    out_specs = (row_spec, row_spec, P("dp", ("yax", "xax")), P("dp"))
    return jax.shard_map(local_step, mesh=mesh, in_specs=in_specs, out_specs=out_specs, check_vma=False)
```

```python
import functools

import jax
import jax.numpy as jnp
from jax import lax
from jax.experimental import pallas as pl
from jax.experimental.pallas import tpu as pltpu
from jax.sharding import PartitionSpec as P

EPS = 1e-6
ROPE_BASE = 10000.0
MESH = pl.DeviceIdType.MESH
F32 = jnp.float32
BF16 = jnp.bfloat16
LOW = -3e38
TWO, QUAD, OCT, OWN, PAIR, HALF, LANES = 2, 4, 8, 16, 32, 64, 128


def place():
    y = lax.axis_index("yax")
    xi = lax.axis_index("xax")
    chip = xi // 2
    core = xi % 2
    return y, xi, chip, core, chip * 2 + (1 - core), (1 - chip) * 2 + core


def send(src, dst, send_sem, recv_sem, y, xi):
    return pltpu.make_async_remote_copy(src_ref=src, dst_ref=dst, send_sem=send_sem, recv_sem=recv_sem,
                                        device_id={"yax": y, "xax": xi}, device_id_type=MESH)


def enter(peers):
    barrier = pltpu.get_barrier_semaphore()
    for y, xi in peers:
        pl.semaphore_signal(barrier, inc=1, device_id={"yax": y, "xax": xi}, device_id_type=MESH)
    return lambda: pl.semaphore_wait(barrier, len(peers))


def to_lanes(first, second):
    rows = first.shape[0]
    lane = lax.broadcasted_iota(jnp.int32, (rows, 128), 1)
    tile = jnp.where(lane == 0, first, jnp.where(lane == 1, second, 0.0))
    if rows < 128:
        tile = jnp.concatenate([tile, jnp.zeros((128 - rows, 128), F32)], axis=0)
    return tile.T[:8]


def to_columns(first, second):
    row = lax.broadcasted_iota(jnp.int32, (128, 128), 0)
    tile = jnp.where(row == 0, first, jnp.where(row == 1, second, 0.0)).T
    return tile[:, 0:1], tile[:, 1:2]


def stat_hops(stat, y, xi, send_sems, recv_sems):
    return [send(stat.at[xi], stat.at[xi], send_sems.at[d - 1], recv_sems.at[d - 1], y, (xi + d) % 4) for d in range(1, 4)]


def put_stats(values, stat, xi):
    mean_own = jnp.sum(values, axis=1, keepdims=True) / values.shape[1]
    diff = values - mean_own
    stat[xi] = to_lanes(mean_own, jnp.sum(diff * diff, axis=1, keepdims=True))


def take_stats(stat, rows, share):
    tiles = [stat[i] for i in range(4)]
    mean_all = sum(t[0:1] for t in tiles) / 4
    spread = sum(t[1:2] for t in tiles) + share * sum((t[0:1] - mean_all) * (t[0:1] - mean_all) for t in tiles)
    mean_col, rstd_col = to_columns(mean_all, lax.rsqrt(spread / (share * 4) + EPS))
    return mean_col[:rows], rstd_col[:rows]


FC = 512
WB = 1024
RING = 6
KVS = 3
VLIM = 121 * 2**19
HELD = 7


def step_kernel(lens, hid_h, gain_h, gain_fh, freq, wq, wk, wv, wg, wu, wo, wd, emb, k_hbm, v_hbm,
                kv_out, z_out, lse_out,
                hid, gain, gain_f, cos, sin, n_perm, ring, w_kv, part_q, ga_q, sb_q, gb_q, total, q_rot, q_full, q_heads, o_heads, kn, vn,
                pool, act, o_in, o_all, k_buf, v_buf, scores, probs, acc, y_got, r_buf, f_all, f_nat, e_tail,
                t_a, t_b, tg_a, tg_b, t_c, tg_c, top, mass_l, stat, stat_f, stat_z,
                i_sem, r_sem, kv_sem, tail_sem, k_sem, v_sem, a_s, a_r, b_s, b_r, m_s, m_r, p_s, p_r, q_s, q_r,
                o_s, o_r, y_s, y_r, f_s, f_r, st_s, st_r, sf_s, sf_r,
                la_s, la_r, lb_s, lb_r, lc_s, lc_r, ta_s, ta_r, tb_s, tb_r, tc_s, tc_r, sz_s, sz_r):
    y, xi, chip, core, partner, twin = place()
    width = n_perm.shape[1]
    hw = width // TWO
    qc, hd = wq.shape[1], wk.shape[1]
    heads = qc // hd
    steps = wg.shape[1] // FC
    seqs = q_heads.shape[0]
    length = k_buf.shape[1]
    share = emb.shape[0] // 4
    full = share // WB
    rest = share - full * WB
    mine = y * 4 + xi
    ready = enter([(y, (xi + d) % 4) for d in (1, TWO, 3)] + [(1 - y, (xi + d) % 4) for d in range(4)])

    def start(copies):
        for copy in copies:
            copy.start()

    inputs = [pltpu.make_async_copy(src, dst, i_sem.at[i])
              for i, (src, dst) in enumerate(((hid_h, hid), (gain_h, gain), (gain_fh, gain_f)))]
    start(inputs)

    def q_loads(s):
        return [pltpu.make_async_copy(wq.at[:, pl.ds((TWO * s + i) * FC, FC)], ring.at[s, i], r_sem.at[s, i]) for i in range(TWO)]

    def w_loads(j):
        cols = pl.ds(pl.multiple_of(j * FC, FC), FC)
        slot = (j + TWO) % RING
        return [pltpu.make_async_copy(w.at[:, cols], ring.at[slot, i], r_sem.at[slot, i]) for i, w in enumerate((wg, wu))]

    kv_w = [pltpu.make_async_copy(w, w_kv.at[:, pl.ds(i * hd, hd)], kv_sem.at[i]) for i, w in enumerate((wk, wv))]
    start(q_loads(0))
    start(q_loads(1))
    start(kv_w)
    for j in range(RING - 3):
        start(w_loads(j))

    nd, no = wd.shape[0] // WB, wo.shape[0] // WB
    np_ = nd + no
    e_base = (np_, TWO * np_ + TWO * full)
    c_base = TWO * np_ + 4 * full
    d_base = c_base + full
    items = d_base + full
    far, near = (1 - chip) * TWO, chip * TWO

    def block(src, row, t):
        slot = t % RING
        return [pltpu.make_async_copy(src.at[pl.ds(row, WB), pl.ds(i * hw, hw)], ring.at[slot, i], r_sem.at[slot, i])
                for i in range(TWO)]

    def emb_row(quarter, k):
        return pl.multiple_of(quarter * share + k * WB, PAIR)

    def load_item(t):
        for base in (0, np_ + TWO * full):
            @pl.when((t >= base) & (t < base + nd))
            def _(base=base):
                start(block(wd, pl.multiple_of((t - base) * WB, WB), t))

            @pl.when((t >= base + nd) & (t < base + np_))
            def _(base=base):
                start(block(wo, pl.multiple_of((t - base - nd) * WB, WB), t))

        for base in e_base:
            @pl.when((t >= base) & (t < base + TWO * full))
            def _(base=base):
                k, own = (t - base) // TWO, (t - base) % TWO
                start(block(emb, emb_row(far + (1 - core) + own * (TWO * core - 1), k), t))

        @pl.when((t >= c_base) & (t < d_base))
        def _():
            start(block(emb, emb_row(near + 1 - core, t - c_base), t))

        @pl.when((t >= d_base) & (t < items))
        def _():
            start(block(emb, emb_row(near + core, t - d_base), t))

    def take_item(t):
        load_item(t + RING - 1)
        for copy in block(wd, 0, t):
            copy.wait()
        return t % RING

    def tail_load(i):
        quarter = (far + 1 - core, far + core, near + 1 - core, near + core)[i]
        rows = pl.ds(pl.multiple_of(quarter * share + full * WB, PAIR), rest)
        return pltpu.make_async_copy(emb.at[rows], e_tail.at[i], tail_sem.at[i])

    def cache_loads(b):
        slot = b % KVS
        return [pltpu.make_async_copy(k_hbm.at[b], k_buf.at[slot], k_sem.at[slot]),
                pltpu.make_async_copy(v_hbm.at[b], v_buf.at[slot], v_sem.at[slot])]

    def hop_a(j):
        return send(pool.at[pl.ds(TWO * j, TWO), 1 - core], pool.at[TWO * steps + j], a_s.at[j], a_r.at[j], y, partner)

    def sum_at(hf, p):
        return pool.at[3 * steps + hf * (steps // 4) + p // TWO, p % TWO]

    def got_at(hf, p):
        return pool.at[3 * steps + (TWO + hf) * (steps // 4) + p // TWO, p % TWO]

    def hop_b(hf, p):
        return send(sum_at(hf, p), got_at(hf, p), b_s.at[hf, p], b_r.at[hf, p], y, twin)

    def hop_m(hf, g):
        return send(act.at[hf, g, core, chip], act.at[hf, g, core, chip], m_s.at[hf, g], m_r.at[hf, g], y, twin)

    def hop_p(hf, g):
        return send(act.at[hf, g, core], act.at[hf, g, core], p_s.at[hf, g], p_r.at[hf, g], y, partner)

    q_cols = (pl.ds(0, TWO * FC), pl.ds(TWO * FC, qc + TWO * hd - TWO * FC))
    hop_qa = [send(part_q.at[:, 1 - core, :, :, cut], ga_q.at[..., cut], q_s.at[i, 0], q_r.at[i, 0], y, partner)
              for i, cut in enumerate(q_cols)]
    hop_qb = [send(sb_q.at[..., cut], gb_q.at[..., cut], q_s.at[i, 1], q_r.at[i, 1], y, twin) for i, cut in enumerate(q_cols)]

    def pair_queries(i):
        hop_qa[i].wait_recv()
        sb_q[:, :, q_cols[i]] = part_q[:, core, 1 - chip, :, q_cols[i]] + ga_q[:, 1 - chip, :, q_cols[i]]
        hop_qb[i].start()

    hop_qc = send(q_rot.at[1 - y], q_full.at[y], q_s.at[0, TWO], q_r.at[0, TWO], 1 - y, xi)

    def hop_o(hf, n):
        if n == 0:
            return send(o_in.at[1 - y, hf], o_all.at[hf, core, chip, y], o_s.at[hf, 0], o_r.at[hf, 0], 1 - y, xi)
        if n == 1:
            return send(o_all.at[hf, core, chip], o_all.at[hf, core, chip], o_s.at[hf, 1], o_r.at[hf, 1], y, twin)
        return send(o_all.at[hf, core], o_all.at[hf, core], o_s.at[hf, TWO], o_r.at[hf, TWO], y, partner)

    def hop_y(hf):
        return send(acc.at[hf, :, 1 - y], y_got.at[hf], y_s.at[hf], y_r.at[hf], 1 - y, xi)

    def hop_f(hf):
        return send(f_all.at[hf, y], f_all.at[hf, y], f_s.at[hf], f_r.at[hf], 1 - y, xi)

    def turns(owner):
        row = lax.broadcasted_iota(jnp.int32, (OWN, hd), 0)
        pos = functools.reduce(lambda acc_, r: jnp.where(row == r, lens[owner * OWN + r], acc_), range(OWN), jnp.zeros((OWN, hd), jnp.int32))
        angle = pos.astype(F32) * freq[...]
        lane = lax.broadcasted_iota(jnp.int32, (OWN, hd), 1)
        return jnp.cos(angle), jnp.where(lane < hd // TWO, -jnp.sin(angle), jnp.sin(angle))

    for load in inputs:
        load.wait()
    h = hid[...].astype(F32).reshape(LANES, width)
    put_stats(h, stat, xi)
    ready()
    first = stat_hops(stat, y, xi, st_s, st_r)
    start(first)
    for copy in first:
        copy.wait()
    mean, rstd = take_stats(stat, LANES, width)
    normed = ((h - mean) * rstd * gain[...]).astype(BF16)
    for hf in range(TWO):
        for core_o in range(TWO):
            for chip_o in range(TWO):
                for y_o in range(TWO):
                    src = (y_o * 4 + chip_o * TWO + core_o) * OWN + hf * 8
                    dst = hf * HALF + core_o * PAIR + chip_o * OWN + y_o * 8
                    n_perm[dst:dst + 8, :] = normed[src:src + 8, :]

    for s in range(TWO):
        for i, load in enumerate(q_loads(s)):
            load.wait()
            prod = jnp.dot(n_perm[...], ring[s, i], preferred_element_type=F32)
            part_q[:, :, :, :, (TWO * s + i) * FC:(TWO * s + i + 1) * FC] = prod.reshape(TWO, TWO, TWO, OWN, FC)
        start(w_loads(RING - 3 + s))
        if s == 0:
            hop_qa[0].start()
    for load in kv_w:
        load.wait()
    part_q[..., qc:] = jnp.dot(n_perm[...], w_kv[...], preferred_element_type=F32).reshape(TWO, TWO, TWO, OWN, TWO * hd)
    hop_qa[1].start()
    pair_queries(0)

    def rotate_queries():
        hop_qb[0].wait_recv()
        hop_qb[1].wait_recv()
        both = part_q[:, core, chip] + ga_q[:, chip] + gb_q[...]
        total[...] = both.astype(BF16).astype(F32).reshape(TWO, TWO, 8, qc + TWO * hd)
        for y_o in range(TWO):
            cos_r, sin_r = cos[y_o], sin[y_o]
            for head in range(heads):
                val = total[:, y_o, :, head * hd:(head + 1) * hd].reshape(OWN, hd)
                q_rot[y_o, :, head * hd:(head + 1) * hd] = (val * cos_r + pltpu.roll(val, hd // TWO, 1) * sin_r).astype(BF16)
        hop_qc.start()
        key = total[:, y, :, qc:qc + hd].reshape(OWN, hd)
        value = total[:, y, :, qc + hd:].reshape(OWN, hd)
        key = (key * cos[y] + pltpu.roll(key, hd // TWO, 1) * sin[y]).astype(BF16)
        kv_out[0] = key
        kv_out[1] = value.astype(BF16)
        kn[:, 0, :] = key.astype(F32)
        vn[:, 0, :] = value
        q_full[y] = q_rot[y]

    def spread_queries():
        hop_qc.wait_recv()
        for y_o in range(TWO):
            for head in range(heads):
                q_heads[:, y_o * heads + head, :] = q_full[y_o, :, head * hd:(head + 1) * hd].astype(F32)

    def add_pair(j):
        hop_a(j).wait_recv()
        for hf in range(TWO):
            sum_at(hf, j // TWO)[j % TWO] = pool[TWO * j + hf, core, 1 - chip] + pool[TWO * steps + j, hf, 1 - chip]

        @pl.when(j % TWO == 1)
        def _():
            hop_b(0, j // TWO).start()

    def project(j, carry):
        @pl.when(j + RING - 1 < steps)
        def _():
            start(w_loads(j + RING - 1))

        slot = (j + TWO) % RING
        for i, load in enumerate(w_loads(j)):
            load.wait()
            prod = jnp.dot(n_perm[...], ring[slot, i], preferred_element_type=F32)
            pool[pl.ds(TWO * j, TWO), :, :, :, i * FC:(i + 1) * FC] = prod.reshape(TWO, TWO, TWO, OWN, FC)
        hop_a(j).start()

        @pl.when(j == 0)
        def _():
            pair_queries(1)

        @pl.when(j >= 1)
        def _():
            add_pair(j - 1)

        @pl.when((j == TWO) | (j == 3))
        def _():
            cos[j - TWO], sin[j - TWO] = turns((j - TWO) * 4 + chip * TWO + core)

        @pl.when(j == 4)
        def _():
            for b in range(KVS):
                start(cache_loads(b))

        @pl.when(j == 8)
        def _():
            rotate_queries()

        @pl.when(j == 12)
        def _():
            spread_queries()
        return carry

    lax.fori_loop(0, steps, project, 0)
    add_pair(steps - 1)
    for t in range(RING - 1):
        start(block(wd, t * WB, t))
    for i in range(4):
        tail_load(i).start()

    def activate(hf, p):
        hop_b(hf, p).wait_recv()
        for i in range(TWO):
            j = TWO * p + i
            both = pool[TWO * j + hf, core, chip] + pool[TWO * steps + j, hf, chip] + got_at(hf, p)[i]
            gate = both[:, :FC].astype(BF16).astype(F32)
            up_val = both[:, FC:].astype(BF16).astype(F32)
            cols = pl.ds(pl.multiple_of(((p % 4) * TWO + i) * FC, FC), FC)
            act[hf, p // 4, core, chip, :, cols] = (jax.nn.silu(gate) * up_val).astype(BF16)

        @pl.when(p % 4 == 3)
        def _():
            hop_m(hf, p // 4).start()

    part_len = 1024

    def attend(b):
        slot = b % KVS
        scale = hd ** -0.5
        q32 = q_heads[b]
        q = q32.astype(BF16)
        limit = lens[mine * OWN + b]
        s_new = jnp.sum(q32 * kn[b], axis=1, keepdims=True) * scale
        load_k, load_v = cache_loads(b)
        load_k.wait()
        high = None
        for i in range(length // part_len):
            rows = slice(i * part_len, (i + 1) * part_len)
            s = lax.dot_general(q, k_buf[slot, rows], (((1,), (1,)), ((), ())), preferred_element_type=F32) * scale
            pos = lax.broadcasted_iota(jnp.int32, s.shape, 1) + i * part_len
            s = jnp.where(pos < limit, s, -jnp.inf)
            scores[:, rows] = s
            for c in range(0, part_len, LANES):
                high = s[:, c:c + LANES] if high is None else jnp.maximum(high, s[:, c:c + LANES])
        best = jnp.maximum(jnp.max(high, axis=1, keepdims=True), s_new)
        mass = None
        for i in range(length // part_len):
            rows = slice(i * part_len, (i + 1) * part_len)
            e = jnp.exp(scores[:, rows] - best)
            scores[:, rows] = e
            for c in range(0, part_len, LANES):
                mass = e[:, c:c + LANES] if mass is None else mass + e[:, c:c + LANES]
        e_new = jnp.exp(s_new - best)
        inv = 1.0 / (jnp.sum(mass, axis=1, keepdims=True) + e_new)
        for i in range(length // part_len):
            rows = slice(i * part_len, (i + 1) * part_len)
            probs[:, rows] = (scores[:, rows] * inv).astype(BF16)
        load_v.wait()
        o = jnp.dot(probs[...], v_buf[slot], preferred_element_type=F32)
        o = o + (e_new * inv).astype(BF16).astype(F32) * vn[b]
        o_heads[b] = o.astype(BF16).astype(F32)

        @pl.when(b + KVS < seqs)
        def _():
            start(cache_loads(b + KVS))

    def send_heads(hf):
        for y_o in range(TWO):
            for head in range(heads):
                o_in[y_o, hf, :, head * hd:(head + 1) * hd] = o_heads[hf * 8:hf * 8 + 8, y_o * heads + head, :].astype(BF16)
        o_all[hf, core, chip, y] = o_in[y, hf]
        hop_o(hf, 0).start()

    def contract(hf):
        base = hf * (np_ + TWO * full)
        acc[hf] = jnp.zeros(acc.shape[1:], F32)

        def add(t, left):
            slot = take_item(t)
            for i in range(TWO):
                prod = jnp.dot(left, ring[slot, i], preferred_element_type=F32)
                acc[hf, :, :, :, i * hw:(i + 1) * hw] += prod.reshape(4, TWO, 8, hw)

        for g in range(TWO):
            hop_p(hf, g).wait_recv()

            def from_act(i, carry):
                add(base + g * (nd // TWO) + i, act[hf, g, :, :, :, pl.ds(pl.multiple_of(i * WB, WB), WB)].reshape(HALF, WB))
                return carry

            lax.fori_loop(0, nd // TWO, from_act, 0)
        hop_o(hf, TWO).wait_recv()

        def from_heads(i, carry):
            add(base + nd + i, o_all[hf, :, :, :, :, pl.ds(pl.multiple_of(i * WB, WB), WB)].reshape(HALF, WB))
            return carry

        lax.fori_loop(0, no, from_heads, 0)

    def finish_sum(hf):
        hop_y(hf).wait_recv()
        res = [hid[y * 4 + (i % 2) * 2 + i // 2, hf * 8:hf * 8 + 8].astype(F32) for i in range(4)]
        branch = acc[hf, :, y] + y_got[hf]
        r_buf[...] = jnp.concatenate(res, axis=0) + branch.reshape(PAIR, width)
        put_stats(r_buf[...], stat_f.at[hf], xi)
        start(stat_hops(stat_f.at[hf], y, xi, sf_s.at[hf], sf_r.at[hf]))

    def finish_norm(hf):
        for copy in stat_hops(stat_f.at[hf], y, xi, sf_s.at[hf], sf_r.at[hf]):
            copy.wait()
        mean, rstd = take_stats(stat_f.at[hf], PAIR, width)
        f = ((r_buf[...] - mean) * rstd * gain_f[...]).astype(BF16)
        for i in range(4):
            f_all[hf, y, (i % 2) * 2 + i // 2] = f[i * 8:(i + 1) * 8]
        hop_f(hf).start()

    def each(body, low, high):
        def step(p, carry):
            body(p)
            return carry

        lax.fori_loop(low, high, step, 0)

    def pass_m(hf):
        for g in range(TWO):
            hop_m(hf, g).wait_recv()
            hop_p(hf, g).start()

    def pass_o(hf, n):
        hop_o(hf, n).wait_recv()
        hop_o(hf, n + 1).start()

    def mix(i):
        pl.when(i == 8)(lambda: send_heads(0))
        attend(i)
        pl.when(i < 8)(lambda: activate(0, i))

        pl.when((i == 5) | (i == 7))(lambda: hop_b(1, (i - 5) // 2).start())

        @pl.when(i == 8)
        def _():
            pass_o(0, 0)
            each(lambda p: hop_b(1, p).start(), 2, HELD)

        pl.when(i == 10)(lambda: pass_m(0))
        pl.when(i == 11)(lambda: pass_o(0, 1))

        @pl.when(i == 12)
        def _():
            each(lambda j: hop_a(j).wait_send(), 0, steps)
            each(lambda p: hop_b(0, p).wait_send(), 0, 8)
            contract(0)
            hop_y(0).start()
            each(lambda p: activate(1, p), 0, 2)

        @pl.when(i == 13)
        def _():
            finish_sum(0)
            each(lambda p: hop_b(1, p).start(), HELD, 8)

        @pl.when(i == 14)
        def _():
            finish_norm(0)
            each(lambda p: activate(1, p), 2, 4)

    each(mix, 0, seqs)
    each(lambda p: activate(1, p), 4, 8)
    hop_f(0).wait_recv()
    send_heads(1)

    def out_at(hf, k):
        return 56 - hf * 6 + k

    def in_at(hf, k):
        return PAIR + k if hf else 20 + TWO * k

    def lhop_a(hf, k):
        return send(pool.at[k], pool.at[8 + TWO * k], la_s.at[hf, k], la_r.at[hf, k], y, partner)

    def lhop_b(hf, k):
        return send(pool.at[out_at(hf, k)], pool.at[in_at(hf, k)], lb_s.at[hf, k], lb_r.at[hf, k], y, twin)

    def lhop_c(k):
        return send(pool.at[pl.ds(6 + TWO * k, TWO)], pool.at[pl.ds(38 + TWO * k, TWO)], lc_s.at[k], lc_r.at[k], y, partner)

    def thop_a(hf):
        return send(t_a.at[hf], tg_a.at[hf], ta_s.at[hf], ta_r.at[hf], y, partner)

    def thop_b(hf):
        return send(t_b.at[hf], tg_b.at[hf], tb_s.at[hf], tb_r.at[hf], y, twin)

    thop_c = send(t_c, tg_c, tc_s.at[0], tc_r.at[0], y, partner)
    nt = (((1,), (1,)), ((), ()))

    def product(left, slot, n):
        rows = slice(n * hw, (n + 1) * hw)
        return (lax.dot_general(left[:, :hw], ring[slot, 0, rows], nt, preferred_element_type=F32)
                + lax.dot_general(left[:, hw:], ring[slot, 1, rows], nt, preferred_element_type=F32))

    def tail_product(left, i):
        return lax.dot_general(left, e_tail[i], nt, preferred_element_type=F32)

    t_a[...] = jnp.zeros_like(t_a)
    t_b[...] = jnp.zeros_like(t_b)
    t_c[...] = jnp.zeros_like(t_c)

    def outward(hf):
        def chunk(k):
            left = f_all[hf].reshape(HALF, width)
            if hf == 1:
                lhop_a(0, k).wait_send()
            slot = take_item(e_base[hf] + TWO * k)
            for n in range(TWO):
                pool[k, :, :, :, n * hw:(n + 1) * hw] = product(left, slot, n).reshape(TWO, TWO, OWN, hw)
            lhop_a(hf, k).start()
            slot = take_item(e_base[hf] + TWO * k + 1)
            for n in range(TWO):
                pool[out_at(hf, k), :, :, :, n * hw:(n + 1) * hw] = product(left, slot, n).reshape(TWO, TWO, OWN, hw)
            lhop_a(hf, k).wait_recv()
            pool[out_at(hf, k)] += pool[8 + TWO * k]
            if hf == 0:
                pl.when(k < full - TWO)(lambda: lhop_b(0, k).start())

                pl.when(k == 0)(lambda: pass_o(1, 0))
            else:
                lhop_b(1, k).start()

        each(chunk, 0, full)
        left = f_all[hf].reshape(HALF, width)
        if hf == 0:
            tail_load(0).wait()
            tail_load(1).wait()
        t_a[hf, :, :rest] = tail_product(left, 0)
        thop_a(hf).start()
        t_b[hf, :, :rest] = tail_product(left, 1)
        thop_a(hf).wait_recv()
        t_b[hf] += tg_a[hf]
        if hf == 1:
            thop_b(1).start()

    outward(0)
    pass_m(1)
    pass_o(1, 1)
    each(lambda p: hop_b(1, p).wait_send(), 0, 8)
    contract(1)
    hop_y(1).start()
    finish_sum(1)
    each(lambda k: lhop_b(0, k).start(), full - 2, full)
    thop_b(0).start()
    finish_norm(1)
    hop_f(1).wait_recv()
    outward(1)

    for g in range(8):
        for hf in range(TWO):
            f_nat[g * OWN + hf * 8:g * OWN + hf * 8 + 8, :] = f_all[hf, g // 4, g % 4]

    def inward(k, carry):
        slot = take_item(c_base + k)
        for n in range(TWO):
            pool[pl.ds(6 + TWO * k, TWO), :, :, :, n * hw:(n + 1) * hw] = product(f_nat[...], slot, n).reshape(TWO, TWO, TWO, OWN, hw)
        lhop_c(k).start()
        return carry

    lax.fori_loop(0, full, inward, 0)
    tail_load(TWO).wait()
    t_c[:, :rest] = tail_product(f_nat[...], TWO)
    thop_c.start()
    tail_load(3).wait()

    top[...] = jnp.full_like(top, LOW)
    mass_l[...] = jnp.zeros_like(mass_l)

    def fold(z):
        tiles = [z[:, i:i + LANES] for i in range(0, z.shape[1], LANES)]
        high = functools.reduce(jnp.maximum, tiles, top[...])
        mass_l[...] = mass_l[...] * jnp.exp(top[...] - high) + sum(jnp.exp(g - high) for g in tiles)
        top[...] = high

    def weave(first, second):
        n = first.shape[-1]
        return jnp.stack([first.reshape(8, 8, n), second.reshape(8, 8, n)], axis=1).reshape(LANES, n)

    def finish(k):
        slot = take_item(d_base + k)
        lhop_c(k).wait_recv()
        here = pl.ds(38 + TWO * k, TWO)
        for n in range(TWO):
            cols = slice(n * hw, (n + 1) * hw)
            pool[here, :, :, :, cols] += product(f_nat[...], slot, n).reshape(TWO, TWO, TWO, OWN, hw)
        lhop_b(0, k).wait_recv()
        lhop_b(1, k).wait_recv()
        for n in range(TWO):
            cols = slice(n * hw, (n + 1) * hw)
            z = pool[here, :, :, :, cols].reshape(LANES, hw)
            z = z + weave(pool[in_at(0, k), :, :, :, cols], pool[in_at(1, k), :, :, :, cols])
            z_out[pl.ds(pl.multiple_of(k * WB + n * hw, hw), hw), :] = z.T
            fold(z)

    thop_c.wait_recv()
    tg_c[:, :rest] += tail_product(f_nat[...], 3)
    each(finish, 0, full)
    thop_b(0).wait_recv()
    thop_b(1).wait_recv()
    z_tail = tg_c[...] + weave(tg_b[0], tg_b[1])
    lane = lax.broadcasted_iota(jnp.int32, z_tail.shape, 1)
    fold(jnp.where(lane < rest, z_tail, LOW))
    z_out[full * WB:, :] = z_tail.T[:rest]

    high = jnp.max(top[...], axis=1, keepdims=True)
    stat_z[mine] = to_lanes(high, jnp.sum(mass_l[...] * jnp.exp(top[...] - high), axis=1, keepdims=True))
    copies = []
    for dy in range(TWO):
        for d in range(4):
            if dy or d:
                i = dy * 4 + d - 1
                copies.append(send(stat_z.at[mine], stat_z.at[mine], sz_s.at[i], sz_r.at[i],
                                   y + dy * (1 - TWO * y), (xi + d) % 4))
    start(copies)
    for copy in copies:
        copy.wait()
    highs = [stat_z[i][0:1] for i in range(8)]
    best_all = functools.reduce(jnp.maximum, highs)
    lse_out[...] = best_all + jnp.log(sum(stat_z[i][1:TWO] * jnp.exp(highs[i] - best_all) for i in range(8)))

    def drain_logits(k, carry):
        lhop_a(1, k).wait_send()
        lhop_b(0, k).wait_send()
        lhop_b(1, k).wait_send()
        lhop_c(k).wait_send()
        return carry

    lax.fori_loop(0, full, drain_logits, 0)
    for hf in range(TWO):
        for g in range(TWO):
            hop_m(hf, g).wait_send()
            hop_p(hf, g).wait_send()
        for n in range(3):
            hop_o(hf, n).wait_send()
        for hop in (hop_y, hop_f, thop_a, thop_b):
            hop(hf).wait_send()
    for hop in (*hop_qa, *hop_qb, hop_qc, thop_c):
        hop.wait_send()


def step_call(lens, hid, gain, gain_f, freq, wq, wk, wv, wg, wu, wo, wd, emb, k_cache, v_cache):
    width = hid.shape[TWO]
    qc, hd = wq.shape[1], wk.shape[1]
    seqs, length, _ = k_cache.shape
    cols = qc + TWO * hd
    steps = wg.shape[1] // FC
    heads = TWO * qc // hd
    share = emb.shape[0] // QUAD
    full = share // WB
    rest = share - full * WB
    tail_w = -(-rest // LANES) * LANES
    vmem = pl.BlockSpec(memory_space=pltpu.VMEM)
    hbm = pl.BlockSpec(memory_space=pl.ANY)

    def f32(*shape):
        return pltpu.VMEM(shape, F32)

    def bf16(*shape):
        return pltpu.VMEM(shape, BF16)

    def dma(*shape):
        return pltpu.SemaphoreType.DMA(shape)

    return pl.pallas_call(
        step_kernel, name="step",
        out_shape=[bf16(TWO, OWN, hd), f32(share, LANES), f32(1, LANES)],
        in_specs=[pl.BlockSpec(memory_space=pltpu.SMEM)] + [hbm] * 3 + [vmem] + [hbm] * 10, out_specs=[vmem] * 3,
        scratch_shapes=[
            bf16(OCT, OWN, width), f32(1, width), f32(1, width), f32(TWO, OWN, hd), f32(TWO, OWN, hd),
            bf16(LANES, width), bf16(RING, TWO, width, FC), bf16(width, TWO * hd),
            f32(TWO, TWO, TWO, OWN, cols), f32(TWO, TWO, OWN, cols), f32(TWO, OWN, cols), f32(TWO, OWN, cols), f32(TWO, TWO, OCT, cols),
            bf16(TWO, OWN, qc), bf16(TWO, OWN, qc), f32(seqs, heads, hd), f32(seqs, heads, hd), f32(seqs, 1, hd), f32(seqs, 1, hd),
            f32(QUAD * steps, TWO, TWO, OWN, TWO * FC), bf16(TWO, TWO, TWO, TWO, OWN, steps // TWO * FC),
            bf16(TWO, TWO, OCT, qc), bf16(TWO, TWO, TWO, TWO, OCT, qc),
            bf16(KVS, length, hd), bf16(KVS, length, hd), f32(heads, length), bf16(heads, length),
            f32(TWO, QUAD, TWO, OCT, width), f32(TWO, QUAD, OCT, width), f32(PAIR, width), bf16(TWO, TWO, QUAD, OCT, width), bf16(LANES, width), bf16(QUAD, rest, width),
            f32(TWO, HALF, tail_w), f32(TWO, HALF, tail_w), f32(TWO, HALF, tail_w), f32(TWO, HALF, tail_w), f32(LANES, tail_w), f32(LANES, tail_w),
            f32(LANES, LANES), f32(LANES, LANES), f32(QUAD, OCT, LANES), f32(TWO, QUAD, OCT, LANES), f32(OCT, OCT, LANES),
            dma(3), dma(RING, TWO), dma(TWO), dma(QUAD), dma(KVS), dma(KVS), dma(steps), dma(steps), dma(TWO, steps // TWO), dma(TWO, steps // TWO),
            dma(TWO, TWO), dma(TWO, TWO), dma(TWO, TWO), dma(TWO, TWO), dma(TWO, 3), dma(TWO, 3),
            dma(TWO, 3), dma(TWO, 3), dma(TWO), dma(TWO), dma(TWO), dma(TWO), dma(3), dma(3), dma(TWO, 3), dma(TWO, 3),
            dma(TWO, full), dma(TWO, full), dma(TWO, full), dma(TWO, full), dma(full), dma(full),
            dma(TWO), dma(TWO), dma(TWO), dma(TWO), dma(1), dma(1), dma(7), dma(7)],
        compiler_params=pltpu.CompilerParams(collective_id=0, has_side_effects=True, vmem_limit_bytes=VLIM),
    )(lens, hid, gain, gain_f, freq, wq, wk, wv, wg, wu, wo, wd, emb, k_cache, v_cache)


def close_kernel(z, lse, kv, out, k_out, v_out, lse_out, buf, out_sem):
    parts = buf.shape[0]
    rows = buf.shape[1]
    stores = [pltpu.make_async_copy(buf.at[i], out.at[pl.ds(i * rows, rows)], out_sem.at[i]) for i in range(parts)]
    for i in range(parts):
        buf[i] = z[i * rows:(i + 1) * rows, :] - lse[...]
        stores[i].start()
    k_out[...] = kv[0]
    v_out[...] = kv[1]
    lse_out[...] = lse[...]
    for store in stores:
        store.wait()


def close_call(z, lse, kv):
    share, rows = z.shape
    parts = 4
    vmem = pl.BlockSpec(memory_space=pltpu.VMEM)
    hbm = pl.BlockSpec(memory_space=pl.ANY)
    small = jax.ShapeDtypeStruct(kv.shape[1:], BF16)
    return pl.pallas_call(
        close_kernel, name="close",
        out_shape=[jax.ShapeDtypeStruct((share, rows), F32), small, small, jax.ShapeDtypeStruct((1, rows), F32)],
        in_specs=[vmem] * 3, out_specs=[hbm, vmem, vmem, vmem],
        scratch_shapes=[pltpu.VMEM((parts, share // parts, rows), F32), pltpu.SemaphoreType.DMA((parts,))],
        compiler_params=pltpu.CompilerParams(vmem_limit_bytes=16 * 2**20),
    )(z, lse, kv)


def solution(mesh):
    row_spec = P(("dp", "yax", "xax"))

    def local_step(hidden, cache_len, k_cache, v_cache, g_attn, w_query, w_key, w_value,
                   w_gate, w_up, w_out, w_down, g_final, embedding):
        width = hidden.shape[1]
        own_rows, _, head_dim = k_cache.shape
        half = head_dim // TWO
        lane = jnp.arange(head_dim)
        inv_freq = ROPE_BASE ** (-((lane % half).astype(F32) * 2.0) / head_dim)
        kv_new, logits_t, log_norm = step_call(
            cache_len, hidden.reshape(8, own_rows, width), g_attn[None], g_final[None], inv_freq[None],
            w_query, w_key, w_value, w_gate, w_up, w_out, w_down, embedding, k_cache, v_cache)
        log_probs, key_own, value_own, log_norm = close_call(logits_t, log_norm, kv_new)
        return key_own, value_own, log_probs.T, log_norm[0]

    in_specs = (P("dp", "xax"), P("dp"), row_spec, row_spec, P("xax"), P("xax", "yax"),
                P("xax", None), P("xax", None), P("xax", "yax"), P("xax", "yax"),
                P("yax", "xax"), P("yax", "xax"), P("xax"), P("yax", "xax"))
    out_specs = (row_spec, row_spec, P("dp", ("yax", "xax")), P("dp"))
    return jax.shard_map(local_step, mesh=mesh, in_specs=in_specs, out_specs=out_specs, check_vma=False)
```

```python
import functools

import jax
import jax.numpy as jnp
from jax import lax
from jax.experimental import pallas as pl
from jax.experimental.pallas import tpu as pltpu
from jax.sharding import PartitionSpec as P

EPS = 1e-6
ROPE_BASE = 10000.0
MESH = pl.DeviceIdType.MESH
F32 = jnp.float32
BF16 = jnp.bfloat16
LOW = -3e38
TWO, QUAD, OCT, OWN, PAIR, HALF, LANES = 2, 4, 8, 16, 32, 64, 128


def place():
    y = lax.axis_index("yax")
    xi = lax.axis_index("xax")
    chip = xi // 2
    core = xi % 2
    return y, xi, chip, core, chip * 2 + (1 - core), (1 - chip) * 2 + core


def send(src, dst, send_sem, recv_sem, y, xi):
    return pltpu.make_async_remote_copy(src_ref=src, dst_ref=dst, send_sem=send_sem, recv_sem=recv_sem,
                                        device_id={"yax": y, "xax": xi}, device_id_type=MESH)


def enter(peers):
    barrier = pltpu.get_barrier_semaphore()
    for y, xi in peers:
        pl.semaphore_signal(barrier, inc=1, device_id={"yax": y, "xax": xi}, device_id_type=MESH)
    return lambda: pl.semaphore_wait(barrier, len(peers))


def to_lanes(first, second):
    rows = first.shape[0]
    lane = lax.broadcasted_iota(jnp.int32, (rows, 128), 1)
    tile = jnp.where(lane == 0, first, jnp.where(lane == 1, second, 0.0))
    if rows < 128:
        tile = jnp.concatenate([tile, jnp.zeros((128 - rows, 128), F32)], axis=0)
    return tile.T[:8]


def to_columns(first, second):
    row = lax.broadcasted_iota(jnp.int32, (128, 128), 0)
    tile = jnp.where(row == 0, first, jnp.where(row == 1, second, 0.0)).T
    return tile[:, 0:1], tile[:, 1:2]


def stat_hops(stat, y, xi, send_sems, recv_sems):
    return [send(stat.at[xi], stat.at[xi], send_sems.at[d - 1], recv_sems.at[d - 1], y, (xi + d) % 4) for d in range(1, 4)]


def put_stats(values, stat, xi):
    mean_own = jnp.sum(values, axis=1, keepdims=True) / values.shape[1]
    diff = values - mean_own
    stat[xi] = to_lanes(mean_own, jnp.sum(diff * diff, axis=1, keepdims=True))


def take_stats(stat, rows, share):
    tiles = [stat[i] for i in range(4)]
    mean_all = sum(t[0:1] for t in tiles) / 4
    spread = sum(t[1:2] for t in tiles) + share * sum((t[0:1] - mean_all) * (t[0:1] - mean_all) for t in tiles)
    mean_col, rstd_col = to_columns(mean_all, lax.rsqrt(spread / (share * 4) + EPS))
    return mean_col[:rows], rstd_col[:rows]


FC = 512
WB = 1024
RING = 6
KVS = 3
VLIM = 121 * 2**19
HELD = 7


def step_kernel(lens, hid_h, gain_h, gain_fh, freq, wq, wk, wv, wg, wu, wo, wd, emb, k_hbm, v_hbm,
                kv_out, z_out, lse_out,
                hid, gain, gain_f, cos, sin, n_perm, ring, w_kv, part_q, ga_q, sb_q, gb_q, total, q_rot, q_full, q_heads, o_heads, kn, vn,
                pool, act, o_in, o_all, k_buf, v_buf, scores, probs, acc, y_got, r_buf, f_all, f_nat, e_tail,
                t_a, t_b, t_x, tg_a, tg_b, t_c, tg_c, top, mass_l, stat, stat_f, stat_z,
                i_sem, r_sem, kv_sem, tail_sem, k_sem, v_sem, a_s, a_r, b_s, b_r, m_s, m_r, p_s, p_r, q_s, q_r,
                o_s, o_r, y_s, y_r, f_s, f_r, st_s, st_r, sf_s, sf_r,
                la_s, la_r, lb_s, lb_r, lc_s, lc_r, ta_s, ta_r, tb_s, tb_r, tc_s, tc_r, sz_s, sz_r):
    y, xi, chip, core, partner, twin = place()
    width = n_perm.shape[1]
    hw = width // TWO
    qc, hd = wq.shape[1], wk.shape[1]
    heads = qc // hd
    steps = wg.shape[1] // FC
    seqs = q_heads.shape[0]
    length = k_buf.shape[1]
    share = emb.shape[0] // 4
    full = share // WB
    rest = share - full * WB
    mine = y * 4 + xi
    ready = enter([(y, (xi + d) % 4) for d in (1, TWO, 3)] + [(1 - y, (xi + d) % 4) for d in range(4)])

    def start(copies):
        for copy in copies:
            copy.start()

    inputs = [pltpu.make_async_copy(src, dst, i_sem.at[i])
              for i, (src, dst) in enumerate(((hid_h, hid), (gain_h, gain), (gain_fh, gain_f)))]
    start(inputs)

    def q_loads(s):
        return [pltpu.make_async_copy(wq.at[:, pl.ds((TWO * s + i) * FC, FC)], ring.at[s, i], r_sem.at[s, i]) for i in range(TWO)]

    def w_loads(j):
        cols = pl.ds(pl.multiple_of(j * FC, FC), FC)
        slot = (j + TWO) % RING
        return [pltpu.make_async_copy(w.at[:, cols], ring.at[slot, i], r_sem.at[slot, i]) for i, w in enumerate((wg, wu))]

    kv_w = [pltpu.make_async_copy(w, w_kv.at[:, pl.ds(i * hd, hd)], kv_sem.at[i]) for i, w in enumerate((wk, wv))]
    for load in inputs:
        load.wait()
    start(q_loads(0))
    start(q_loads(1))
    start(kv_w)
    for j in range(RING - 3):
        start(w_loads(j))

    nd, no = wd.shape[0] // WB, wo.shape[0] // WB
    np_ = nd + no
    e_base = (np_, TWO * np_ + TWO * full)
    c_base = TWO * np_ + 4 * full
    d_base = c_base + full
    items = d_base + full
    far, near = (1 - chip) * TWO, chip * TWO

    def block(src, row, t):
        slot = t % RING
        return [pltpu.make_async_copy(src.at[pl.ds(row, WB), pl.ds(i * hw, hw)], ring.at[slot, i], r_sem.at[slot, i])
                for i in range(TWO)]

    def emb_row(quarter, k):
        return pl.multiple_of(quarter * share + k * WB, PAIR)

    def load_item(t):
        for base in (0, np_ + TWO * full):
            @pl.when((t >= base) & (t < base + nd))
            def _(base=base):
                start(block(wd, pl.multiple_of((t - base) * WB, WB), t))

            @pl.when((t >= base + nd) & (t < base + np_))
            def _(base=base):
                start(block(wo, pl.multiple_of((t - base - nd) * WB, WB), t))

        for base in e_base:
            @pl.when((t >= base) & (t < base + TWO * full))
            def _(base=base):
                k, own = (t - base) // TWO, (t - base) % TWO
                start(block(emb, emb_row(far + (1 - core) + own * (TWO * core - 1), k), t))

        @pl.when((t >= c_base) & (t < d_base))
        def _():
            start(block(emb, emb_row(near + 1 - core, t - c_base), t))

        @pl.when((t >= d_base) & (t < items))
        def _():
            start(block(emb, emb_row(near + core, t - d_base), t))

    def take_item(t):
        load_item(t + RING - 1)
        for copy in block(wd, 0, t):
            copy.wait()
        return t % RING

    def tail_load(i):
        quarter = (far + 1 - core, far + core, near + 1 - core, near + core)[i]
        rows = pl.ds(pl.multiple_of(quarter * share + full * WB, PAIR), rest)
        return pltpu.make_async_copy(emb.at[rows], e_tail.at[i], tail_sem.at[i])

    def cache_loads(b):
        slot = b % KVS
        return [pltpu.make_async_copy(k_hbm.at[b], k_buf.at[slot], k_sem.at[slot]),
                pltpu.make_async_copy(v_hbm.at[b], v_buf.at[slot], v_sem.at[slot])]

    def hop_a(j):
        return send(pool.at[pl.ds(TWO * j, TWO), 1 - core], pool.at[TWO * steps + j], a_s.at[j], a_r.at[j], y, partner)

    def sum_at(hf, p):
        return pool.at[3 * steps + hf * (steps // 4) + p // TWO, p % TWO]

    def got_at(hf, p):
        return pool.at[3 * steps + (TWO + hf) * (steps // 4) + p // TWO, p % TWO]

    def hop_b(hf, p):
        return send(sum_at(hf, p), got_at(hf, p), b_s.at[hf, p], b_r.at[hf, p], y, twin)

    def hop_m(hf, g):
        return send(act.at[hf, g, core, chip], act.at[hf, g, core, chip], m_s.at[hf, g], m_r.at[hf, g], y, twin)

    def hop_p(hf, g):
        return send(act.at[hf, g, core], act.at[hf, g, core], p_s.at[hf, g], p_r.at[hf, g], y, partner)

    q_cols = (pl.ds(0, TWO * FC), pl.ds(TWO * FC, qc + TWO * hd - TWO * FC))
    hop_qa = [send(part_q.at[:, 1 - core, :, :, cut], ga_q.at[..., cut], q_s.at[i, 0], q_r.at[i, 0], y, partner)
              for i, cut in enumerate(q_cols)]
    hop_qb = [send(sb_q.at[..., cut], gb_q.at[..., cut], q_s.at[i, 1], q_r.at[i, 1], y, twin) for i, cut in enumerate(q_cols)]

    def pair_queries(i):
        hop_qa[i].wait_recv()
        sb_q[:, :, q_cols[i]] = part_q[:, core, 1 - chip, :, q_cols[i]] + ga_q[:, 1 - chip, :, q_cols[i]]
        hop_qb[i].start()

    hop_qc = send(q_rot.at[1 - y], q_full.at[y], q_s.at[0, TWO], q_r.at[0, TWO], 1 - y, xi)

    def hop_o(hf, n):
        if n == 0:
            return send(o_in.at[1 - y, hf], o_all.at[hf, core, chip, y], o_s.at[hf, 0], o_r.at[hf, 0], 1 - y, xi)
        if n == 1:
            return send(o_all.at[hf, core, chip], o_all.at[hf, core, chip], o_s.at[hf, 1], o_r.at[hf, 1], y, twin)
        return send(o_all.at[hf, core], o_all.at[hf, core], o_s.at[hf, TWO], o_r.at[hf, TWO], y, partner)

    def hop_y(hf):
        return send(acc.at[hf, :, 1 - y], y_got.at[hf], y_s.at[hf], y_r.at[hf], 1 - y, xi)

    def hop_f(hf):
        return send(f_all.at[hf, y], f_all.at[hf, y], f_s.at[hf], f_r.at[hf], 1 - y, xi)

    def turns(owner):
        row = lax.broadcasted_iota(jnp.int32, (OWN, hd), 0)
        pos = functools.reduce(lambda acc_, r: jnp.where(row == r, lens[owner * OWN + r], acc_), range(OWN), jnp.zeros((OWN, hd), jnp.int32))
        angle = pos.astype(F32) * freq[...]
        lane = lax.broadcasted_iota(jnp.int32, (OWN, hd), 1)
        return jnp.cos(angle), jnp.where(lane < hd // TWO, -jnp.sin(angle), jnp.sin(angle))

    h = hid[...].astype(F32).reshape(LANES, width)
    put_stats(h, stat, xi)
    ready()
    first = stat_hops(stat, y, xi, st_s, st_r)
    start(first)
    for copy in first:
        copy.wait()
    mean, rstd = take_stats(stat, LANES, width)
    normed = ((h - mean) * rstd * gain[...]).astype(BF16)
    for hf in range(TWO):
        for core_o in range(TWO):
            for chip_o in range(TWO):
                for y_o in range(TWO):
                    src = (y_o * 4 + chip_o * TWO + core_o) * OWN + hf * 8
                    dst = hf * HALF + core_o * PAIR + chip_o * OWN + y_o * 8
                    n_perm[dst:dst + 8, :] = normed[src:src + 8, :]

    for s in range(TWO):
        for i, load in enumerate(q_loads(s)):
            load.wait()
            prod = jnp.dot(n_perm[...], ring[s, i], preferred_element_type=F32)
            part_q[:, :, :, :, (TWO * s + i) * FC:(TWO * s + i + 1) * FC] = prod.reshape(TWO, TWO, TWO, OWN, FC)
        start(w_loads(RING - 3 + s))
        if s == 0:
            hop_qa[0].start()
    for load in kv_w:
        load.wait()
    part_q[..., qc:] = jnp.dot(n_perm[...], w_kv[...], preferred_element_type=F32).reshape(TWO, TWO, TWO, OWN, TWO * hd)
    hop_qa[1].start()
    pair_queries(0)

    def rotate_queries():
        hop_qb[0].wait_recv()
        hop_qb[1].wait_recv()
        both = part_q[:, core, chip] + ga_q[:, chip] + gb_q[...]
        total[...] = both.astype(BF16).astype(F32).reshape(TWO, TWO, 8, qc + TWO * hd)
        for y_o in range(TWO):
            cos_r, sin_r = cos[y_o], sin[y_o]
            for head in range(heads):
                val = total[:, y_o, :, head * hd:(head + 1) * hd].reshape(OWN, hd)
                q_rot[y_o, :, head * hd:(head + 1) * hd] = (val * cos_r + pltpu.roll(val, hd // TWO, 1) * sin_r).astype(BF16)
        hop_qc.start()
        key = total[:, y, :, qc:qc + hd].reshape(OWN, hd)
        value = total[:, y, :, qc + hd:].reshape(OWN, hd)
        key = (key * cos[y] + pltpu.roll(key, hd // TWO, 1) * sin[y]).astype(BF16)
        kv_out[0] = key
        kv_out[1] = value.astype(BF16)
        kn[:, 0, :] = key.astype(F32)
        vn[:, 0, :] = value
        q_full[y] = q_rot[y]

    def spread_queries():
        hop_qc.wait_recv()
        for y_o in range(TWO):
            for head in range(heads):
                q_heads[:, y_o * heads + head, :] = q_full[y_o, :, head * hd:(head + 1) * hd].astype(F32)

    def add_pair(j):
        hop_a(j).wait_recv()
        for hf in range(TWO):
            sum_at(hf, j // TWO)[j % TWO] = pool[TWO * j + hf, core, 1 - chip] + pool[TWO * steps + j, hf, 1 - chip]

        @pl.when(j % TWO == 1)
        def _():
            hop_b(0, j // TWO).start()

    def project(j, carry):
        @pl.when(j + RING - 1 < steps)
        def _():
            start(w_loads(j + RING - 1))

        slot = (j + TWO) % RING
        for i, load in enumerate(w_loads(j)):
            load.wait()
            prod = jnp.dot(n_perm[...], ring[slot, i], preferred_element_type=F32)
            pool[pl.ds(TWO * j, TWO), :, :, :, i * FC:(i + 1) * FC] = prod.reshape(TWO, TWO, TWO, OWN, FC)
        hop_a(j).start()

        @pl.when(j == 0)
        def _():
            pair_queries(1)

        @pl.when(j >= 1)
        def _():
            add_pair(j - 1)

        @pl.when((j == TWO) | (j == 3))
        def _():
            cos[j - TWO], sin[j - TWO] = turns((j - TWO) * 4 + chip * TWO + core)

        @pl.when(j == 4)
        def _():
            for b in range(KVS):
                start(cache_loads(b))

        @pl.when(j == 8)
        def _():
            rotate_queries()

        @pl.when(j == 12)
        def _():
            spread_queries()
        return carry

    lax.fori_loop(0, steps, project, 0)
    add_pair(steps - 1)
    for t in range(RING - 1):
        start(block(wd, t * WB, t))
    for i in range(4):
        tail_load(i).start()

    def activate(hf, p):
        hop_b(hf, p).wait_recv()
        for i in range(TWO):
            j = TWO * p + i
            both = pool[TWO * j + hf, core, chip] + pool[TWO * steps + j, hf, chip] + got_at(hf, p)[i]
            gate = both[:, :FC].astype(BF16).astype(F32)
            up_val = both[:, FC:].astype(BF16).astype(F32)
            cols = pl.ds(pl.multiple_of(((p % 4) * TWO + i) * FC, FC), FC)
            act[hf, p // 4, core, chip, :, cols] = (jax.nn.silu(gate) * up_val).astype(BF16)

        @pl.when(p % 4 == 3)
        def _():
            hop_m(hf, p // 4).start()

    part_len = 1024

    def attend(b):
        slot = b % KVS
        scale = hd ** -0.5
        q32 = q_heads[b]
        q = q32.astype(BF16)
        limit = lens[mine * OWN + b]
        s_new = jnp.sum(q32 * kn[b], axis=1, keepdims=True) * scale
        load_k, load_v = cache_loads(b)
        load_k.wait()
        high = None
        for i in range(length // part_len):
            rows = slice(i * part_len, (i + 1) * part_len)
            s = lax.dot_general(q, k_buf[slot, rows], (((1,), (1,)), ((), ())), preferred_element_type=F32) * scale
            pos = lax.broadcasted_iota(jnp.int32, s.shape, 1) + i * part_len
            s = jnp.where(pos < limit, s, -jnp.inf)
            scores[:, rows] = s
            for c in range(0, part_len, LANES):
                high = s[:, c:c + LANES] if high is None else jnp.maximum(high, s[:, c:c + LANES])
        best = jnp.maximum(jnp.max(high, axis=1, keepdims=True), s_new)
        mass = None
        for i in range(length // part_len):
            rows = slice(i * part_len, (i + 1) * part_len)
            e = jnp.exp(scores[:, rows] - best)
            scores[:, rows] = e
            for c in range(0, part_len, LANES):
                mass = e[:, c:c + LANES] if mass is None else mass + e[:, c:c + LANES]
        e_new = jnp.exp(s_new - best)
        inv = 1.0 / (jnp.sum(mass, axis=1, keepdims=True) + e_new)
        for i in range(length // part_len):
            rows = slice(i * part_len, (i + 1) * part_len)
            probs[:, rows] = (scores[:, rows] * inv).astype(BF16)
        load_v.wait()
        o = jnp.dot(probs[...], v_buf[slot], preferred_element_type=F32)
        o = o + (e_new * inv).astype(BF16).astype(F32) * vn[b]
        o_heads[b] = o.astype(BF16).astype(F32)

        @pl.when(b + KVS < seqs)
        def _():
            start(cache_loads(b + KVS))

    def send_heads(hf):
        for y_o in range(TWO):
            for head in range(heads):
                o_in[y_o, hf, :, head * hd:(head + 1) * hd] = o_heads[hf * 8:hf * 8 + 8, y_o * heads + head, :].astype(BF16)
        o_all[hf, core, chip, y] = o_in[y, hf]
        hop_o(hf, 0).start()

    def contract(hf):
        base = hf * (np_ + TWO * full)
        acc[hf] = jnp.zeros(acc.shape[1:], F32)

        def add(t, left):
            slot = take_item(t)
            for i in range(TWO):
                prod = jnp.dot(left, ring[slot, i], preferred_element_type=F32)
                acc[hf, :, :, :, i * hw:(i + 1) * hw] += prod.reshape(4, TWO, 8, hw)

        for g in range(TWO):
            hop_p(hf, g).wait_recv()

            def from_act(i, carry):
                add(base + g * (nd // TWO) + i, act[hf, g, :, :, :, pl.ds(pl.multiple_of(i * WB, WB), WB)].reshape(HALF, WB))
                return carry

            lax.fori_loop(0, nd // TWO, from_act, 0)
        hop_o(hf, TWO).wait_recv()

        def from_heads(i, carry):
            add(base + nd + i, o_all[hf, :, :, :, :, pl.ds(pl.multiple_of(i * WB, WB), WB)].reshape(HALF, WB))
            return carry

        lax.fori_loop(0, no, from_heads, 0)

    def finish_sum(hf):
        hop_y(hf).wait_recv()
        res = [hid[y * 4 + (i % 2) * 2 + i // 2, hf * 8:hf * 8 + 8].astype(F32) for i in range(4)]
        branch = acc[hf, :, y] + y_got[hf]
        r_buf[...] = jnp.concatenate(res, axis=0) + branch.reshape(PAIR, width)
        put_stats(r_buf[...], stat_f.at[hf], xi)
        start(stat_hops(stat_f.at[hf], y, xi, sf_s.at[hf], sf_r.at[hf]))

    def finish_norm(hf):
        for copy in stat_hops(stat_f.at[hf], y, xi, sf_s.at[hf], sf_r.at[hf]):
            copy.wait()
        mean, rstd = take_stats(stat_f.at[hf], PAIR, width)
        f = ((r_buf[...] - mean) * rstd * gain_f[...]).astype(BF16)
        for i in range(4):
            f_all[hf, y, (i % 2) * 2 + i // 2] = f[i * 8:(i + 1) * 8]
        hop_f(hf).start()

    def each(body, low, high):
        def step(p, carry):
            body(p)
            return carry

        lax.fori_loop(low, high, step, 0)

    def pass_m(hf):
        for g in range(TWO):
            hop_m(hf, g).wait_recv()
            hop_p(hf, g).start()

    def pass_o(hf, n):
        hop_o(hf, n).wait_recv()
        hop_o(hf, n + 1).start()

    def mix(i):
        pl.when(i == 8)(lambda: send_heads(0))
        attend(i)
        pl.when(i < 8)(lambda: activate(0, i))

        pl.when((i == 5) | (i == 7))(lambda: hop_b(1, (i - 5) // 2).start())

        @pl.when(i == 8)
        def _():
            pass_o(0, 0)
            each(lambda p: hop_b(1, p).start(), 2, HELD)

        pl.when(i == 10)(lambda: pass_m(0))
        pl.when(i == 11)(lambda: pass_o(0, 1))

        @pl.when(i == 12)
        def _():
            each(lambda j: hop_a(j).wait_send(), 0, steps)
            each(lambda p: hop_b(0, p).wait_send(), 0, 8)
            contract(0)
            hop_y(0).start()
            each(lambda p: activate(1, p), 0, 2)

        @pl.when(i == 13)
        def _():
            finish_sum(0)
            each(lambda p: hop_b(1, p).start(), HELD, 8)

        @pl.when(i == 14)
        def _():
            finish_norm(0)
            each(lambda p: activate(1, p), 2, 4)

    each(mix, 0, seqs)
    each(lambda p: activate(1, p), 4, 8)
    hop_f(0).wait_recv()
    send_heads(1)

    def out_at(hf, k):
        return 56 - hf * 6 + k

    def in_at(hf, k):
        return PAIR + k if hf else 20 + TWO * k

    def lhop_a(hf, k):
        return send(pool.at[k], pool.at[8 + TWO * k], la_s.at[hf, k], la_r.at[hf, k], y, partner)

    def lhop_b(hf, k):
        return send(pool.at[out_at(hf, k)], pool.at[in_at(hf, k)], lb_s.at[hf, k], lb_r.at[hf, k], y, twin)

    def lhop_c(k):
        return send(pool.at[pl.ds(6 + TWO * k, TWO)], pool.at[pl.ds(38 + TWO * k, TWO)], lc_s.at[k], lc_r.at[k], y, partner)

    def thop_a(hf):
        return send(t_a.at[hf], tg_a.at[hf], ta_s.at[hf], ta_r.at[hf], y, partner)

    def thop_b(hf):
        return send(t_x.at[hf], tg_b.at[hf], tb_s.at[hf], tb_r.at[hf], y, twin)

    thop_c = send(t_c, tg_c, tc_s.at[0], tc_r.at[0], y, partner)
    nt = (((1,), (1,)), ((), ()))

    def product(left, slot, n):
        rows = slice(n * hw, (n + 1) * hw)
        return (lax.dot_general(left[:, :hw], ring[slot, 0, rows], nt, preferred_element_type=F32)
                + lax.dot_general(left[:, hw:], ring[slot, 1, rows], nt, preferred_element_type=F32))

    def tail_product(left, i):
        return lax.dot_general(left, e_tail[i], nt, preferred_element_type=F32)

    t_a[...] = jnp.zeros_like(t_a)
    t_b[...] = jnp.zeros_like(t_b)
    t_c[...] = jnp.zeros_like(t_c)

    def outward(hf):
        def chunk(k):
            left = f_all[hf].reshape(HALF, width)
            if hf == 1:
                lhop_a(0, k).wait_send()
            slot = take_item(e_base[hf] + TWO * k)
            for n in range(TWO):
                pool[k, :, :, :, n * hw:(n + 1) * hw] = product(left, slot, n).reshape(TWO, TWO, OWN, hw)
            lhop_a(hf, k).start()
            slot = take_item(e_base[hf] + TWO * k + 1)
            for n in range(TWO):
                pool[out_at(hf, k), :, :, :, n * hw:(n + 1) * hw] = product(left, slot, n).reshape(TWO, TWO, OWN, hw)
            lhop_a(hf, k).wait_recv()
            pool[out_at(hf, k)] += pool[8 + TWO * k]
            if hf == 0:
                pl.when(k < full - TWO)(lambda: lhop_b(0, k).start())

                pl.when(k == 0)(lambda: pass_o(1, 0))
            else:
                lhop_b(1, k).start()

        each(chunk, 0, full)
        left = f_all[hf].reshape(HALF, width)
        if hf == 0:
            tail_load(0).wait()
            tail_load(1).wait()
        t_a[hf, :, :rest] = tail_product(left, 0)
        thop_a(hf).start()
        t_b[hf, :, :rest] = tail_product(left, 1)
        thop_a(hf).wait_recv()
        both = t_b[hf] + tg_a[hf]
        t_x[hf, :HALF] = both[:, :LANES]
        quarters = [both[i * OWN:(i + 1) * OWN, LANES:rest] for i in range(QUAD)]
        t_x[hf, HALF:] = jnp.concatenate(quarters, axis=1)
        if hf == 1:
            thop_b(1).start()

    outward(0)
    pass_m(1)
    pass_o(1, 1)
    each(lambda p: hop_b(1, p).wait_send(), 0, 8)
    contract(1)
    hop_y(1).start()
    finish_sum(1)
    each(lambda k: lhop_b(0, k).start(), full - 2, full)
    thop_b(0).start()
    finish_norm(1)
    hop_f(1).wait_recv()
    outward(1)

    for g in range(8):
        for hf in range(TWO):
            f_nat[g * OWN + hf * 8:g * OWN + hf * 8 + 8, :] = f_all[hf, g // 4, g % 4]

    def inward(k, carry):
        slot = take_item(c_base + k)
        for n in range(TWO):
            pool[pl.ds(6 + TWO * k, TWO), :, :, :, n * hw:(n + 1) * hw] = product(f_nat[...], slot, n).reshape(TWO, TWO, TWO, OWN, hw)
        lhop_c(k).start()
        return carry

    lax.fori_loop(0, full, inward, 0)
    tail_load(TWO).wait()
    t_c[:, :rest] = tail_product(f_nat[...], TWO)
    thop_c.start()
    tail_load(3).wait()

    top[...] = jnp.full_like(top, LOW)
    mass_l[...] = jnp.zeros_like(mass_l)

    def fold(z):
        tiles = [z[:, i:i + LANES] for i in range(0, z.shape[1], LANES)]
        high = functools.reduce(jnp.maximum, tiles, top[...])
        mass_l[...] = mass_l[...] * jnp.exp(top[...] - high) + sum(jnp.exp(g - high) for g in tiles)
        top[...] = high

    def weave(first, second):
        n = first.shape[-1]
        return jnp.stack([first.reshape(8, 8, n), second.reshape(8, 8, n)], axis=1).reshape(LANES, n)

    def finish(k):
        slot = take_item(d_base + k)
        lhop_c(k).wait_recv()
        here = pl.ds(38 + TWO * k, TWO)
        for n in range(TWO):
            cols = slice(n * hw, (n + 1) * hw)
            pool[here, :, :, :, cols] += product(f_nat[...], slot, n).reshape(TWO, TWO, TWO, OWN, hw)
        lhop_b(0, k).wait_recv()
        lhop_b(1, k).wait_recv()
        for n in range(TWO):
            cols = slice(n * hw, (n + 1) * hw)
            z = pool[here, :, :, :, cols].reshape(LANES, hw)
            z = z + weave(pool[in_at(0, k), :, :, :, cols], pool[in_at(1, k), :, :, :, cols])
            z_out[pl.ds(pl.multiple_of(k * WB + n * hw, hw), hw), :] = z.T
            fold(z)

    thop_c.wait_recv()
    tg_c[:, :rest] += tail_product(f_nat[...], 3)
    each(finish, 0, full)
    thop_b(0).wait_recv()
    thop_b(1).wait_recv()
    over = rest - LANES

    def unpack(block):
        edge = jnp.concatenate([block[HALF:, i * over:(i + 1) * over] for i in range(QUAD)], axis=0)
        return jnp.concatenate([block[:HALF], edge, jnp.zeros((HALF, LANES - over), F32)], axis=1)

    z_tail = tg_c[...] + weave(unpack(tg_b[0]), unpack(tg_b[1]))
    lane = lax.broadcasted_iota(jnp.int32, z_tail.shape, 1)
    fold(jnp.where(lane < rest, z_tail, LOW))
    z_out[full * WB:, :] = z_tail.T[:rest]

    high = jnp.max(top[...], axis=1, keepdims=True)
    stat_z[mine] = to_lanes(high, jnp.sum(mass_l[...] * jnp.exp(top[...] - high), axis=1, keepdims=True))
    copies = []
    for dy in range(TWO):
        for d in range(4):
            if dy or d:
                i = dy * 4 + d - 1
                copies.append(send(stat_z.at[mine], stat_z.at[mine], sz_s.at[i], sz_r.at[i],
                                   y + dy * (1 - TWO * y), (xi + d) % 4))
    start(copies)
    for copy in copies:
        copy.wait()
    highs = [stat_z[i][0:1] for i in range(8)]
    best_all = functools.reduce(jnp.maximum, highs)
    lse_out[...] = best_all + jnp.log(sum(stat_z[i][1:TWO] * jnp.exp(highs[i] - best_all) for i in range(8)))

    def drain_logits(k, carry):
        lhop_a(1, k).wait_send()
        lhop_b(0, k).wait_send()
        lhop_b(1, k).wait_send()
        lhop_c(k).wait_send()
        return carry

    lax.fori_loop(0, full, drain_logits, 0)
    for hf in range(TWO):
        for g in range(TWO):
            hop_m(hf, g).wait_send()
            hop_p(hf, g).wait_send()
        for n in range(3):
            hop_o(hf, n).wait_send()
        for hop in (hop_y, hop_f, thop_a, thop_b):
            hop(hf).wait_send()
    for hop in (*hop_qa, *hop_qb, hop_qc, thop_c):
        hop.wait_send()


def step_call(lens, hid, gain, gain_f, freq, wq, wk, wv, wg, wu, wo, wd, emb, k_cache, v_cache):
    width = hid.shape[TWO]
    qc, hd = wq.shape[1], wk.shape[1]
    seqs, length, _ = k_cache.shape
    cols = qc + TWO * hd
    steps = wg.shape[1] // FC
    heads = TWO * qc // hd
    share = emb.shape[0] // QUAD
    full = share // WB
    rest = share - full * WB
    tail_w = -(-rest // LANES) * LANES
    vmem = pl.BlockSpec(memory_space=pltpu.VMEM)
    hbm = pl.BlockSpec(memory_space=pl.ANY)

    def f32(*shape):
        return pltpu.VMEM(shape, F32)

    def bf16(*shape):
        return pltpu.VMEM(shape, BF16)

    def dma(*shape):
        return pltpu.SemaphoreType.DMA(shape)

    return pl.pallas_call(
        step_kernel, name="step",
        out_shape=[bf16(TWO, OWN, hd), f32(share, LANES), f32(1, LANES)],
        in_specs=[pl.BlockSpec(memory_space=pltpu.SMEM)] + [hbm] * 3 + [vmem] + [hbm] * 10, out_specs=[vmem] * 3,
        scratch_shapes=[
            bf16(OCT, OWN, width), f32(1, width), f32(1, width), f32(TWO, OWN, hd), f32(TWO, OWN, hd),
            bf16(LANES, width), bf16(RING, TWO, width, FC), bf16(width, TWO * hd),
            f32(TWO, TWO, TWO, OWN, cols), f32(TWO, TWO, OWN, cols), f32(TWO, OWN, cols), f32(TWO, OWN, cols), f32(TWO, TWO, OCT, cols),
            bf16(TWO, OWN, qc), bf16(TWO, OWN, qc), f32(seqs, heads, hd), f32(seqs, heads, hd), f32(seqs, 1, hd), f32(seqs, 1, hd),
            f32(QUAD * steps, TWO, TWO, OWN, TWO * FC), bf16(TWO, TWO, TWO, TWO, OWN, steps // TWO * FC),
            bf16(TWO, TWO, OCT, qc), bf16(TWO, TWO, TWO, TWO, OCT, qc),
            bf16(KVS, length, hd), bf16(KVS, length, hd), f32(heads, length), bf16(heads, length),
            f32(TWO, QUAD, TWO, OCT, width), f32(TWO, QUAD, OCT, width), f32(PAIR, width), bf16(TWO, TWO, QUAD, OCT, width), bf16(LANES, width), bf16(QUAD, rest, width),
            f32(TWO, HALF, tail_w), f32(TWO, HALF, tail_w), f32(TWO, HALF + OWN, LANES), f32(TWO, HALF, tail_w), f32(TWO, HALF + OWN, LANES), f32(LANES, tail_w), f32(LANES, tail_w),
            f32(LANES, LANES), f32(LANES, LANES), f32(QUAD, OCT, LANES), f32(TWO, QUAD, OCT, LANES), f32(OCT, OCT, LANES),
            dma(3), dma(RING, TWO), dma(TWO), dma(QUAD), dma(KVS), dma(KVS), dma(steps), dma(steps), dma(TWO, steps // TWO), dma(TWO, steps // TWO),
            dma(TWO, TWO), dma(TWO, TWO), dma(TWO, TWO), dma(TWO, TWO), dma(TWO, 3), dma(TWO, 3),
            dma(TWO, 3), dma(TWO, 3), dma(TWO), dma(TWO), dma(TWO), dma(TWO), dma(3), dma(3), dma(TWO, 3), dma(TWO, 3),
            dma(TWO, full), dma(TWO, full), dma(TWO, full), dma(TWO, full), dma(full), dma(full),
            dma(TWO), dma(TWO), dma(TWO), dma(TWO), dma(1), dma(1), dma(7), dma(7)],
        compiler_params=pltpu.CompilerParams(collective_id=0, has_side_effects=True, vmem_limit_bytes=VLIM),
    )(lens, hid, gain, gain_f, freq, wq, wk, wv, wg, wu, wo, wd, emb, k_cache, v_cache)


def close_kernel(z, lse, kv, out, k_out, v_out, lse_out, buf, out_sem):
    parts = buf.shape[0]
    rows = buf.shape[1]
    stores = [pltpu.make_async_copy(buf.at[i], out.at[pl.ds(i * rows, rows)], out_sem.at[i]) for i in range(parts)]
    for i in range(parts):
        buf[i] = z[i * rows:(i + 1) * rows, :] - lse[...]
        stores[i].start()
    k_out[...] = kv[0]
    v_out[...] = kv[1]
    lse_out[...] = lse[...]
    for store in stores:
        store.wait()


def close_call(z, lse, kv):
    share, rows = z.shape
    parts = 4
    vmem = pl.BlockSpec(memory_space=pltpu.VMEM)
    hbm = pl.BlockSpec(memory_space=pl.ANY)
    small = jax.ShapeDtypeStruct(kv.shape[1:], BF16)
    return pl.pallas_call(
        close_kernel, name="close",
        out_shape=[jax.ShapeDtypeStruct((share, rows), F32), small, small, jax.ShapeDtypeStruct((1, rows), F32)],
        in_specs=[vmem] * 3, out_specs=[hbm, vmem, vmem, vmem],
        scratch_shapes=[pltpu.VMEM((parts, share // parts, rows), F32), pltpu.SemaphoreType.DMA((parts,))],
        compiler_params=pltpu.CompilerParams(vmem_limit_bytes=16 * 2**20),
    )(z, lse, kv)


def solution(mesh):
    row_spec = P(("dp", "yax", "xax"))

    def local_step(hidden, cache_len, k_cache, v_cache, g_attn, w_query, w_key, w_value,
                   w_gate, w_up, w_out, w_down, g_final, embedding):
        width = hidden.shape[1]
        own_rows, _, head_dim = k_cache.shape
        half = head_dim // TWO
        lane = jnp.arange(head_dim)
        inv_freq = ROPE_BASE ** (-((lane % half).astype(F32) * 2.0) / head_dim)
        kv_new, logits_t, log_norm = step_call(
            cache_len, hidden.reshape(8, own_rows, width), g_attn[None], g_final[None], inv_freq[None],
            w_query, w_key, w_value, w_gate, w_up, w_out, w_down, embedding, k_cache, v_cache)
        log_probs, key_own, value_own, log_norm = close_call(logits_t, log_norm, kv_new)
        return key_own, value_own, log_probs.T, log_norm[0]

    in_specs = (P("dp", "xax"), P("dp"), row_spec, row_spec, P("xax"), P("xax", "yax"),
                P("xax", None), P("xax", None), P("xax", "yax"), P("xax", "yax"),
                P("yax", "xax"), P("yax", "xax"), P("xax"), P("yax", "xax"))
    out_specs = (row_spec, row_spec, P("dp", ("yax", "xax")), P("dp"))
    return jax.shard_map(local_step, mesh=mesh, in_specs=in_specs, out_specs=out_specs, check_vma=False)
```

```python
import functools

import jax
import jax.numpy as jnp
from jax import lax
from jax.experimental import pallas as pl
from jax.experimental.pallas import tpu as pltpu
from jax.sharding import PartitionSpec as P

EPS = 1e-6
ROPE_BASE = 10000.0
MESH = pl.DeviceIdType.MESH
F32 = jnp.float32
BF16 = jnp.bfloat16
LOW = -3e38
TWO, QUAD, OCT, OWN, PAIR, HALF, LANES = 2, 4, 8, 16, 32, 64, 128


def place():
    y = lax.axis_index("yax")
    xi = lax.axis_index("xax")
    chip = xi // 2
    core = xi % 2
    return y, xi, chip, core, chip * 2 + (1 - core), (1 - chip) * 2 + core


def send(src, dst, send_sem, recv_sem, y, xi):
    return pltpu.make_async_remote_copy(src_ref=src, dst_ref=dst, send_sem=send_sem, recv_sem=recv_sem,
                                        device_id={"yax": y, "xax": xi}, device_id_type=MESH)


def enter(peers):
    barrier = pltpu.get_barrier_semaphore()
    for y, xi in peers:
        pl.semaphore_signal(barrier, inc=1, device_id={"yax": y, "xax": xi}, device_id_type=MESH)
    return lambda: pl.semaphore_wait(barrier, len(peers))


def to_lanes(first, second):
    rows = first.shape[0]
    lane = lax.broadcasted_iota(jnp.int32, (rows, 128), 1)
    tile = jnp.where(lane == 0, first, jnp.where(lane == 1, second, 0.0))
    if rows < 128:
        tile = jnp.concatenate([tile, jnp.zeros((128 - rows, 128), F32)], axis=0)
    return tile.T[:8]


def to_columns(first, second):
    row = lax.broadcasted_iota(jnp.int32, (128, 128), 0)
    tile = jnp.where(row == 0, first, jnp.where(row == 1, second, 0.0)).T
    return tile[:, 0:1], tile[:, 1:2]


def stat_hops(stat, y, xi, send_sems, recv_sems):
    return [send(stat.at[xi], stat.at[xi], send_sems.at[d - 1], recv_sems.at[d - 1], y, (xi + d) % 4) for d in range(1, 4)]


def put_stats(values, stat, xi):
    mean_own = jnp.sum(values, axis=1, keepdims=True) / values.shape[1]
    diff = values - mean_own
    stat[xi] = to_lanes(mean_own, jnp.sum(diff * diff, axis=1, keepdims=True))


def take_stats(stat, rows, share):
    tiles = [stat[i] for i in range(4)]
    mean_all = sum(t[0:1] for t in tiles) / 4
    spread = sum(t[1:2] for t in tiles) + share * sum((t[0:1] - mean_all) * (t[0:1] - mean_all) for t in tiles)
    mean_col, rstd_col = to_columns(mean_all, lax.rsqrt(spread / (share * 4) + EPS))
    return mean_col[:rows], rstd_col[:rows]


FC = 512
WB = 1024
RING = 6
KVS = 3
VLIM = 121 * 2**19
HELD = 7


def step_kernel(lens, hid_h, gain_h, gain_fh, wq, wk, wv, wg, wu, wo, wd, emb, k_hbm, v_hbm,
                kv_out, z_out, lse_out,
                hid, gain, gain_f, cos, sin, n_perm, ring, w_kv, part_q, ga_q, sb_q, gb_q, total, q_rot, q_full, q_heads, o_heads, kn, vn,
                pool, act, o_in, o_all, k_buf, v_buf, scores, probs, acc, y_got, r_buf, f_all, f_nat, e_tail,
                t_a, t_b, t_x, tg_a, tg_b, t_c, tg_c, top, mass_l, stat, stat_f, stat_z,
                i_sem, r_sem, kv_sem, tail_sem, k_sem, v_sem, a_s, a_r, b_s, b_r, m_s, m_r, p_s, p_r, q_s, q_r,
                o_s, o_r, y_s, y_r, f_s, f_r, st_s, st_r, sf_s, sf_r,
                la_s, la_r, lb_s, lb_r, lc_s, lc_r, ta_s, ta_r, tb_s, tb_r, tc_s, tc_r, sz_s, sz_r):
    y, xi, chip, core, partner, twin = place()
    width = n_perm.shape[1]
    hw = width // TWO
    qc, hd = wq.shape[1], wk.shape[1]
    heads = qc // hd
    steps = wg.shape[1] // FC
    seqs = q_heads.shape[0]
    length = k_buf.shape[1]
    share = emb.shape[0] // 4
    full = share // WB
    rest = share - full * WB
    mine = y * 4 + xi
    ready = enter([(y, (xi + d) % 4) for d in (1, TWO, 3)] + [(1 - y, (xi + d) % 4) for d in range(4)])

    def start(copies):
        for copy in copies:
            copy.start()

    inputs = [pltpu.make_async_copy(src, dst, i_sem.at[i])
              for i, (src, dst) in enumerate(((hid_h, hid), (gain_h, gain), (gain_fh, gain_f)))]
    start(inputs)

    def q_loads(s):
        return [pltpu.make_async_copy(wq.at[:, pl.ds((TWO * s + i) * FC, FC)], ring.at[s, i], r_sem.at[s, i]) for i in range(TWO)]

    def w_loads(j):
        cols = pl.ds(pl.multiple_of(j * FC, FC), FC)
        slot = (j + TWO) % RING
        return [pltpu.make_async_copy(w.at[:, cols], ring.at[slot, i], r_sem.at[slot, i]) for i, w in enumerate((wg, wu))]

    kv_w = [pltpu.make_async_copy(w, w_kv.at[:, pl.ds(i * hd, hd)], kv_sem.at[i]) for i, w in enumerate((wk, wv))]
    for load in inputs:
        load.wait()
    start(q_loads(0))
    start(q_loads(1))
    start(kv_w)
    for j in range(RING - 3):
        start(w_loads(j))

    nd, no = wd.shape[0] // WB, wo.shape[0] // WB
    np_ = nd + no
    e_base = (np_, TWO * np_ + TWO * full)
    c_base = TWO * np_ + 4 * full
    d_base = c_base + full
    items = d_base + full
    far, near = (1 - chip) * TWO, chip * TWO

    def block(src, row, t):
        slot = t % RING
        return [pltpu.make_async_copy(src.at[pl.ds(row, WB), pl.ds(i * hw, hw)], ring.at[slot, i], r_sem.at[slot, i])
                for i in range(TWO)]

    def emb_row(quarter, k):
        return pl.multiple_of(quarter * share + k * WB, PAIR)

    def load_item(t):
        for base in (0, np_ + TWO * full):
            @pl.when((t >= base) & (t < base + nd))
            def _(base=base):
                start(block(wd, pl.multiple_of((t - base) * WB, WB), t))

            @pl.when((t >= base + nd) & (t < base + np_))
            def _(base=base):
                start(block(wo, pl.multiple_of((t - base - nd) * WB, WB), t))

        for base in e_base:
            @pl.when((t >= base) & (t < base + TWO * full))
            def _(base=base):
                k, own = (t - base) // TWO, (t - base) % TWO
                start(block(emb, emb_row(far + (1 - core) + own * (TWO * core - 1), k), t))

        @pl.when((t >= c_base) & (t < d_base))
        def _():
            start(block(emb, emb_row(near + 1 - core, t - c_base), t))

        @pl.when((t >= d_base) & (t < items))
        def _():
            start(block(emb, emb_row(near + core, t - d_base), t))

    def take_item(t):
        load_item(t + RING - 1)
        for copy in block(wd, 0, t):
            copy.wait()
        return t % RING

    def tail_load(i):
        quarter = (far + 1 - core, far + core, near + 1 - core, near + core)[i]
        rows = pl.ds(pl.multiple_of(quarter * share + full * WB, PAIR), rest)
        return pltpu.make_async_copy(emb.at[rows], e_tail.at[i], tail_sem.at[i])

    def cache_loads(b):
        slot = b % KVS
        return [pltpu.make_async_copy(k_hbm.at[b], k_buf.at[slot], k_sem.at[slot]),
                pltpu.make_async_copy(v_hbm.at[b], v_buf.at[slot], v_sem.at[slot])]

    def hop_a(j):
        return send(pool.at[pl.ds(TWO * j, TWO), 1 - core], pool.at[TWO * steps + j], a_s.at[j], a_r.at[j], y, partner)

    def sum_at(hf, p):
        return pool.at[3 * steps + hf * (steps // 4) + p // TWO, p % TWO]

    def got_at(hf, p):
        return pool.at[3 * steps + (TWO + hf) * (steps // 4) + p // TWO, p % TWO]

    def hop_b(hf, p):
        return send(sum_at(hf, p), got_at(hf, p), b_s.at[hf, p], b_r.at[hf, p], y, twin)

    def hop_m(hf, g):
        return send(act.at[hf, g, core, chip], act.at[hf, g, core, chip], m_s.at[hf, g], m_r.at[hf, g], y, twin)

    def hop_p(hf, g):
        return send(act.at[hf, g, core], act.at[hf, g, core], p_s.at[hf, g], p_r.at[hf, g], y, partner)

    q_cols = (pl.ds(0, TWO * FC), pl.ds(TWO * FC, qc + TWO * hd - TWO * FC))
    hop_qa = [send(part_q.at[:, 1 - core, :, :, cut], ga_q.at[..., cut], q_s.at[i, 0], q_r.at[i, 0], y, partner)
              for i, cut in enumerate(q_cols)]
    hop_qb = [send(sb_q.at[..., cut], gb_q.at[..., cut], q_s.at[i, 1], q_r.at[i, 1], y, twin) for i, cut in enumerate(q_cols)]

    def pair_queries(i):
        hop_qa[i].wait_recv()
        sb_q[:, :, q_cols[i]] = part_q[:, core, 1 - chip, :, q_cols[i]] + ga_q[:, 1 - chip, :, q_cols[i]]
        hop_qb[i].start()

    hop_qc = send(q_rot.at[1 - y], q_full.at[y], q_s.at[0, TWO], q_r.at[0, TWO], 1 - y, xi)

    def hop_o(hf, n):
        if n == 0:
            return send(o_in.at[1 - y, hf], o_all.at[hf, core, chip, y], o_s.at[hf, 0], o_r.at[hf, 0], 1 - y, xi)
        if n == 1:
            return send(o_all.at[hf, core, chip], o_all.at[hf, core, chip], o_s.at[hf, 1], o_r.at[hf, 1], y, twin)
        return send(o_all.at[hf, core], o_all.at[hf, core], o_s.at[hf, TWO], o_r.at[hf, TWO], y, partner)

    def hop_y(hf):
        return send(acc.at[hf, :, 1 - y], y_got.at[hf], y_s.at[hf], y_r.at[hf], 1 - y, xi)

    def hop_f(hf):
        return send(f_all.at[hf, y], f_all.at[hf, y], f_s.at[hf], f_r.at[hf], 1 - y, xi)

    def turns(owner):
        row = lax.broadcasted_iota(jnp.int32, (OWN, hd), 0)
        pos = functools.reduce(lambda acc_, r: jnp.where(row == r, lens[owner * OWN + r], acc_), range(OWN), jnp.zeros((OWN, hd), jnp.int32))
        lane = lax.broadcasted_iota(jnp.int32, (OWN, hd), 1)
        angle = pos.astype(F32) * ROPE_BASE ** (-((lane % (hd // 2)).astype(F32) * 2.0) / hd)
        return jnp.cos(angle), jnp.where(lane < hd // TWO, -jnp.sin(angle), jnp.sin(angle))

    h = hid[...].astype(F32).reshape(LANES, width)
    put_stats(h, stat, xi)
    ready()
    first = stat_hops(stat, y, xi, st_s, st_r)
    start(first)
    for copy in first:
        copy.wait()
    mean, rstd = take_stats(stat, LANES, width)
    normed = ((h - mean) * rstd * gain[...]).astype(BF16)
    for hf in range(TWO):
        for core_o in range(TWO):
            for chip_o in range(TWO):
                for y_o in range(TWO):
                    src = (y_o * 4 + chip_o * TWO + core_o) * OWN + hf * 8
                    dst = hf * HALF + core_o * PAIR + chip_o * OWN + y_o * 8
                    n_perm[dst:dst + 8, :] = normed[src:src + 8, :]

    for s in range(TWO):
        for i, load in enumerate(q_loads(s)):
            load.wait()
            prod = jnp.dot(n_perm[...], ring[s, i], preferred_element_type=F32)
            part_q[:, :, :, :, (TWO * s + i) * FC:(TWO * s + i + 1) * FC] = prod.reshape(TWO, TWO, TWO, OWN, FC)
        start(w_loads(RING - 3 + s))
        if s == 0:
            hop_qa[0].start()
    for load in kv_w:
        load.wait()
    part_q[..., qc:] = jnp.dot(n_perm[...], w_kv[...], preferred_element_type=F32).reshape(TWO, TWO, TWO, OWN, TWO * hd)
    hop_qa[1].start()
    pair_queries(0)

    def rotate_queries():
        hop_qb[0].wait_recv()
        hop_qb[1].wait_recv()
        both = part_q[:, core, chip] + ga_q[:, chip] + gb_q[...]
        total[...] = both.astype(BF16).astype(F32).reshape(TWO, TWO, 8, qc + TWO * hd)
        for y_o in range(TWO):
            cos_r, sin_r = cos[y_o], sin[y_o]
            for head in range(heads):
                val = total[:, y_o, :, head * hd:(head + 1) * hd].reshape(OWN, hd)
                q_rot[y_o, :, head * hd:(head + 1) * hd] = (val * cos_r + pltpu.roll(val, hd // TWO, 1) * sin_r).astype(BF16)
        hop_qc.start()
        key = total[:, y, :, qc:qc + hd].reshape(OWN, hd)
        value = total[:, y, :, qc + hd:].reshape(OWN, hd)
        key = (key * cos[y] + pltpu.roll(key, hd // TWO, 1) * sin[y]).astype(BF16)
        kv_out[0] = key
        kv_out[1] = value.astype(BF16)
        kn[:, 0, :] = key.astype(F32)
        vn[:, 0, :] = value
        q_full[y] = q_rot[y]

    def spread_queries():
        hop_qc.wait_recv()
        for y_o in range(TWO):
            for head in range(heads):
                q_heads[:, y_o * heads + head, :] = q_full[y_o, :, head * hd:(head + 1) * hd].astype(F32)

    def add_pair(j):
        hop_a(j).wait_recv()
        for hf in range(TWO):
            sum_at(hf, j // TWO)[j % TWO] = pool[TWO * j + hf, core, 1 - chip] + pool[TWO * steps + j, hf, 1 - chip]

        @pl.when(j % TWO == 1)
        def _():
            hop_b(0, j // TWO).start()

    def project(j, carry):
        @pl.when(j + RING - 1 < steps)
        def _():
            start(w_loads(j + RING - 1))

        slot = (j + TWO) % RING
        for i, load in enumerate(w_loads(j)):
            load.wait()
            prod = jnp.dot(n_perm[...], ring[slot, i], preferred_element_type=F32)
            pool[pl.ds(TWO * j, TWO), :, :, :, i * FC:(i + 1) * FC] = prod.reshape(TWO, TWO, TWO, OWN, FC)
        hop_a(j).start()

        @pl.when(j == 0)
        def _():
            pair_queries(1)

        @pl.when(j >= 1)
        def _():
            add_pair(j - 1)

        @pl.when((j == TWO) | (j == 3))
        def _():
            cos[j - TWO], sin[j - TWO] = turns((j - TWO) * 4 + chip * TWO + core)

        @pl.when(j == 4)
        def _():
            for b in range(KVS):
                start(cache_loads(b))

        @pl.when(j == 8)
        def _():
            rotate_queries()

        @pl.when(j == 12)
        def _():
            spread_queries()
        return carry

    lax.fori_loop(0, steps, project, 0)
    add_pair(steps - 1)
    for t in range(RING - 1):
        start(block(wd, t * WB, t))
    for i in range(4):
        tail_load(i).start()

    def activate(hf, p):
        hop_b(hf, p).wait_recv()
        for i in range(TWO):
            j = TWO * p + i
            both = pool[TWO * j + hf, core, chip] + pool[TWO * steps + j, hf, chip] + got_at(hf, p)[i]
            gate = both[:, :FC].astype(BF16).astype(F32)
            up_val = both[:, FC:].astype(BF16).astype(F32)
            cols = pl.ds(pl.multiple_of(((p % 4) * TWO + i) * FC, FC), FC)
            act[hf, p // 4, core, chip, :, cols] = (jax.nn.silu(gate) * up_val).astype(BF16)

        @pl.when(p % 4 == 3)
        def _():
            hop_m(hf, p // 4).start()

    part_len = 1024

    def attend(b):
        slot = b % KVS
        scale = hd ** -0.5
        q32 = q_heads[b]
        q = q32.astype(BF16)
        limit = lens[mine * OWN + b]
        s_new = jnp.sum(q32 * kn[b], axis=1, keepdims=True) * scale
        load_k, load_v = cache_loads(b)
        load_k.wait()
        high = None
        for i in range(length // part_len):
            rows = slice(i * part_len, (i + 1) * part_len)
            s = lax.dot_general(q, k_buf[slot, rows], (((1,), (1,)), ((), ())), preferred_element_type=F32) * scale
            pos = lax.broadcasted_iota(jnp.int32, s.shape, 1) + i * part_len
            s = jnp.where(pos < limit, s, -jnp.inf)
            scores[:, rows] = s
            for c in range(0, part_len, LANES):
                high = s[:, c:c + LANES] if high is None else jnp.maximum(high, s[:, c:c + LANES])
        best = jnp.maximum(jnp.max(high, axis=1, keepdims=True), s_new)
        mass = None
        for i in range(length // part_len):
            rows = slice(i * part_len, (i + 1) * part_len)
            e = jnp.exp(scores[:, rows] - best)
            scores[:, rows] = e
            for c in range(0, part_len, LANES):
                mass = e[:, c:c + LANES] if mass is None else mass + e[:, c:c + LANES]
        e_new = jnp.exp(s_new - best)
        inv = 1.0 / (jnp.sum(mass, axis=1, keepdims=True) + e_new)
        for i in range(length // part_len):
            rows = slice(i * part_len, (i + 1) * part_len)
            probs[:, rows] = (scores[:, rows] * inv).astype(BF16)
        load_v.wait()
        o = jnp.dot(probs[...], v_buf[slot], preferred_element_type=F32)
        o = o + (e_new * inv).astype(BF16).astype(F32) * vn[b]
        o_heads[b] = o.astype(BF16).astype(F32)

        @pl.when(b + KVS < seqs)
        def _():
            start(cache_loads(b + KVS))

    def send_heads(hf):
        for y_o in range(TWO):
            for head in range(heads):
                o_in[y_o, hf, :, head * hd:(head + 1) * hd] = o_heads[hf * 8:hf * 8 + 8, y_o * heads + head, :].astype(BF16)
        o_all[hf, core, chip, y] = o_in[y, hf]
        hop_o(hf, 0).start()

    def contract(hf):
        base = hf * (np_ + TWO * full)
        acc[hf] = jnp.zeros(acc.shape[1:], F32)

        def add(t, left):
            slot = take_item(t)
            for i in range(TWO):
                prod = jnp.dot(left, ring[slot, i], preferred_element_type=F32)
                acc[hf, :, :, :, i * hw:(i + 1) * hw] += prod.reshape(4, TWO, 8, hw)

        for g in range(TWO):
            hop_p(hf, g).wait_recv()

            def from_act(i, carry):
                add(base + g * (nd // TWO) + i, act[hf, g, :, :, :, pl.ds(pl.multiple_of(i * WB, WB), WB)].reshape(HALF, WB))
                return carry

            lax.fori_loop(0, nd // TWO, from_act, 0)
        hop_o(hf, TWO).wait_recv()

        def from_heads(i, carry):
            add(base + nd + i, o_all[hf, :, :, :, :, pl.ds(pl.multiple_of(i * WB, WB), WB)].reshape(HALF, WB))
            return carry

        lax.fori_loop(0, no, from_heads, 0)

    def finish_sum(hf):
        hop_y(hf).wait_recv()
        res = [hid[y * 4 + (i % 2) * 2 + i // 2, hf * 8:hf * 8 + 8].astype(F32) for i in range(4)]
        branch = acc[hf, :, y] + y_got[hf]
        r_buf[...] = jnp.concatenate(res, axis=0) + branch.reshape(PAIR, width)
        put_stats(r_buf[...], stat_f.at[hf], xi)
        start(stat_hops(stat_f.at[hf], y, xi, sf_s.at[hf], sf_r.at[hf]))

    def finish_norm(hf):
        for copy in stat_hops(stat_f.at[hf], y, xi, sf_s.at[hf], sf_r.at[hf]):
            copy.wait()
        mean, rstd = take_stats(stat_f.at[hf], PAIR, width)
        f = ((r_buf[...] - mean) * rstd * gain_f[...]).astype(BF16)
        for i in range(4):
            f_all[hf, y, (i % 2) * 2 + i // 2] = f[i * 8:(i + 1) * 8]
        hop_f(hf).start()

    def each(body, low, high):
        def step(p, carry):
            body(p)
            return carry

        lax.fori_loop(low, high, step, 0)

    def pass_m(hf):
        for g in range(TWO):
            hop_m(hf, g).wait_recv()
            hop_p(hf, g).start()

    def pass_o(hf, n):
        hop_o(hf, n).wait_recv()
        hop_o(hf, n + 1).start()

    def mix(i):
        pl.when(i == 8)(lambda: send_heads(0))
        attend(i)
        pl.when(i < 8)(lambda: activate(0, i))

        pl.when((i == 5) | (i == 7))(lambda: hop_b(1, (i - 5) // 2).start())

        @pl.when(i == 8)
        def _():
            pass_o(0, 0)
            each(lambda p: hop_b(1, p).start(), 2, HELD)

        pl.when(i == 10)(lambda: pass_m(0))
        pl.when(i == 11)(lambda: pass_o(0, 1))

        @pl.when(i == 12)
        def _():
            each(lambda j: hop_a(j).wait_send(), 0, steps)
            each(lambda p: hop_b(0, p).wait_send(), 0, 8)
            contract(0)
            hop_y(0).start()
            each(lambda p: activate(1, p), 0, 2)

        @pl.when(i == 13)
        def _():
            finish_sum(0)
            each(lambda p: hop_b(1, p).start(), HELD, 8)

        @pl.when(i == 14)
        def _():
            finish_norm(0)
            each(lambda p: activate(1, p), 2, 4)

    each(mix, 0, seqs)
    each(lambda p: activate(1, p), 4, 8)
    hop_f(0).wait_recv()
    send_heads(1)

    def out_at(hf, k):
        return 56 - hf * 6 + k

    def in_at(hf, k):
        return PAIR + k if hf else 20 + TWO * k

    def lhop_a(hf, k):
        return send(pool.at[k], pool.at[8 + TWO * k], la_s.at[hf, k], la_r.at[hf, k], y, partner)

    def lhop_b(hf, k):
        return send(pool.at[out_at(hf, k)], pool.at[in_at(hf, k)], lb_s.at[hf, k], lb_r.at[hf, k], y, twin)

    def lhop_c(k):
        return send(pool.at[pl.ds(6 + TWO * k, TWO)], pool.at[pl.ds(38 + TWO * k, TWO)], lc_s.at[k], lc_r.at[k], y, partner)

    def thop_a(hf):
        return send(t_a.at[hf], tg_a.at[hf], ta_s.at[hf], ta_r.at[hf], y, partner)

    def thop_b(hf):
        return send(t_x.at[hf], tg_b.at[hf], tb_s.at[hf], tb_r.at[hf], y, twin)

    thop_c = send(t_c, tg_c, tc_s.at[0], tc_r.at[0], y, partner)
    nt = (((1,), (1,)), ((), ()))

    def product(left, slot, n):
        rows = slice(n * hw, (n + 1) * hw)
        return (lax.dot_general(left[:, :hw], ring[slot, 0, rows], nt, preferred_element_type=F32)
                + lax.dot_general(left[:, hw:], ring[slot, 1, rows], nt, preferred_element_type=F32))

    def tail_product(left, i):
        return lax.dot_general(left, e_tail[i], nt, preferred_element_type=F32)

    t_a[...] = jnp.zeros_like(t_a)
    t_b[...] = jnp.zeros_like(t_b)
    t_c[...] = jnp.zeros_like(t_c)

    def outward(hf):
        def chunk(k):
            left = f_all[hf].reshape(HALF, width)
            if hf == 1:
                lhop_a(0, k).wait_send()
            slot = take_item(e_base[hf] + TWO * k)
            for n in range(TWO):
                pool[k, :, :, :, n * hw:(n + 1) * hw] = product(left, slot, n).reshape(TWO, TWO, OWN, hw)
            lhop_a(hf, k).start()
            slot = take_item(e_base[hf] + TWO * k + 1)
            for n in range(TWO):
                pool[out_at(hf, k), :, :, :, n * hw:(n + 1) * hw] = product(left, slot, n).reshape(TWO, TWO, OWN, hw)
            lhop_a(hf, k).wait_recv()
            pool[out_at(hf, k)] += pool[8 + TWO * k]
            if hf == 0:
                pl.when(k < full - TWO)(lambda: lhop_b(0, k).start())

                pl.when(k == 0)(lambda: pass_o(1, 0))
            else:
                lhop_b(1, k).start()

        each(chunk, 0, full)
        left = f_all[hf].reshape(HALF, width)
        if hf == 0:
            tail_load(0).wait()
            tail_load(1).wait()
        t_a[hf, :, :rest] = tail_product(left, 0)
        thop_a(hf).start()
        t_b[hf, :, :rest] = tail_product(left, 1)
        thop_a(hf).wait_recv()
        both = t_b[hf] + tg_a[hf]
        t_x[hf, :HALF] = both[:, :LANES]
        quarters = [both[i * OWN:(i + 1) * OWN, LANES:rest] for i in range(QUAD)]
        t_x[hf, HALF:] = jnp.concatenate(quarters, axis=1)
        if hf == 1:
            thop_b(1).start()

    outward(0)
    pass_m(1)
    pass_o(1, 1)
    each(lambda p: hop_b(1, p).wait_send(), 0, 8)
    contract(1)
    hop_y(1).start()
    finish_sum(1)
    each(lambda k: lhop_b(0, k).start(), full - 2, full)
    thop_b(0).start()
    finish_norm(1)
    hop_f(1).wait_recv()
    outward(1)

    for g in range(8):
        for hf in range(TWO):
            f_nat[g * OWN + hf * 8:g * OWN + hf * 8 + 8, :] = f_all[hf, g // 4, g % 4]

    def inward(k, carry):
        slot = take_item(c_base + k)
        for n in range(TWO):
            pool[pl.ds(6 + TWO * k, TWO), :, :, :, n * hw:(n + 1) * hw] = product(f_nat[...], slot, n).reshape(TWO, TWO, TWO, OWN, hw)
        lhop_c(k).start()
        return carry

    lax.fori_loop(0, full, inward, 0)
    tail_load(TWO).wait()
    t_c[:, :rest] = tail_product(f_nat[...], TWO)
    thop_c.start()
    tail_load(3).wait()

    top[...] = jnp.full_like(top, LOW)
    mass_l[...] = jnp.zeros_like(mass_l)

    def fold(z):
        tiles = [z[:, i:i + LANES] for i in range(0, z.shape[1], LANES)]
        high = functools.reduce(jnp.maximum, tiles, top[...])
        mass_l[...] = mass_l[...] * jnp.exp(top[...] - high) + sum(jnp.exp(g - high) for g in tiles)
        top[...] = high

    def weave(first, second):
        n = first.shape[-1]
        return jnp.stack([first.reshape(8, 8, n), second.reshape(8, 8, n)], axis=1).reshape(LANES, n)

    def finish(k):
        slot = take_item(d_base + k)
        lhop_c(k).wait_recv()
        here = pl.ds(38 + TWO * k, TWO)
        for n in range(TWO):
            cols = slice(n * hw, (n + 1) * hw)
            pool[here, :, :, :, cols] += product(f_nat[...], slot, n).reshape(TWO, TWO, TWO, OWN, hw)
        lhop_b(0, k).wait_recv()
        lhop_b(1, k).wait_recv()
        for n in range(TWO):
            cols = slice(n * hw, (n + 1) * hw)
            z = pool[here, :, :, :, cols].reshape(LANES, hw)
            z = z + weave(pool[in_at(0, k), :, :, :, cols], pool[in_at(1, k), :, :, :, cols])
            z_out[pl.ds(pl.multiple_of(k * WB + n * hw, hw), hw), :] = z.T
            fold(z)

    thop_c.wait_recv()
    tg_c[:, :rest] += tail_product(f_nat[...], 3)
    each(finish, 0, full)
    thop_b(0).wait_recv()
    thop_b(1).wait_recv()
    over = rest - LANES

    def unpack(block):
        edge = jnp.concatenate([block[HALF:, i * over:(i + 1) * over] for i in range(QUAD)], axis=0)
        return jnp.concatenate([block[:HALF], edge, jnp.zeros((HALF, LANES - over), F32)], axis=1)

    z_tail = tg_c[...] + weave(unpack(tg_b[0]), unpack(tg_b[1]))
    lane = lax.broadcasted_iota(jnp.int32, z_tail.shape, 1)
    fold(jnp.where(lane < rest, z_tail, LOW))
    z_out[full * WB:, :] = z_tail.T[:rest]

    high = jnp.max(top[...], axis=1, keepdims=True)
    stat_z[mine] = to_lanes(high, jnp.sum(mass_l[...] * jnp.exp(top[...] - high), axis=1, keepdims=True))
    copies = []
    for dy in range(TWO):
        for d in range(4):
            if dy or d:
                i = dy * 4 + d - 1
                copies.append(send(stat_z.at[mine], stat_z.at[mine], sz_s.at[i], sz_r.at[i],
                                   y + dy * (1 - TWO * y), (xi + d) % 4))
    start(copies)
    for copy in copies:
        copy.wait()
    highs = [stat_z[i][0:1] for i in range(8)]
    best_all = functools.reduce(jnp.maximum, highs)
    lse_out[...] = best_all + jnp.log(sum(stat_z[i][1:TWO] * jnp.exp(highs[i] - best_all) for i in range(8)))

    def drain_logits(k, carry):
        lhop_a(1, k).wait_send()
        lhop_b(0, k).wait_send()
        lhop_b(1, k).wait_send()
        lhop_c(k).wait_send()
        return carry

    lax.fori_loop(0, full, drain_logits, 0)
    for hf in range(TWO):
        for g in range(TWO):
            hop_m(hf, g).wait_send()
            hop_p(hf, g).wait_send()
        for n in range(3):
            hop_o(hf, n).wait_send()
        for hop in (hop_y, hop_f, thop_a, thop_b):
            hop(hf).wait_send()
    for hop in (*hop_qa, *hop_qb, hop_qc, thop_c):
        hop.wait_send()


def step_call(lens, hid, gain, gain_f, wq, wk, wv, wg, wu, wo, wd, emb, k_cache, v_cache):
    width = hid.shape[TWO]
    qc, hd = wq.shape[1], wk.shape[1]
    seqs, length, _ = k_cache.shape
    cols = qc + TWO * hd
    steps = wg.shape[1] // FC
    heads = TWO * qc // hd
    share = emb.shape[0] // QUAD
    full = share // WB
    rest = share - full * WB
    tail_w = -(-rest // LANES) * LANES
    vmem = pl.BlockSpec(memory_space=pltpu.VMEM)
    hbm = pl.BlockSpec(memory_space=pl.ANY)

    def f32(*shape):
        return pltpu.VMEM(shape, F32)

    def bf16(*shape):
        return pltpu.VMEM(shape, BF16)

    def dma(*shape):
        return pltpu.SemaphoreType.DMA(shape)

    return pl.pallas_call(
        step_kernel, name="step",
        out_shape=[bf16(TWO, OWN, hd), f32(share, LANES), f32(1, LANES)],
        in_specs=[pl.BlockSpec(memory_space=pltpu.SMEM)] + [hbm] * 13, out_specs=[vmem] * 3,
        scratch_shapes=[
            bf16(OCT, OWN, width), f32(1, width), f32(1, width), f32(TWO, OWN, hd), f32(TWO, OWN, hd),
            bf16(LANES, width), bf16(RING, TWO, width, FC), bf16(width, TWO * hd),
            f32(TWO, TWO, TWO, OWN, cols), f32(TWO, TWO, OWN, cols), f32(TWO, OWN, cols), f32(TWO, OWN, cols), f32(TWO, TWO, OCT, cols),
            bf16(TWO, OWN, qc), bf16(TWO, OWN, qc), f32(seqs, heads, hd), f32(seqs, heads, hd), f32(seqs, 1, hd), f32(seqs, 1, hd),
            f32(QUAD * steps, TWO, TWO, OWN, TWO * FC), bf16(TWO, TWO, TWO, TWO, OWN, steps // TWO * FC),
            bf16(TWO, TWO, OCT, qc), bf16(TWO, TWO, TWO, TWO, OCT, qc),
            bf16(KVS, length, hd), bf16(KVS, length, hd), f32(heads, length), bf16(heads, length),
            f32(TWO, QUAD, TWO, OCT, width), f32(TWO, QUAD, OCT, width), f32(PAIR, width), bf16(TWO, TWO, QUAD, OCT, width), bf16(LANES, width), bf16(QUAD, rest, width),
            f32(TWO, HALF, tail_w), f32(TWO, HALF, tail_w), f32(TWO, HALF + OWN, LANES), f32(TWO, HALF, tail_w), f32(TWO, HALF + OWN, LANES), f32(LANES, tail_w), f32(LANES, tail_w),
            f32(LANES, LANES), f32(LANES, LANES), f32(QUAD, OCT, LANES), f32(TWO, QUAD, OCT, LANES), f32(OCT, OCT, LANES),
            dma(3), dma(RING, TWO), dma(TWO), dma(QUAD), dma(KVS), dma(KVS), dma(steps), dma(steps), dma(TWO, steps // TWO), dma(TWO, steps // TWO),
            dma(TWO, TWO), dma(TWO, TWO), dma(TWO, TWO), dma(TWO, TWO), dma(TWO, 3), dma(TWO, 3),
            dma(TWO, 3), dma(TWO, 3), dma(TWO), dma(TWO), dma(TWO), dma(TWO), dma(3), dma(3), dma(TWO, 3), dma(TWO, 3),
            dma(TWO, full), dma(TWO, full), dma(TWO, full), dma(TWO, full), dma(full), dma(full),
            dma(TWO), dma(TWO), dma(TWO), dma(TWO), dma(1), dma(1), dma(7), dma(7)],
        compiler_params=pltpu.CompilerParams(collective_id=0, has_side_effects=True, vmem_limit_bytes=VLIM),
    )(lens, hid, gain, gain_f, wq, wk, wv, wg, wu, wo, wd, emb, k_cache, v_cache)


def close_kernel(z, lse, kv, out, k_out, v_out, lse_out, buf, out_sem):
    parts = buf.shape[0]
    rows = buf.shape[1]
    stores = [pltpu.make_async_copy(buf.at[i], out.at[pl.ds(i * rows, rows)], out_sem.at[i]) for i in range(parts)]
    for i in range(parts):
        buf[i] = z[i * rows:(i + 1) * rows, :] - lse[...]
        stores[i].start()
    k_out[...] = kv[0]
    v_out[...] = kv[1]
    lse_out[...] = lse[...]
    for store in stores:
        store.wait()


def close_call(z, lse, kv):
    share, rows = z.shape
    parts = 4
    vmem = pl.BlockSpec(memory_space=pltpu.VMEM)
    hbm = pl.BlockSpec(memory_space=pl.ANY)
    small = jax.ShapeDtypeStruct(kv.shape[1:], BF16)
    return pl.pallas_call(
        close_kernel, name="close",
        out_shape=[jax.ShapeDtypeStruct((share, rows), F32), small, small, jax.ShapeDtypeStruct((1, rows), F32)],
        in_specs=[vmem] * 3, out_specs=[hbm, vmem, vmem, vmem],
        scratch_shapes=[pltpu.VMEM((parts, share // parts, rows), F32), pltpu.SemaphoreType.DMA((parts,))],
        compiler_params=pltpu.CompilerParams(vmem_limit_bytes=16 * 2**20),
    )(z, lse, kv)


def solution(mesh):
    row_spec = P(("dp", "yax", "xax"))

    def local_step(hidden, cache_len, k_cache, v_cache, g_attn, w_query, w_key, w_value,
                   w_gate, w_up, w_out, w_down, g_final, embedding):
        width = hidden.shape[1]
        own_rows = k_cache.shape[0]
        kv_new, logits_t, log_norm = step_call(
            cache_len, hidden.reshape(8, own_rows, width), g_attn[None], g_final[None],
            w_query, w_key, w_value, w_gate, w_up, w_out, w_down, embedding, k_cache, v_cache)
        log_probs, key_own, value_own, log_norm = close_call(logits_t, log_norm, kv_new)
        return key_own, value_own, log_probs.T, log_norm[0]

    in_specs = (P("dp", "xax"), P("dp"), row_spec, row_spec, P("xax"), P("xax", "yax"),
                P("xax", None), P("xax", None), P("xax", "yax"), P("xax", "yax"),
                P("yax", "xax"), P("yax", "xax"), P("xax"), P("yax", "xax"))
    out_specs = (row_spec, row_spec, P("dp", ("yax", "xax")), P("dp"))
    return jax.shard_map(local_step, mesh=mesh, in_specs=in_specs, out_specs=out_specs, check_vma=False)
```
